8 devices in a mesh: dp: 2 (over z, y), ep: 4 (over x, core).
Axes of the slice: x: 2, y: 2, z: 1, core: 2. Of those that a mesh axis runs over, the one named last changes fastest.
Arguments:
- x_tokens: bfloat16 [1024, 2048], P(('dp', 'ep')), parts along dimension 0
- dy_tokens: bfloat16 [1024, 2048], P(('dp', 'ep')), parts along dimension 0
- expert_ids: int32 [1024, 10], P(('dp', 'ep')), parts along dimension 0
- gate_vals: float32 [1024, 10], P(('dp', 'ep')), parts along dimension 0
- slot_pos: int32 [1024, 10], P(('dp', 'ep')), parts along dimension 0
- w_gate: bfloat16 [32, 2048, 512], P('ep')
- w_up: bfloat16 [32, 2048, 512], P('ep')
- w_down: bfloat16 [32, 512, 2048], P('ep')
- shared_gate: bfloat16 [2048, 512], replicated
- shared_up: bfloat16 [2048, 512], replicated
- shared_down: bfloat16 [512, 2048], replicated
Outputs:
- output 1: bfloat16 [1024, 2048], P(('dp', 'ep')), parts along dimension 0
- output 2: float32 [64, 2048, 512], P(('dp', 'ep')), parts along dimension 0
- output 3: float32 [64, 2048, 512], P(('dp', 'ep')), parts along dimension 0
- output 4: float32 [64, 512, 2048], P(('dp', 'ep')), parts along dimension 0
- output 5: float32 [8, 2048, 512], P(('dp', 'ep')), parts along dimension 0
- output 6: float32 [8, 2048, 512], P(('dp', 'ep')), parts along dimension 0
- output 7: float32 [8, 512, 2048], P(('dp', 'ep')), parts along dimension 0
There are 2 independent parts. The reference program is written for one: setup_inputs(seed, part) draws one part's arguments, and reference() takes and returns one part's arrays. A program takes and returns all parts, laid end to end along the dimension named above; an argument that names none is the same for every part.
All inputs are finite; a program needn't handle non-finite values.
Results may differ from the reference program's by a relative error of at most 0.0104471.
Values are sent between devices in bfloat16 or wider.
A program may use at most 1 GiB of HBM per device.

```python
import jax
import jax.numpy as jnp
from jax import lax

MODEL_DIM = 2048
EXPERT_FF = 512
SHARED_FF = 512
TOP_K = 10
TOK_DEV = 128
GROUP_SIZE = 4
NUM_EXPERTS = 32
CAPACITY = 60


def draw_routing(route_key):
    bias_key, hot_key, noise_key = jax.random.split(route_key, 3)
    expert_range = jnp.arange(NUM_EXPERTS, dtype=jnp.int32)
    expert_bias = jax.random.randint(bias_key, (NUM_EXPERTS,), 0, 256)
    hot_expert = jax.random.randint(hot_key, (GROUP_SIZE,), 0, NUM_EXPERTS)
    noise = jax.random.randint(noise_key, (GROUP_SIZE, TOK_DEV, NUM_EXPERTS), 0, 1024)
    forced = (jnp.arange(TOK_DEV)[None, :, None] < CAPACITY) & (expert_range[None, None, :] == hot_expert[:, None, None])
    score = (noise + expert_bias[None, None, :] + 4096 * forced.astype(jnp.int32)) * NUM_EXPERTS + expert_range
    choices = lax.top_k(score, TOP_K)[1]

    def source_slots(source_choices):
        flat_choices = source_choices.reshape(-1)
        onehot = (flat_choices[:, None] == expert_range[None, :]).astype(jnp.int32)
        earlier = jnp.cumsum(onehot, axis=0) - onehot
        slot_rank = jnp.sum(earlier * onehot, axis=1)
        return jnp.where(slot_rank < CAPACITY, slot_rank, -1).reshape(TOK_DEV, TOP_K)

    positions = lax.map(source_slots, choices)
    return choices.reshape(-1, TOP_K).astype(jnp.int32), positions.reshape(-1, TOP_K).astype(jnp.int32)


def setup_inputs(seed: int = 0, part: int = 0) -> dict:
    part_key = jax.random.fold_in(jax.random.key(seed), part)
    key_x, key_dy, key_gate, key_route = jax.random.split(part_key, 4)
    weight_keys = jax.random.split(jax.random.key(seed + 1), 6)
    tokens = GROUP_SIZE * TOK_DEV
    x_tokens = jax.random.normal(key_x, (tokens, MODEL_DIM), jnp.float32).astype(jnp.bfloat16)
    dy_tokens = jax.random.normal(key_dy, (tokens, MODEL_DIM), jnp.float32).astype(jnp.bfloat16)
    gate_vals = jax.random.uniform(key_gate, (tokens, TOP_K), jnp.float32, 0.25, 1.0)
    expert_ids, slot_pos = draw_routing(key_route)
    in_scale = MODEL_DIM ** -0.5
    ff_scale = EXPERT_FF ** -0.5
    shared_scale = SHARED_FF ** -0.5
    w_gate = (jax.random.normal(weight_keys[0], (NUM_EXPERTS, MODEL_DIM, EXPERT_FF), jnp.float32) * in_scale).astype(jnp.bfloat16)
    w_up = (jax.random.normal(weight_keys[1], (NUM_EXPERTS, MODEL_DIM, EXPERT_FF), jnp.float32) * in_scale).astype(jnp.bfloat16)
    w_down = (jax.random.normal(weight_keys[2], (NUM_EXPERTS, EXPERT_FF, MODEL_DIM), jnp.float32) * ff_scale).astype(jnp.bfloat16)
    shared_gate = (jax.random.normal(weight_keys[3], (MODEL_DIM, SHARED_FF), jnp.float32) * in_scale).astype(jnp.bfloat16)
    shared_up = (jax.random.normal(weight_keys[4], (MODEL_DIM, SHARED_FF), jnp.float32) * in_scale).astype(jnp.bfloat16)
    shared_down = (jax.random.normal(weight_keys[5], (SHARED_FF, MODEL_DIM), jnp.float32) * shared_scale).astype(jnp.bfloat16)
    return {'x_tokens': x_tokens, 'dy_tokens': dy_tokens, 'expert_ids': expert_ids, 'gate_vals': gate_vals, 'slot_pos': slot_pos, 'w_gate': w_gate, 'w_up': w_up, 'w_down': w_down, 'shared_gate': shared_gate, 'shared_up': shared_up, 'shared_down': shared_down}


def expert_grads(x_rows, dz_rows, gate_w, up_w, down_w):
    act_gate = jnp.dot(x_rows, gate_w, preferred_element_type=jnp.float32).astype(jnp.bfloat16)
    act_up = jnp.dot(x_rows, up_w, preferred_element_type=jnp.float32).astype(jnp.bfloat16)
    gate_f32 = act_gate.astype(jnp.float32)
    up_f32 = act_up.astype(jnp.float32)
    sigma = jax.nn.sigmoid(gate_f32)
    silu_gate = gate_f32 * sigma
    hidden = (silu_gate * up_f32).astype(jnp.bfloat16)
    grad_hidden = jnp.dot(dz_rows, down_w.T, preferred_element_type=jnp.float32)
    grad_gate = (grad_hidden * up_f32 * sigma * (1.0 + gate_f32 * (1.0 - sigma))).astype(jnp.bfloat16)
    grad_up = (grad_hidden * silu_gate).astype(jnp.bfloat16)
    grad_down_w = jnp.dot(hidden.T, dz_rows, preferred_element_type=jnp.float32)
    grad_gate_w = jnp.dot(x_rows.T, grad_gate, preferred_element_type=jnp.float32)
    grad_up_w = jnp.dot(x_rows.T, grad_up, preferred_element_type=jnp.float32)
    grad_rows = jnp.dot(grad_gate, gate_w.T, preferred_element_type=jnp.float32) + jnp.dot(grad_up, up_w.T, preferred_element_type=jnp.float32)
    return grad_rows, grad_gate_w, grad_up_w, grad_down_w


def reference(x_tokens, dy_tokens, expert_ids, gate_vals, slot_pos, w_gate, w_up, w_down, shared_gate, shared_up, shared_down):
    tokens = GROUP_SIZE * TOK_DEV
    slot_rows = GROUP_SIZE * CAPACITY
    total_rows = NUM_EXPERTS * slot_rows
    source = jnp.arange(tokens, dtype=jnp.int32)[:, None] // TOK_DEV
    target = jnp.where(slot_pos >= 0, expert_ids * slot_rows + source * CAPACITY + slot_pos, total_rows).reshape(-1)
    token_index = jnp.broadcast_to(jnp.arange(tokens, dtype=jnp.int32)[:, None], (tokens, TOP_K)).reshape(-1)
    row_token = jnp.full((total_rows + 1,), tokens, jnp.int32).at[target].set(token_index)[:total_rows].reshape(NUM_EXPERTS, slot_rows)
    row_gate = jnp.zeros((total_rows + 1,), jnp.float32).at[target].set(gate_vals.reshape(-1))[:total_rows].reshape(NUM_EXPERTS, slot_rows)

    def expert_step(routed_sum, expert_in):
        token_rows, gate_rows, gate_w, up_w, down_w = expert_in
        x_rows = jnp.take(x_tokens, token_rows, axis=0, mode='fill', fill_value=0)
        dy_rows = jnp.take(dy_tokens, token_rows, axis=0, mode='fill', fill_value=0)
        dz_rows = (dy_rows.astype(jnp.float32) * gate_rows[:, None]).astype(jnp.bfloat16)
        grad_rows, grad_gate_w, grad_up_w, grad_down_w = expert_grads(x_rows, dz_rows, gate_w, up_w, down_w)
        returned = grad_rows.astype(jnp.bfloat16).astype(jnp.float32)
        routed_sum = routed_sum.at[token_rows].add(returned, mode='drop')
        return routed_sum, (grad_gate_w, grad_up_w, grad_down_w)

    routed_sum, expert_w_grads = lax.scan(expert_step, jnp.zeros((tokens, MODEL_DIM), jnp.float32), (row_token, row_gate, w_gate, w_up, w_down))
    grad_w_gate, grad_w_up, grad_w_down = expert_w_grads

    def shared_step(source_in):
        x_rows, dy_rows = source_in
        return expert_grads(x_rows, dy_rows, shared_gate, shared_up, shared_down)

    shared_dx, grad_shared_gate, grad_shared_up, grad_shared_down = lax.map(shared_step, (x_tokens.reshape(GROUP_SIZE, TOK_DEV, MODEL_DIM), dy_tokens.reshape(GROUP_SIZE, TOK_DEV, MODEL_DIM)))
    grad_x = (routed_sum + shared_dx.reshape(tokens, MODEL_DIM)).astype(jnp.bfloat16)
    return (grad_x, grad_w_gate, grad_w_up, grad_w_down, grad_shared_gate, grad_shared_up, grad_shared_down)
```

```python
import jax
import jax.numpy as jnp
from jax import lax
from jax.experimental import pallas as pl
from jax.experimental.pallas import tpu as pltpu
from jax.sharding import PartitionSpec as P


F32, BF16 = jnp.float32, jnp.bfloat16
SLOTS = 64


def dot(a, b):
    return jnp.dot(a, b, preferred_element_type=F32)


def dot_nt(a, b):
    return lax.dot_general(a, b, (((1,), (1,)), ((), ())), preferred_element_type=F32)


def dot_tt(a, b):
    return lax.dot_general(a, b, (((0,), (1,)), ((), ())), preferred_element_type=F32)


def swiglu_parts(a, b, g):
    a, b = a.astype(F32), b.astype(F32)
    sigma = jax.nn.sigmoid(a)
    silu = a * sigma
    hidden = (silu * b).astype(BF16)
    grad_a = (g * b * sigma * (1.0 + a * (1.0 - sigma))).astype(BF16)
    grad_b = (g * silu).astype(BF16)
    return hidden, grad_a, grad_b


def shared_kernel(x, dy, w1, w3, w2, rt, dw1, dw3, dw2):
    at = dot(x[...], w1[...]).astype(BF16).astype(F32).T
    bt = dot(x[...], w3[...]).astype(BF16).astype(F32).T
    gt = dot_nt(w2[...], dy[...])
    ht, dat, dbt = swiglu_parts(at, bt, gt)
    dw1[0] = dot_tt(x[...], dat)
    dw3[0] = dot_tt(x[...], dbt)
    dw2[0] = dot(ht, dy[...])
    part = dot(w1[...], dat) + dot(w3[...], dbt)

    @pl.when(pl.program_id(0) == 0)
    def _():
        rt[...] = part

    @pl.when(pl.program_id(0) != 0)
    def _():
        rt[...] += part


def shared_call(x, dy, w1, w3, w2):
    toks, d = x.shape
    ff = w1.shape[1]
    fb = ff // 2
    return pl.pallas_call(
        shared_kernel,
        grid=(ff // fb,),
        in_specs=[pl.BlockSpec((toks, d), lambda i: (0, 0)), pl.BlockSpec((toks, d), lambda i: (0, 0)), pl.BlockSpec((d, fb), lambda i: (0, i)), pl.BlockSpec((d, fb), lambda i: (0, i)), pl.BlockSpec((fb, d), lambda i: (i, 0))],
        out_specs=[pl.BlockSpec((d, toks), lambda i: (0, 0)), pl.BlockSpec((1, d, fb), lambda i: (0, 0, i)), pl.BlockSpec((1, d, fb), lambda i: (0, 0, i)), pl.BlockSpec((1, fb, d), lambda i: (0, i, 0))],
        out_shape=[jax.ShapeDtypeStruct((d, toks), F32), jax.ShapeDtypeStruct((1, d, ff), F32), jax.ShapeDtypeStruct((1, d, ff), F32), jax.ShapeDtypeStruct((1, ff, d), F32)],
        compiler_params=pltpu.CompilerParams(vmem_limit_bytes=56 * 2**20),
        cost_estimate=pl.CostEstimate(flops=16 * toks * d * ff, bytes_accessed=20 * 2**20, transcendentals=0),
        name='shared',
    )(x, dy, w1, w3, w2)


def one_hot_rows(slot_row, toks):
    rows = lax.broadcasted_iota(jnp.int32, (SLOTS, toks), 0).astype(F32)
    return rows == slot_row


def dispatch(tabs, toks, first, pick, rows_out, gated):
    experts = rows_out.shape[0]
    n, d = toks[0].shape
    cols = 512
    for q in range(len(toks)):
        gates = []
        for e in range(experts):
            hit = one_hot_rows(tabs[q][0, pl.ds(first + e, 1), :], n)
            pick[q, e * SLOTS:(e + 1) * SLOTS, :] = jnp.where(hit, 1.0, 0.0).astype(BF16)
            if gated:
                gates.append(jnp.sum(jnp.where(hit, tabs[q][1, pl.ds(first + e, 1), :], 0.0), axis=1, keepdims=True))

        def chunk(c, carry):
            at = pl.ds(pl.multiple_of(c * cols, cols), cols)
            got = dot(pick[q], toks[q][:, at])
            for e in range(experts):
                part = got[e * SLOTS:(e + 1) * SLOTS]
                if gated:
                    part = part * gates[e]
                rows_out[e, q * SLOTS:(q + 1) * SLOTS, at] = part.astype(BF16)
            return carry

        lax.fori_loop(0, d // cols, chunk, 0)


def forward_kernel(first, t0, t1, t2, t3, x0, x1, x2, x3, w1, w3, at, bt, x_out, rows, pick, sem):
    e = pl.program_id(0)
    copy = pltpu.make_async_copy(rows, x_out, sem)

    @pl.when(e == 0)
    def _():
        dispatch((t0, t1, t2, t3), (x0, x1, x2, x3), first[0], pick, rows, False)
        copy.start()

    at[0] = dot(rows[e], w1[0]).T.astype(BF16)
    bt[0] = dot(rows[e], w3[0]).T.astype(BF16)

    @pl.when(e == pl.num_programs(0) - 1)
    def _():
        copy.wait()


def whole(shape):
    return pl.BlockSpec(shape, lambda e: (0,) * len(shape))


def block(shape):
    return pl.BlockSpec((1,) + shape, lambda e: (e,) + (0,) * len(shape))


def forward_call(first, tabs, toks, w1, w3):
    experts, d, ff = w1.shape
    n = toks[0].shape[0]
    rows = SLOTS * len(toks)
    return pl.pallas_call(
        forward_kernel,
        grid=(experts,),
        in_specs=[pl.BlockSpec(memory_space=pltpu.SMEM)] + [whole(t.shape) for t in tabs] + [whole(t.shape) for t in toks] + [block((d, ff)), block((d, ff))],
        out_specs=[block((ff, rows)), block((ff, rows)), pl.BlockSpec(memory_space=pl.ANY)],
        out_shape=[jax.ShapeDtypeStruct((experts, ff, rows), BF16)] * 2 + [jax.ShapeDtypeStruct((experts, rows, d), BF16)],
        scratch_shapes=[pltpu.VMEM((experts, rows, d), BF16), pltpu.VMEM((len(toks), experts * SLOTS, n), BF16), pltpu.SemaphoreType.DMA],
        compiler_params=pltpu.CompilerParams(vmem_limit_bytes=56 * 2**20),
        cost_estimate=pl.CostEstimate(flops=4 * experts * rows * d * ff, bytes_accessed=48 * 2**20, transcendentals=0),
        name='forward',
    )(first, *tabs, *toks, w1, w3)


def backward_kernel(first, t0, t1, t2, t3, y0, y1, y2, y3, at, bt, w1, w3, w2, dat_out, dbt_out, dw2, keep, send, rows, pick, ret, spread):
    e = pl.program_id(0)
    experts = pl.num_programs(0)

    @pl.when(e == 0)
    def _():
        dispatch((t0, t1, t2, t3), (y0, y1, y2, y3), first[0], pick, rows, True)

    z = rows[e]
    gt = dot_nt(w2[0], z)
    ht, dat, dbt = swiglu_parts(at[0], bt[0], gt)
    dat_out[0] = dat
    dbt_out[0] = dbt
    dw2[0] = dot(ht, z)
    back = (dot(w1[0], dat) + dot(w3[0], dbt)).astype(BF16)
    lanes = pl.ds(pl.multiple_of(e * 2 * SLOTS, 2 * SLOTS), 2 * SLOTS)
    for p in range(2):
        ret[p, :, lanes] = back[:, p * 2 * SLOTS:(p + 1) * 2 * SLOTS]

    @pl.when(e == experts - 1)
    def _():
        n = y0.shape[0]
        d = y0.shape[1]
        count = rows.shape[0]
        for p in range(2):
            spread[p] = jnp.zeros_like(spread[p])
            for k in range(count):
                for h in range(2):
                    spread[p, k * 2 * SLOTS + h * SLOTS:k * 2 * SLOTS + (h + 1) * SLOTS, h * n:(h + 1) * n] = pick[2 * p + h, k * SLOTS:(k + 1) * SLOTS, :]

            def chunk(c, carry):
                m = pl.ds(pl.multiple_of(c * 512, 512), 512)
                tot = dot(ret[p, m, :], spread[p])
                keep[p, m, :] = tot[:, :n]
                send[p, m, :] = tot[:, n:]
                return carry

            lax.fori_loop(0, d // 512, chunk, 0)


def backward_call(first, tabs, toks, at, bt, w1, w3, w2):
    experts, d, ff = w1.shape
    n = toks[0].shape[0]
    rows = SLOTS * len(toks)
    return pl.pallas_call(
        backward_kernel,
        grid=(experts,),
        in_specs=[pl.BlockSpec(memory_space=pltpu.SMEM)] + [whole(t.shape) for t in tabs] + [whole(t.shape) for t in toks] + [block((ff, rows)), block((ff, rows)), block((d, ff)), block((d, ff)), block((ff, d))],
        out_specs=[block((ff, rows)), block((ff, rows)), block((ff, d)), whole((2, d, n)), whole((2, d, n))],
        out_shape=[jax.ShapeDtypeStruct((experts, ff, rows), BF16)] * 2 + [jax.ShapeDtypeStruct((experts, ff, d), F32)] + [jax.ShapeDtypeStruct((2, d, n), F32)] * 2,
        scratch_shapes=[pltpu.VMEM((experts, rows, d), BF16), pltpu.VMEM((len(toks), experts * SLOTS, n), BF16), pltpu.VMEM((2, d, experts * 2 * SLOTS), BF16), pltpu.VMEM((2, experts * 2 * SLOTS, 2 * n), BF16)],
        compiler_params=pltpu.CompilerParams(vmem_limit_bytes=60 * 2**20),
        cost_estimate=pl.CostEstimate(flops=8 * experts * rows * d * ff, bytes_accessed=96 * 2**20, transcendentals=0),
        name='backward',
    )(first, *tabs, *toks, at, bt, w1, w3, w2)


def weight_kernel(x, dat, dbt, dw1, dw3):
    dw1[0] = dot_tt(x[0], dat[0])
    dw3[0] = dot_tt(x[0], dbt[0])


def weight_call(x, dat, dbt):
    experts, rows, d = x.shape
    ff = dat.shape[1]
    return pl.pallas_call(
        weight_kernel,
        grid=(experts,),
        in_specs=[block((rows, d)), block((ff, rows)), block((ff, rows))],
        out_specs=[block((d, ff)), block((d, ff))],
        out_shape=[jax.ShapeDtypeStruct((experts, d, ff), F32)] * 2,
        compiler_params=pltpu.CompilerParams(vmem_limit_bytes=56 * 2**20),
        cost_estimate=pl.CostEstimate(flops=4 * experts * rows * d * ff, bytes_accessed=80 * 2**20, transcendentals=0),
        name='weights',
    )(x, dat, dbt)


def final_kernel(own, back, shared, out):
    out[...] = (own[0] + back[...] + shared[...]).T.astype(BF16)


def final_call(own, back, shared):
    d, n = shared.shape
    db = 512
    return pl.pallas_call(
        final_kernel,
        grid=(d // db,),
        in_specs=[pl.BlockSpec((1, db, n), lambda i: (0, i, 0)), pl.BlockSpec((db, n), lambda i: (i, 0)), pl.BlockSpec((db, n), lambda i: (i, 0))],
        out_specs=pl.BlockSpec((n, db), lambda i: (0, i)),
        out_shape=jax.ShapeDtypeStruct((n, d), BF16),
        name='final',
    )(own, back, shared)


def solution(mesh):
    token_spec = P(('dp', 'ep'), None)
    expert_spec = P('ep', None, None)
    whole_spec = P(None, None)
    grad_spec = P(('dp', 'ep'), None, None)
    group = mesh.shape['ep']

    def swap(v, bit):
        return lax.ppermute(v, 'ep', [(i, i ^ bit) for i in range(group)])

    def local_backward(x, dy, expert_ids, gate_vals, slot_pos, w1, w3, w2, s1, s3, s2):
        local = w1.shape[0]
        num_experts = local * group
        ids_t, slots_t, gates_t = expert_ids.T, slot_pos.T, gate_vals.T
        chosen = ids_t[:, None, :] == jnp.arange(num_experts, dtype=jnp.int32)[None, :, None]
        slot_tab = jnp.max(jnp.where(chosen, slots_t[:, None, :], -1), axis=0).astype(F32)
        gate_tab = jnp.sum(jnp.where(chosen, gates_t[:, None, :], 0.0), axis=0)
        tab = jnp.stack([slot_tab, gate_tab])
        first = (lax.axis_index('ep') * local).astype(jnp.int32).reshape(1)

        x, dy, tab = lax.optimization_barrier((x, dy, tab))
        t1, t2, t3 = swap(tab, 1), swap(tab, 2), swap(tab, 3)
        x2 = swap(x, 2)
        x1 = swap(x, 1)
        dy2 = swap(dy, 2)
        dy1 = swap(dy, 1)
        x3 = swap(x2, 1)
        dy3 = swap(dy2, 1)
        shared_t, ds1, ds3, ds2 = shared_call(x, dy, s1, s3, s2)
        tabs = (tab, t1, t2, t3)
        at, bt, x_rows = forward_call(first, tabs, (x, x1, x2, x3), w1, w3)
        dat, dbt, dw2, keep, send = backward_call(first, tabs, (dy, dy1, dy2, dy3), at, bt, w1, w3, w2)
        chip = keep + swap(send, 1)
        back = swap(chip[1], 2)
        dw1, dw3 = weight_call(x_rows, dat, dbt)
        grad_x = final_call(chip, back, shared_t)
        return grad_x, dw1, dw3, dw2, ds1, ds3, ds2

    return jax.shard_map(local_backward, mesh=mesh, in_specs=(token_spec, token_spec, token_spec, token_spec, token_spec, expert_spec, expert_spec, expert_spec, whole_spec, whole_spec, whole_spec), out_specs=(token_spec, grad_spec, grad_spec, grad_spec, grad_spec, grad_spec, grad_spec), check_vma=False)
```

```python
import jax
import jax.numpy as jnp
from jax import lax
from jax.experimental import pallas as pl
from jax.experimental.pallas import tpu as pltpu
from jax.sharding import PartitionSpec as P


F32, BF16 = jnp.float32, jnp.bfloat16
MESH = pl.DeviceIdType.MESH
SLOTS = 64
COLS = 512
RING, RING2 = 12, 8


def dot(a, b):
    return jnp.dot(a, b, preferred_element_type=F32)


def dot_nt(a, b):
    return lax.dot_general(a, b, (((1,), (1,)), ((), ())), preferred_element_type=F32)


def dot_tt(a, b):
    return lax.dot_general(a, b, (((0,), (1,)), ((), ())), preferred_element_type=F32)


def span(index, size):
    return pl.ds(pl.multiple_of(index * size, size), size)


def swiglu_parts(a, b, g):
    a, b = a.astype(F32), b.astype(F32)
    sigma = jax.nn.sigmoid(a)
    silu = a * sigma
    hidden = (silu * b).astype(BF16)
    grad_a = (g * b * sigma * (1.0 + a * (1.0 - sigma))).astype(BF16)
    grad_b = (g * silu).astype(BF16)
    return hidden, grad_a, grad_b


def make_picks(tabs, first, pick, gate):
    experts = pick.shape[1] // SLOTS
    toks = pick.shape[2]
    rows = lax.broadcasted_iota(jnp.int32, (SLOTS, toks), 0).astype(F32)
    for q in range(pick.shape[0]):
        def one(e, carry):
            hit = rows == tabs[q][0, pl.ds(first + e, 1), :]
            pick[q, span(e, SLOTS), :] = jnp.where(hit, 1.0, 0.0).astype(BF16)
            gate[q, span(e, SLOTS), :] = jnp.sum(jnp.where(hit, tabs[q][1, pl.ds(first + e, 1), :], 0.0), axis=1, keepdims=True)
            return carry

        lax.fori_loop(0, experts, one, 0)


def put_rows(got, q, rows):
    for e in range(rows.shape[0]):
        rows[e, q * SLOTS:(q + 1) * SLOTS, :] = got[e * SLOTS:(e + 1) * SLOTS]


def exchange_kernel(x, dy, tab, w1, w3, w2, s1, s3, s2, dat_o, dbt_o, ht_o, xg_o, yg_o, tg_o, sdat_o, sdbt_o, sht_o, own, far,
                    xg, yg, tg, wring, w2ring, s1v, s3v, s2v, acc, gacc, act, rows, pick, gate, ret, spread, sbuf, rbuf,
                    near_s, near_r, far_s, far_r, hop_s, hop_r, tab_s, tab_r, sum_s, sum_r, wsem, w2sem, ssem, osem):
    me = lax.axis_index('ep')
    core = me % 2
    mate = me + 1 - 2 * core
    other = (me + 2) % 4
    diag = (mate + 2) % 4
    experts, d, _ = w1.shape
    n = x.shape[0]
    chunks = d // COLS
    pieces = chunks * experts
    first = me * experts

    barrier = pltpu.get_barrier_semaphore()
    for peer in (mate, other, diag):
        pl.semaphore_signal(barrier, inc=1, device_id={'ep': peer}, device_id_type=MESH)
    pl.semaphore_wait(barrier, 3)

    def remote(src, dst, send, recv, peer):
        return pltpu.make_async_remote_copy(src_ref=src, dst_ref=dst, send_sem=send, recv_sem=recv, device_id={'ep': peer}, device_id_type=MESH)

    own_of, got_of = (x, dy), (xg, yg)

    def far_copy(a, c):
        return remote(own_of[a].at[:, span(c, COLS)], got_of[a].at[0, :, span(c, COLS)], far_s.at[a, c], far_r.at[a, c], other)

    def near_copy(a):
        return remote(own_of[a], got_of[a].at[1], near_s.at[a], near_r.at[a], mate)

    def hop_copy(a, c):
        return remote(got_of[a].at[0, :, span(c, COLS)], got_of[a].at[2, :, span(c, COLS)], hop_s.at[a, c], hop_r.at[a, c], mate)

    def tab_copy(k):
        return remote(tab, tg.at[k], tab_s.at[k], tab_r.at[k], (other, mate, diag)[k])

    def sum_copy(m):
        return remote(sbuf.at[m], rbuf.at[m], sum_s.at[m], sum_r.at[m], mate)

    def w_copy(i, k):
        src = (w1, w3)[k].at[i % experts, span((i // experts) % chunks, COLS), :]
        return pltpu.make_async_copy(src, wring.at[i % RING, k], wsem.at[i % RING, k])

    def w2_copy(j):
        return pltpu.make_async_copy(w2.at[j % experts, :, span(j // experts, COLS)], w2ring.at[j % RING2], w2sem.at[j % RING2])

    def s_copy(k):
        return pltpu.make_async_copy((s1, s3, s2)[k], (s1v, s3v, s2v)[k], ssem.at[k])

    def each(count, body):
        def step(i, carry):
            body(i)
            return carry

        lax.fori_loop(0, count, step, 0)

    for k in range(3):
        tab_copy(k).start()
    each(chunks, lambda c: far_copy(0, c).start())
    near_copy(0).start()
    each(chunks, lambda c: far_copy(1, c).start())
    near_copy(1).start()
    for k in range(3):
        s_copy(k).start()

    def start_w(i):
        w_copy(i, 0).start()
        w_copy(i, 1).start()

    def wait_w(i):
        w_copy(i, 0).wait()
        w_copy(i, 1).wait()

    each(RING, start_w)
    each(RING2, lambda j: w2_copy(j).start())

    def clear(e):
        acc[0, e] = jnp.zeros_like(acc[0, e])
        acc[1, e] = jnp.zeros_like(acc[1, e])
        gacc[e] = jnp.zeros_like(gacc[e])

    each(experts, clear)

    for k in range(3):
        s_copy(k).wait()
    at = dot(x[...], s1v[...]).astype(BF16).astype(F32).T
    bt = dot(x[...], s3v[...]).astype(BF16).astype(F32).T
    sht, sdat, sdbt = swiglu_parts(at, bt, dot_nt(s2v[...], dy[...]))
    sht_o[...], sdat_o[...], sdbt_o[...] = sht, sdat, sdbt

    def shared_back(m):
        own[span(m, COLS), :] = dot(s1v[span(m, COLS), :], sdat_o[...]) + dot(s3v[span(m, COLS), :], sdbt_o[...])

    each(chunks, shared_back)

    for k in range(3):
        tab_copy(k).wait()
    tg_o[...] = tg[...]
    make_picks((tab, tg.at[0], tg.at[1], tg.at[2]), first, pick, gate)
    for h in range(2):
        spread[h] = jnp.zeros_like(spread[h])
        for e in range(experts):
            for j in range(2):
                spread[h, e * 2 * SLOTS + j * SLOTS:e * 2 * SLOTS + (j + 1) * SLOTS, j * n:(j + 1) * n] = pick[2 * h + j, e * SLOTS:(e + 1) * SLOTS, :]

    def gather_chunk(a, c):
        far_copy(a, c).wait()
        hop_copy(a, c).start()
        for q in range(4):
            if q == 3:
                hop_copy(a, c).wait()
            src = own_of[a] if q == 0 else got_of[a].at[q - 1]
            got = dot(pick[q], src[:, span(c, COLS)])
            if a == 1:
                got = got * gate[q]
            put_rows(got.astype(BF16), q, rows)

    near_copy(0).wait()

    def up_chunk(c):
        gather_chunk(0, c)

        def up(e):
            i = c * experts + e
            wait_w(i)
            acc[0, e] += dot(rows[e], wring[i % RING, 0])
            acc[1, e] += dot(rows[e], wring[i % RING, 1])
            start_w(i + RING)

        each(experts, up)

    each(chunks, up_chunk)
    pltpu.make_async_copy(xg, xg_o, osem.at[0]).start()

    def turn(e):
        act[0, e] = acc[0, e].T.astype(BF16)
        act[1, e] = acc[1, e].T.astype(BF16)

    each(experts, turn)
    near_copy(1).wait()

    def down_chunk(c):
        gather_chunk(1, c)

        def down(e):
            j = c * experts + e
            w2_copy(j).wait()
            gacc[e] += dot_nt(w2ring[j % RING2], rows[e])

            @pl.when(j + RING2 < pieces)
            def _():
                w2_copy(j + RING2).start()

        each(experts, down)

    each(chunks, down_chunk)
    pltpu.make_async_copy(yg, yg_o, osem.at[1]).start()

    def middle(e):
        ht, dat, dbt = swiglu_parts(act[0, e], act[1, e], gacc[e])
        act[0, e], act[1, e], act[2, e] = dat, dbt, ht

    each(experts, middle)
    for k in range(3):
        pltpu.make_async_copy(act.at[k], (dat_o, dbt_o, ht_o)[k], osem.at[2 + k]).start()

    def back_chunk(m):
        def back(e):
            i = pieces + m * experts + e
            wait_w(i)
            part = (dot(wring[i % RING, 0], act[0, e]) + dot(wring[i % RING, 1], act[1, e])).astype(BF16)
            for h in range(2):
                ret[h, :, span(e, 2 * SLOTS)] = part[:, h * 2 * SLOTS:(h + 1) * 2 * SLOTS]

            @pl.when(i + RING < 2 * pieces)
            def _():
                start_w(i + RING)

        each(experts, back)
        sbuf[m] = dot(ret[1], spread[1])
        sum_copy(m).start()
        keep = dot(ret[0], spread[0])
        own[span(m, COLS), :] += keep[:, :n]
        far[span(m, COLS), :] = keep[:, n:]

    each(chunks, back_chunk)

    def add_mate(m):
        sum_copy(m).wait()
        own[span(m, COLS), :] += rbuf[m, :, :n]
        far[span(m, COLS), :] += rbuf[m, :, n:]

    each(chunks, add_mate)
    pltpu.make_async_copy(xg, xg_o, osem.at[0]).wait()
    pltpu.make_async_copy(yg, yg_o, osem.at[1]).wait()
    for k in range(3):
        pltpu.make_async_copy(act.at[k], (dat_o, dbt_o, ht_o)[k], osem.at[2 + k]).wait()


def exchange_call(x, dy, tab, w1, w3, w2, s1, s3, s2):
    experts, d, ff = w1.shape
    n = x.shape[0]
    chunks, rows = d // COLS, 4 * SLOTS
    vmem, hbm = pl.BlockSpec(memory_space=pltpu.VMEM), pl.BlockSpec(memory_space=pl.ANY)
    dma = pltpu.SemaphoreType.DMA
    return pl.pallas_call(
        exchange_kernel,
        in_specs=[vmem] * 3 + [hbm] * 6,
        out_specs=[hbm] * 5 + [vmem] * 6,
        out_shape=[jax.ShapeDtypeStruct((experts, ff, rows), BF16)] * 3 + [jax.ShapeDtypeStruct((3, n, d), BF16)] * 2 + [jax.ShapeDtypeStruct((3,) + tab.shape, F32)] + [jax.ShapeDtypeStruct((ff, n), BF16)] * 3 + [jax.ShapeDtypeStruct((d, n), F32)] * 2,
        scratch_shapes=[
            pltpu.VMEM((3, n, d), BF16), pltpu.VMEM((3, n, d), BF16), pltpu.VMEM((3,) + tab.shape, F32),
            pltpu.VMEM((RING, 2, COLS, ff), BF16), pltpu.VMEM((RING2, ff, COLS), BF16),
            pltpu.VMEM((d, ff), BF16), pltpu.VMEM((d, ff), BF16), pltpu.VMEM((ff, d), BF16),
            pltpu.VMEM((2, experts, rows, ff), F32), pltpu.VMEM((experts, ff, rows), F32), pltpu.VMEM((3, experts, ff, rows), BF16),
            pltpu.VMEM((experts, rows, COLS), BF16), pltpu.VMEM((4, experts * SLOTS, n), BF16), pltpu.VMEM((4, experts * SLOTS, 1), F32),
            pltpu.VMEM((2, COLS, experts * 2 * SLOTS), BF16), pltpu.VMEM((2, experts * 2 * SLOTS, 2 * n), BF16),
            pltpu.VMEM((chunks, COLS, 2 * n), F32), pltpu.VMEM((chunks, COLS, 2 * n), F32),
            dma((2,)), dma((2,)), dma((2, chunks)), dma((2, chunks)), dma((2, chunks)), dma((2, chunks)), dma((3,)), dma((3,)), dma((chunks,)), dma((chunks,)),
            dma((RING, 2)), dma((RING2,)), dma((3,)), dma((5,)),
        ],
        compiler_params=pltpu.CompilerParams(collective_id=0, has_side_effects=True, vmem_limit_bytes=67043328),
        cost_estimate=pl.CostEstimate(flops=12 * experts * rows * d * ff, bytes_accessed=96 * 2**20, transcendentals=0),
        name='exchange',
    )(x, dy, tab, w1, w3, w2, s1, s3, s2)


def weight_kernel(first, tab, tg, x, dy, xg, yg, dat, dbt, ht, sdat, sdbt, sht, dw1, dw3, dw2, ds1, ds3, ds2, rows, pick, gate):
    c, e = pl.program_id(0), pl.program_id(1)

    @pl.when((c == 0) & (e == 0))
    def _():
        make_picks((tab, tg.at[0], tg.at[1], tg.at[2]), first[0], pick, gate)

    @pl.when(e == 0)
    def _():
        for q in range(4):
            src_x, src_y = (x, dy) if q == 0 else (xg.at[q - 1], yg.at[q - 1])
            put_rows(dot(pick[q], src_x[:, span(c, COLS)]).astype(BF16), q, rows.at[0])
            put_rows((dot(pick[q], src_y[:, span(c, COLS)]) * gate[q]).astype(BF16), q, rows.at[1])
        ds1[0] = dot_tt(x[:, span(c, COLS)], sdat[...])
        ds3[0] = dot_tt(x[:, span(c, COLS)], sdbt[...])
        ds2[0] = dot(sht[...], dy[:, span(c, COLS)])

    dw1[0] = dot_tt(rows[0, e], dat[e])
    dw3[0] = dot_tt(rows[0, e], dbt[e])
    dw2[0] = dot(ht[e], rows[1, e])


def weight_call(first, tab, tg, x, dy, xg, yg, dat, dbt, ht, sdat, sdbt, sht):
    experts, ff, rows = dat.shape
    n, d = x.shape
    vmem = pl.BlockSpec(memory_space=pltpu.VMEM)
    tall = pl.BlockSpec((1, COLS, ff), lambda c, e: (e, c, 0))
    wide = pl.BlockSpec((1, ff, COLS), lambda c, e: (e, 0, c))
    tall_shared = pl.BlockSpec((1, COLS, ff), lambda c, e: (0, c, 0))
    wide_shared = pl.BlockSpec((1, ff, COLS), lambda c, e: (0, 0, c))
    return pl.pallas_call(
        weight_kernel,
        grid=(d // COLS, experts),
        in_specs=[pl.BlockSpec(memory_space=pltpu.SMEM)] + [vmem] * 12,
        out_specs=[tall, tall, wide, tall_shared, tall_shared, wide_shared],
        out_shape=[jax.ShapeDtypeStruct((experts, d, ff), F32)] * 2 + [jax.ShapeDtypeStruct((experts, ff, d), F32)] + [jax.ShapeDtypeStruct((1, d, ff), F32)] * 2 + [jax.ShapeDtypeStruct((1, ff, d), F32)],
        scratch_shapes=[pltpu.VMEM((2, experts, rows, COLS), BF16), pltpu.VMEM((4, experts * SLOTS, n), BF16), pltpu.VMEM((4, experts * SLOTS, 1), F32)],
        compiler_params=pltpu.CompilerParams(vmem_limit_bytes=56 * 2**20),
        cost_estimate=pl.CostEstimate(flops=6 * experts * rows * d * ff, bytes_accessed=124 * 2**20, transcendentals=0),
        name='weights',
    )(first, tab, tg, x, dy, xg, yg, dat, dbt, ht, sdat, sdbt, sht)


def final_kernel(own, back, out):
    out[...] = (own[...] + back[...]).T.astype(BF16)


def final_call(own, back):
    d, n = own.shape
    vmem = pl.BlockSpec(memory_space=pltpu.VMEM)
    return pl.pallas_call(
        final_kernel,
        in_specs=[vmem, vmem],
        out_specs=vmem,
        out_shape=jax.ShapeDtypeStruct((n, d), BF16),
        name='final',
    )(own, back)


def solution(mesh):
    token_spec = P(('dp', 'ep'), None)
    expert_spec = P('ep', None, None)
    whole_spec = P(None, None)
    grad_spec = P(('dp', 'ep'), None, None)
    group = mesh.shape['ep']

    def local_backward(x, dy, expert_ids, gate_vals, slot_pos, w1, w3, w2, s1, s3, s2):
        local = w1.shape[0]
        num_experts = local * group
        ids_t, slots_t, gates_t = expert_ids.T, slot_pos.T, gate_vals.T
        chosen = ids_t[:, None, :] == jnp.arange(num_experts, dtype=jnp.int32)[None, :, None]
        slot_tab = jnp.max(jnp.where(chosen, slots_t[:, None, :], -1), axis=0).astype(F32)
        gate_tab = jnp.sum(jnp.where(chosen, gates_t[:, None, :], 0.0), axis=0)
        tab = jnp.stack([slot_tab, gate_tab])
        first = (lax.axis_index('ep') * local).astype(jnp.int32).reshape(1)

        dat, dbt, ht, xg, yg, tg, sdat, sdbt, sht, own, far = exchange_call(x, dy, tab, w1, w3, w2, s1, s3, s2)
        back = lax.ppermute(far, 'ep', [(i, i ^ 2) for i in range(group)])
        dw1, dw3, dw2, ds1, ds3, ds2 = weight_call(first, tab, tg, x, dy, xg, yg, dat, dbt, ht, sdat, sdbt, sht)
        grad_x = final_call(own, back)
        return grad_x, dw1, dw3, dw2, ds1, ds3, ds2

    return jax.shard_map(local_backward, mesh=mesh, in_specs=(token_spec, token_spec, token_spec, token_spec, token_spec, expert_spec, expert_spec, expert_spec, whole_spec, whole_spec, whole_spec), out_specs=(token_spec, grad_spec, grad_spec, grad_spec, grad_spec, grad_spec, grad_spec), check_vma=False)
```

```python
import jax
import jax.numpy as jnp
from jax import lax
from jax.experimental import pallas as pl
from jax.experimental.pallas import tpu as pltpu
from jax.sharding import PartitionSpec as P


F32, BF16 = jnp.float32, jnp.bfloat16
MESH = pl.DeviceIdType.MESH
SLOTS = 64
COLS = 512
RING, RING2 = 12, 8
UP, DOWN, BACK = 4, 4, 4


def dot(a, b):
    return jnp.dot(a, b, preferred_element_type=F32)


def dot_nt(a, b):
    return lax.dot_general(a, b, (((1,), (1,)), ((), ())), preferred_element_type=F32)


def dot_tt(a, b):
    return lax.dot_general(a, b, (((0,), (1,)), ((), ())), preferred_element_type=F32)


def span(index, size):
    return pl.ds(pl.multiple_of(index * size, size), size)


def swiglu_parts(a, b, g):
    a, b = a.astype(F32), b.astype(F32)
    sigma = jax.nn.sigmoid(a)
    silu = a * sigma
    hidden = (silu * b).astype(BF16)
    grad_a = (g * b * sigma * (1.0 + a * (1.0 - sigma))).astype(BF16)
    grad_b = (g * silu).astype(BF16)
    return hidden, grad_a, grad_b


def put_rows(got, q, rows):
    for e in range(rows.shape[0]):
        rows[e, span(q, SLOTS), :] = got[e * SLOTS:(e + 1) * SLOTS]


def exchange_kernel(x, dy, ids, slots, gates, w1, w3, w2, s1, s3, s2, dat_o, dbt_o, ht_o, tok_o, pick_o, gate_o, sdat_o, sdbt_o, sht_o, own, far,
                    xg, yg, idg, slotg, gateg, wring, w2ring, s1v, s3v, s2v, acc, gacc, act, rows, pick, gate, ret, spread, sbuf, rbuf,
                    near_s, near_r, far_s, far_r, hop_s, hop_r, tab_s, tab_r, sum_s, sum_r, wsem, w2sem, ssem, osem):
    me = lax.axis_index('ep')
    core = me % 2
    mate = me + 1 - 2 * core
    other = (me + 2) % 4
    diag = (mate + 2) % 4
    experts, d, ff = w1.shape
    n = x.shape[0]
    chunks = d // COLS
    pieces = chunks * experts

    barrier = pltpu.get_barrier_semaphore()
    for peer in (mate, other, diag):
        pl.semaphore_signal(barrier, inc=1, device_id={'ep': peer}, device_id_type=MESH)

    def w_copy(i, k):
        src = (w1, w3)[k].at[i % experts, span((i // experts) % chunks, COLS), :]
        return pltpu.make_async_copy(src, wring.at[i % RING, k], wsem.at[i % RING, k])

    def w2_copy(j):
        return pltpu.make_async_copy(w2.at[j % experts, :, span(j // experts, COLS)], w2ring.at[j % RING2], w2sem.at[j % RING2])

    def s_copy(k):
        return pltpu.make_async_copy((s1, s3, s2)[k], (s1v, s3v, s2v)[k], ssem.at[k])

    def each(count, body):
        def step(i, carry):
            body(i)
            return carry

        lax.fori_loop(0, count, step, 0)

    def start_w(i):
        w_copy(i, 0).start()
        w_copy(i, 1).start()

    def wait_w(i):
        w_copy(i, 0).wait()
        w_copy(i, 1).wait()

    for k in range(3):
        s_copy(k).start()
    each(RING, start_w)
    each(RING2, lambda j: w2_copy(j).start())

    def remote(src, dst, send, recv, peer):
        return pltpu.make_async_remote_copy(src_ref=src, dst_ref=dst, send_sem=send, recv_sem=recv, device_id={'ep': peer}, device_id_type=MESH)

    own_of, got_of = (x, dy), (xg, yg)

    def far_copy(a, c):
        return remote(own_of[a].at[:, span(c, COLS)], got_of[a].at[0, :, span(c, COLS)], far_s.at[a, c], far_r.at[a, c], other)

    def near_copy(a):
        return remote(own_of[a], got_of[a].at[1], near_s.at[a], near_r.at[a], mate)

    def hop_copy(a, c):
        return remote(got_of[a].at[0, :, span(c, COLS)], got_of[a].at[2, :, span(c, COLS)], hop_s.at[a, c], hop_r.at[a, c], mate)

    def tab_copy(t, k):
        return remote((ids, slots, gates)[t], (idg, slotg, gateg)[t].at[k], tab_s.at[t, k], tab_r.at[t, k], (other, mate, diag)[k])

    def sum_copy(m):
        return remote(sbuf.at[m], rbuf.at[m], sum_s.at[m], sum_r.at[m], mate)

    pl.semaphore_wait(barrier, 3)
    for t in range(3):
        for k in range(3):
            tab_copy(t, k).start()
    each(chunks, lambda c: far_copy(0, c).start())
    near_copy(0).start()
    each(chunks, lambda c: far_copy(1, c).start())
    near_copy(1).start()

    def clear(e):
        acc[0, e] = jnp.zeros_like(acc[0, e])
        acc[1, e] = jnp.zeros_like(acc[1, e])
        gacc[e] = jnp.zeros_like(gacc[e])

    each(experts, clear)
    for k in range(3):
        s_copy(k).wait()
    at = dot(x[...], s1v[...]).astype(BF16).astype(F32).T
    bt = dot(x[...], s3v[...]).astype(BF16).astype(F32).T
    sht, sdat, sdbt = swiglu_parts(at, bt, dot_nt(s2v[...], dy[...]))
    sht_o[...], sdat_o[...], sdbt_o[...] = sht, sdat, sdbt

    def shared_back(m):
        own[span(m, COLS), :] = dot(s1v[span(m, COLS), :], sdat_o[...]) + dot(s3v[span(m, COLS), :], sdbt_o[...])

    each(chunks, shared_back)

    for t in range(3):
        for k in range(3):
            tab_copy(t, k).wait()
    mine = me * experts + lax.broadcasted_iota(jnp.int32, (experts, n), 0)
    rank = lax.broadcasted_iota(jnp.int32, (SLOTS, n), 0)
    for q in range(4):
        idq, slotq, gateq = (ids, slots, gates) if q == 0 else (idg.at[q - 1], slotg.at[q - 1], gateg.at[q - 1])
        slot = jnp.full((experts, n), -1, jnp.int32)
        weight = jnp.zeros((experts, n), F32)
        for j in range(ids.shape[0]):
            hit = mine == idq[j:j + 1, :]
            slot = jnp.where(hit, slotq[j:j + 1, :], slot)
            weight = jnp.where(hit, gateq[j:j + 1, :], weight)
        for e in range(experts):
            hit = rank == slot[e:e + 1, :]
            pick[q, e * SLOTS:(e + 1) * SLOTS, :] = jnp.where(hit, 1.0, 0.0).astype(BF16)
            gate[q, e * SLOTS:(e + 1) * SLOTS, :] = jnp.sum(jnp.where(hit, weight[e:e + 1, :], 0.0), axis=1, keepdims=True)
    for h in range(2):
        spread[h] = jnp.zeros_like(spread[h])
        for e in range(experts):
            for j in range(2):
                spread[h, e * 2 * SLOTS + j * SLOTS:e * 2 * SLOTS + (j + 1) * SLOTS, j * n:(j + 1) * n] = pick[2 * h + j, e * SLOTS:(e + 1) * SLOTS, :]

    def expect(a, c):
        far_copy(a, c).wait()
        hop_copy(a, c).start()

    def gather_chunk(a, c):
        hop_copy(a, c).wait()
        for q in range(4):
            src = own_of[a] if q == 0 else got_of[a].at[q - 1]
            got = dot(pick[q], src[:, span(c, COLS)])
            if a == 1:
                got = got * gate[q]
            put_rows(got.astype(BF16), q, rows)

    expect(0, 0)
    near_copy(0).wait()

    def up_chunk(c):
        gather_chunk(0, c)

        def up(p):
            base = c * experts + UP * p
            for k in range(UP):
                wait_w(base + k)
            for k in range(UP):
                e, i = UP * p + k, base + k
                acc[0, e] += dot(rows[e], wring[i % RING, 0])
                acc[1, e] += dot(rows[e], wring[i % RING, 1])
            for k in range(UP):
                start_w(base + k + RING)

        each(experts // UP // 2, up)

        @pl.when(c + 1 < chunks)
        def _():
            expect(0, c + 1)

        @pl.when(c + 1 == chunks)
        def _():
            expect(1, 0)

        each(experts // UP // 2, lambda p: up(p + experts // UP // 2))

    each(chunks, up_chunk)
    near_copy(1).wait()

    def down_chunk(c):
        gather_chunk(1, c)

        def down(p):
            base = c * experts + DOWN * p
            for k in range(DOWN):
                w2_copy(base + k).wait()
            parts = [dot_nt(w2ring[(base + k) % RING2], rows[DOWN * p + k]) for k in range(DOWN)]
            for k in range(DOWN):
                gacc[DOWN * p + k] += parts[k]

            @pl.when(base + RING2 < pieces)
            def _():
                for k in range(DOWN):
                    w2_copy(base + k + RING2).start()

        down(0)

        @pl.when(c + 1 < chunks)
        def _():
            expect(1, c + 1)

        each(experts // DOWN - 1, lambda p: down(p + 1))

    each(chunks, down_chunk)
    outs = [pltpu.make_async_copy(x, tok_o.at[0, 0], osem.at[0]), pltpu.make_async_copy(xg, tok_o.at[0, 1:4], osem.at[1]),
            pltpu.make_async_copy(dy, tok_o.at[1, 0], osem.at[2]), pltpu.make_async_copy(yg, tok_o.at[1, 1:4], osem.at[3]),
            pltpu.make_async_copy(pick, pick_o, osem.at[4]), pltpu.make_async_copy(gate, gate_o, osem.at[5])]
    for copy in outs:
        copy.start()

    half = ff // 2

    def middle(i):
        e, part = i // 2, span(i % 2, half)
        a, b = acc[0, e, :, part].T.astype(BF16), acc[1, e, :, part].T.astype(BF16)
        act[2, e, part, :], act[0, e, part, :], act[1, e, part, :] = swiglu_parts(a, b, gacc[e, part, :])

    each(2 * experts, middle)
    outs += [pltpu.make_async_copy(act.at[k], (dat_o, dbt_o, ht_o)[k], osem.at[6 + k]) for k in range(3)]
    for copy in outs[6:]:
        copy.start()

    def back_chunk(m):
        def back(p):
            base = pieces + m * experts + BACK * p
            for k in range(BACK):
                wait_w(base + k)
            for k in range(BACK):
                e, i = BACK * p + k, base + k
                part = (dot(wring[i % RING, 0], act[0, e]) + dot(wring[i % RING, 1], act[1, e])).astype(BF16)
                for h in range(2):
                    ret[h, :, span(e, 2 * SLOTS)] = part[:, h * 2 * SLOTS:(h + 1) * 2 * SLOTS]

            @pl.when(base + RING < 2 * pieces)
            def _():
                for k in range(BACK):
                    start_w(base + k + RING)

        each(experts // BACK, back)
        give = dot(ret[1], spread[1])
        keep = dot(ret[0], spread[0])
        sbuf[m] = give
        own[span(m, COLS), :] += keep[:, :n]
        far[span(m, COLS), :] = keep[:, n:]
        sum_copy(m).start()

    each(chunks, back_chunk)

    def add_mate(m):
        sum_copy(m).wait()
        own[span(m, COLS), :] += rbuf[m, :, :n]
        far[span(m, COLS), :] += rbuf[m, :, n:]

    each(chunks, add_mate)
    for copy in outs:
        copy.wait()


def exchange_call(x, dy, ids, slots, gates, w1, w3, w2, s1, s3, s2):
    experts, d, ff = w1.shape
    n = x.shape[0]
    chunks, rows = d // COLS, 4 * SLOTS
    vmem, hbm = pl.BlockSpec(memory_space=pltpu.VMEM), pl.BlockSpec(memory_space=pl.ANY)
    dma = pltpu.SemaphoreType.DMA
    return pl.pallas_call(
        exchange_kernel,
        in_specs=[vmem] * 5 + [hbm] * 6,
        out_specs=[hbm] * 6 + [vmem] * 5,
        out_shape=[jax.ShapeDtypeStruct((experts, ff, rows), BF16)] * 3 + [jax.ShapeDtypeStruct((2, 4, n, d), BF16), jax.ShapeDtypeStruct((4, experts * SLOTS, n), BF16), jax.ShapeDtypeStruct((4, experts * SLOTS, 1), F32)] + [jax.ShapeDtypeStruct((ff, n), BF16)] * 3 + [jax.ShapeDtypeStruct((d, n), F32)] * 2,
        scratch_shapes=[
            pltpu.VMEM((3, n, d), BF16), pltpu.VMEM((3, n, d), BF16), pltpu.VMEM((3,) + ids.shape, jnp.int32), pltpu.VMEM((3,) + ids.shape, jnp.int32), pltpu.VMEM((3,) + ids.shape, F32),
            pltpu.VMEM((RING, 2, COLS, ff), BF16), pltpu.VMEM((RING2, ff, COLS), BF16),
            pltpu.VMEM((d, ff), BF16), pltpu.VMEM((d, ff), BF16), pltpu.VMEM((ff, d), BF16),
            pltpu.VMEM((2, experts, rows, ff), F32), pltpu.VMEM((experts, ff, rows), F32), pltpu.VMEM((3, experts, ff, rows), BF16),
            pltpu.VMEM((experts, rows, COLS), BF16), pltpu.VMEM((4, experts * SLOTS, n), BF16), pltpu.VMEM((4, experts * SLOTS, 1), F32),
            pltpu.VMEM((2, COLS, experts * 2 * SLOTS), BF16), pltpu.VMEM((2, experts * 2 * SLOTS, 2 * n), BF16),
            pltpu.VMEM((chunks, COLS, 2 * n), F32), pltpu.VMEM((chunks, COLS, 2 * n), F32),
            dma((2,)), dma((2,)), dma((2, chunks)), dma((2, chunks)), dma((2, chunks)), dma((2, chunks)), dma((3, 3)), dma((3, 3)), dma((chunks,)), dma((chunks,)),
            dma((RING, 2)), dma((RING2,)), dma((3,)), dma((9,)),
        ],
        compiler_params=pltpu.CompilerParams(collective_id=0, has_side_effects=True, vmem_limit_bytes=67043328),
        cost_estimate=pl.CostEstimate(flops=12 * experts * rows * d * ff, bytes_accessed=96 * 2**20, transcendentals=0),
        name='exchange',
    )(x, dy, ids, slots, gates, w1, w3, w2, s1, s3, s2)


def weight_kernel(tok, pick, gate, dat_h, dbt_h, ht_h, sdat, sdbt, sht, dw1, dw3, dw2, ds1, ds3, ds2, rows, act, sem):
    c, e = pl.program_id(0), pl.program_id(1)
    chunks, experts = pl.num_programs(0), rows.shape[2]
    now, later = c % 2, (c + 1) % 2

    def act_copy(k, i):
        return pltpu.make_async_copy((dat_h, dbt_h, ht_h)[k].at[i], act.at[k, i], sem.at[k, i])

    def put(a, q, col, buf):
        got = dot(pick[q], tok[a, q, :, span(col, COLS)])
        if isinstance(a, int):
            got = got * gate[q] if a == 1 else got
        else:
            got = got * jnp.where(a == 1, gate[q], 1.0)
        put_rows(got.astype(BF16), q, rows.at[buf, a])

    @pl.when((c == 0) & (e == 0))
    def _():
        for i in range(experts):
            for k in range(3):
                act_copy(k, i).start()
        for q in range(4):
            put(0, q, 0, 0)
            put(1, q, 0, 0)

    @pl.when(c == 0)
    def _():
        for k in range(3):
            act_copy(k, e).wait()

    @pl.when(e == 0)
    def _():
        ds1[0] = dot_tt(tok[0, 0, :, span(c, COLS)], sdat[...])
        ds3[0] = dot_tt(tok[0, 0, :, span(c, COLS)], sdbt[...])
        ds2[0] = dot(sht[...], tok[1, 0, :, span(c, COLS)])

    @pl.when(c + 1 < chunks)
    def _():
        put(e % 2, e // 2, c + 1, later)

    xt = rows[now, 0, e].T
    dw1[0] = dot_nt(xt, act[0, e])
    dw3[0] = dot_nt(xt, act[1, e])
    dw2[0] = dot(act[2, e], rows[now, 1, e])


def weight_call(tok, pick, gate, dat, dbt, ht, sdat, sdbt, sht):
    experts, ff, rows = dat.shape
    _, d = tok.shape[2:]
    vmem, hbm = pl.BlockSpec(memory_space=pltpu.VMEM), pl.BlockSpec(memory_space=pl.ANY)
    tall = pl.BlockSpec((1, COLS, ff), lambda c, e: (e, c, 0))
    wide = pl.BlockSpec((1, ff, COLS), lambda c, e: (e, 0, c))
    tall_shared = pl.BlockSpec((1, COLS, ff), lambda c, e: (0, c, 0))
    wide_shared = pl.BlockSpec((1, ff, COLS), lambda c, e: (0, 0, c))
    return pl.pallas_call(
        weight_kernel,
        grid=(d // COLS, experts),
        in_specs=[vmem] * 3 + [hbm] * 3 + [vmem] * 3,
        out_specs=[tall, tall, wide, tall_shared, tall_shared, wide_shared],
        out_shape=[jax.ShapeDtypeStruct((experts, d, ff), F32)] * 2 + [jax.ShapeDtypeStruct((experts, ff, d), F32)] + [jax.ShapeDtypeStruct((1, d, ff), F32)] * 2 + [jax.ShapeDtypeStruct((1, ff, d), F32)],
        scratch_shapes=[pltpu.VMEM((2, 2, experts, rows, COLS), BF16), pltpu.VMEM((3, experts, ff, rows), BF16), pltpu.SemaphoreType.DMA((3, experts))],
        compiler_params=pltpu.CompilerParams(vmem_limit_bytes=56 * 2**20),
        cost_estimate=pl.CostEstimate(flops=6 * experts * rows * d * ff, bytes_accessed=124 * 2**20, transcendentals=0),
        name='weights',
    )(tok, pick, gate, dat, dbt, ht, sdat, sdbt, sht)


def final_kernel(own, back, out):
    out[...] = (own[...] + back[...]).T.astype(BF16)


def final_call(own, back):
    d, n = own.shape
    vmem = pl.BlockSpec(memory_space=pltpu.VMEM)
    return pl.pallas_call(
        final_kernel,
        in_specs=[vmem, vmem],
        out_specs=vmem,
        out_shape=jax.ShapeDtypeStruct((n, d), BF16),
        name='final',
    )(own, back)


def solution(mesh):
    token_spec = P(('dp', 'ep'), None)
    expert_spec = P('ep', None, None)
    whole_spec = P(None, None)
    grad_spec = P(('dp', 'ep'), None, None)
    group = mesh.shape['ep']

    def local_backward(x, dy, expert_ids, gate_vals, slot_pos, w1, w3, w2, s1, s3, s2):
        dat, dbt, ht, tok, pick, gate, sdat, sdbt, sht, own, far = exchange_call(x, dy, expert_ids.T, slot_pos.T, gate_vals.T, w1, w3, w2, s1, s3, s2)
        back = lax.ppermute(far, 'ep', [(i, i ^ 2) for i in range(group)])
        dw1, dw3, dw2, ds1, ds3, ds2 = weight_call(tok, pick, gate, dat, dbt, ht, sdat, sdbt, sht)
        grad_x = final_call(own, back)
        return grad_x, dw1, dw3, dw2, ds1, ds3, ds2

    return jax.shard_map(local_backward, mesh=mesh, in_specs=(token_spec, token_spec, token_spec, token_spec, token_spec, expert_spec, expert_spec, expert_spec, whole_spec, whole_spec, whole_spec), out_specs=(token_spec, grad_spec, grad_spec, grad_spec, grad_spec, grad_spec, grad_spec), check_vma=False)
```

```python
import jax
import jax.numpy as jnp
from jax import lax
from jax.experimental import pallas as pl
from jax.experimental.pallas import tpu as pltpu
from jax.sharding import PartitionSpec as P


F32, BF16 = jnp.float32, jnp.bfloat16
MESH = pl.DeviceIdType.MESH
SLOTS = 64
COLS = 512
RING, RING2 = 12, 8
OUTS = 5
UP, DOWN, BACK = 4, 4, 4


def dot(a, b):
    return jnp.dot(a, b, preferred_element_type=F32)


def dot_nt(a, b):
    return lax.dot_general(a, b, (((1,), (1,)), ((), ())), preferred_element_type=F32)


def span(index, size):
    return pl.ds(pl.multiple_of(index * size, size), size)


def swiglu_parts(a, b, g):
    a, b = a.astype(F32), b.astype(F32)
    sigma = 0.5 * jnp.tanh(0.5 * a) + 0.5
    silu = a * sigma
    hidden = (silu * b).astype(BF16)
    grad_a = (g * b * (sigma + silu * (1.0 - sigma))).astype(BF16)
    grad_b = (g * silu).astype(BF16)
    return hidden, grad_a, grad_b


def put_rows(got, q, rows):
    for e in range(rows.shape[0]):
        rows[e, span(q, SLOTS), :] = got[e * SLOTS:(e + 1) * SLOTS]


def exchange_kernel(x, dy, ids, slots, gates, w1, w3, w2, s1, s3, s2, dat_o, dbt_o, ht_o, tok_o, pick_o, gate_o, sdat_o, sdbt_o, sht_o, own, far,
                    xg, yg, idg, slotg, gateg, wring, w2ring, s1v, s3v, s2v, acc, gacc, act, rows, pick, gate, ret, spread, sbuf, rbuf,
                    near_s, near_r, far_s, far_r, hop_s, hop_r, tab_s, tab_r, sum_s, sum_r, wsem, w2sem, ssem, osem):
    me = lax.axis_index('ep')
    core = me % 2
    mate = me + 1 - 2 * core
    other = (me + 2) % 4
    diag = (mate + 2) % 4
    experts, d, ff = w1.shape
    n = x.shape[0]
    chunks = d // COLS
    pieces = chunks * experts

    barrier = pltpu.get_barrier_semaphore()
    for peer in (mate, other, diag):
        pl.semaphore_signal(barrier, inc=1, device_id={'ep': peer}, device_id_type=MESH)

    def w_copy(i, k):
        src = (w1, w3)[k].at[i % experts, span((i // experts) % chunks, COLS), :]
        return pltpu.make_async_copy(src, wring.at[i % RING, k], wsem.at[i % RING, k])

    def w2_copy(j):
        return pltpu.make_async_copy(w2.at[j % experts, :, span(j // experts, COLS)], w2ring.at[j % RING2], w2sem.at[j % RING2])

    def s_copy(k):
        return pltpu.make_async_copy((s1, s3, s2)[k], (s1v, s3v, s2v)[k], ssem.at[k])

    def each(count, body):
        def step(i, carry):
            body(i)
            return carry

        lax.fori_loop(0, count, step, 0)

    def start_w(i):
        w_copy(i, 0).start()
        w_copy(i, 1).start()

    def wait_w(i):
        w_copy(i, 0).wait()
        w_copy(i, 1).wait()

    for k in range(3):
        s_copy(k).start()
    each(RING, start_w)
    each(RING2, lambda j: w2_copy(j).start())

    def remote(src, dst, send, recv, peer):
        return pltpu.make_async_remote_copy(src_ref=src, dst_ref=dst, send_sem=send, recv_sem=recv, device_id={'ep': peer}, device_id_type=MESH)

    own_of, got_of = (x, dy), (xg, yg)

    def far_copy(a, c):
        return remote(own_of[a].at[:, span(c, COLS)], got_of[a].at[0, :, span(c, COLS)], far_s.at[a, c], far_r.at[a, c], other)

    def near_copy(a):
        return remote(own_of[a], got_of[a].at[1], near_s.at[a], near_r.at[a], mate)

    def hop_copy(a, c):
        return remote(got_of[a].at[0, :, span(c, COLS)], got_of[a].at[2, :, span(c, COLS)], hop_s.at[a, c], hop_r.at[a, c], mate)

    def tab_copy(t, k):
        return remote((ids, slots, gates)[t], (idg, slotg, gateg)[t].at[k], tab_s.at[t, k], tab_r.at[t, k], (other, mate, diag)[k])

    def sum_copy(m):
        return remote(sbuf.at[m], rbuf.at[m], sum_s.at[m], sum_r.at[m], mate)

    pl.semaphore_wait(barrier, 3)
    for t in range(3):
        for k in range(3):
            tab_copy(t, k).start()
    each(chunks, lambda c: far_copy(0, c).start())
    near_copy(0).start()
    near_copy(1).start()

    def clear(e):
        acc[0, e] = jnp.zeros_like(acc[0, e])
        acc[1, e] = jnp.zeros_like(acc[1, e])
        gacc[e] = jnp.zeros_like(gacc[e])

    each(experts, clear)
    for k in range(3):
        s_copy(k).wait()
    at = dot(x[...], s1v[...]).astype(BF16).astype(F32).T
    bt = dot(x[...], s3v[...]).astype(BF16).astype(F32).T
    sht, sdat, sdbt = swiglu_parts(at, bt, dot_nt(s2v[...], dy[...]))
    sht_o[...], sdat_o[...], sdbt_o[...] = sht, sdat, sdbt

    def shared_back(m):
        own[span(m, COLS), :] = dot(s1v[span(m, COLS), :], sdat_o[...]) + dot(s3v[span(m, COLS), :], sdbt_o[...])

    each(chunks, shared_back)

    for t in range(3):
        for k in range(3):
            tab_copy(t, k).wait()
    mine = me * experts + lax.broadcasted_iota(jnp.int32, (experts, n), 0)
    rank = lax.broadcasted_iota(jnp.int32, (SLOTS, n), 0)
    for q in range(4):
        idq, slotq, gateq = (ids, slots, gates) if q == 0 else (idg.at[q - 1], slotg.at[q - 1], gateg.at[q - 1])
        slot = jnp.full((experts, n), -1, jnp.int32)
        weight = jnp.zeros((experts, n), F32)
        for j in range(ids.shape[0]):
            hit = mine == idq[j:j + 1, :]
            slot = jnp.where(hit, slotq[j:j + 1, :], slot)
            weight = jnp.where(hit, gateq[j:j + 1, :], weight)
        for e in range(experts):
            hit = rank == slot[e:e + 1, :]
            pick[q, e * SLOTS:(e + 1) * SLOTS, :] = jnp.where(hit, 1.0, 0.0).astype(BF16)
            gate[q, e * SLOTS:(e + 1) * SLOTS, :] = jnp.sum(jnp.where(hit, weight[e:e + 1, :], 0.0), axis=1, keepdims=True)
    for h in range(2):
        spread[h] = jnp.zeros_like(spread[h])
        for e in range(experts):
            for j in range(2):
                spread[h, e * 2 * SLOTS + j * SLOTS:e * 2 * SLOTS + (j + 1) * SLOTS, j * n:(j + 1) * n] = pick[2 * h + j, e * SLOTS:(e + 1) * SLOTS, :]

    def expect(a, c):
        far_copy(a, c).wait()
        hop_copy(a, c).start()

    def gather_chunk(a, c):
        hop_copy(a, c).wait()
        for q in range(4):
            src = own_of[a] if q == 0 else got_of[a].at[q - 1]
            got = dot(pick[q], src[:, span(c, COLS)])
            if a == 1:
                got = got * gate[q]
            put_rows(got.astype(BF16), q, rows)

    expect(0, 0)
    near_copy(0).wait()

    def up_chunk(c):
        far_copy(1, c).start()
        gather_chunk(0, c)

        def up(p):
            base = c * experts + UP * p
            for k in range(UP):
                wait_w(base + k)
            for k in range(UP):
                e, i = UP * p + k, base + k
                acc[0, e] += dot(rows[e], wring[i % RING, 0])
                acc[1, e] += dot(rows[e], wring[i % RING, 1])
            for k in range(UP):
                start_w(base + k + RING)

        each(experts // UP // 2, up)

        @pl.when(c + 1 < chunks)
        def _():
            expect(0, c + 1)

        @pl.when(c + 1 == chunks)
        def _():
            expect(1, 0)

        each(experts // UP // 2, lambda p: up(p + experts // UP // 2))

    each(chunks, up_chunk)
    near_copy(1).wait()

    def down_chunk(c):
        gather_chunk(1, c)

        def down(p):
            base = c * experts + DOWN * p
            for k in range(DOWN):
                w2_copy(base + k).wait()
            parts = [dot_nt(w2ring[(base + k) % RING2], rows[DOWN * p + k]) for k in range(DOWN)]
            for k in range(DOWN):
                gacc[DOWN * p + k] += parts[k]

            @pl.when(base + RING2 < pieces)
            def _():
                for k in range(DOWN):
                    w2_copy(base + k + RING2).start()

        down(0)

        @pl.when(c + 1 < chunks)
        def _():
            expect(1, c + 1)

        each(experts // DOWN - 1, lambda p: down(p + 1))

    each(chunks, down_chunk)
    outs = [pltpu.make_async_copy(x, tok_o.at[0, 0], osem.at[0]), pltpu.make_async_copy(xg, tok_o.at[0, 1:4], osem.at[1]),
            pltpu.make_async_copy(dy, tok_o.at[1, 0], osem.at[2]), pltpu.make_async_copy(yg, tok_o.at[1, 1:4], osem.at[3]),
            pltpu.make_async_copy(pick, pick_o, osem.at[4]), pltpu.make_async_copy(gate, gate_o, osem.at[5])]
    for copy in outs:
        copy.start()

    half = ff // 2

    def middle(i):
        e, part = i // 2, span(i % 2, half)
        a, b = acc[0, e, :, part].T.astype(BF16), acc[1, e, :, part].T.astype(BF16)
        act[2, e, part, :], act[0, e, part, :], act[1, e, part, :] = swiglu_parts(a, b, gacc[e, part, :])

    each(2 * experts, middle)
    outs += [pltpu.make_async_copy(act.at[k], (dat_o, dbt_o, ht_o)[k], osem.at[6 + k]) for k in range(3)]
    for copy in outs[6:]:
        copy.start()

    def back_chunk(m):
        def back(p):
            base = pieces + m * experts + BACK * p
            for k in range(BACK):
                wait_w(base + k)
            for k in range(BACK):
                e, i = BACK * p + k, base + k
                part = (dot(wring[i % RING, 0], act[0, e]) + dot(wring[i % RING, 1], act[1, e])).astype(BF16)
                for h in range(2):
                    ret[h, :, span(e, 2 * SLOTS)] = part[:, h * 2 * SLOTS:(h + 1) * 2 * SLOTS]

            @pl.when(base + RING < 2 * pieces)
            def _():
                for k in range(BACK):
                    start_w(base + k + RING)

        each(experts // BACK, back)
        give = dot(ret[1], spread[1])
        keep = dot(ret[0], spread[0])
        sbuf[m] = give
        own[span(m, COLS), :] += keep[:, :n]
        far[span(m, COLS), :] = keep[:, n:]
        sum_copy(m).start()

    each(chunks, back_chunk)

    def add_mate(m):
        sum_copy(m).wait()
        own[span(m, COLS), :] += rbuf[m, :, :n]
        far[span(m, COLS), :] += rbuf[m, :, n:]

    each(chunks, add_mate)
    for copy in outs:
        copy.wait()


def exchange_call(x, dy, ids, slots, gates, w1, w3, w2, s1, s3, s2):
    experts, d, ff = w1.shape
    n = x.shape[0]
    chunks, rows = d // COLS, 4 * SLOTS
    vmem, hbm = pl.BlockSpec(memory_space=pltpu.VMEM), pl.BlockSpec(memory_space=pl.ANY)
    dma = pltpu.SemaphoreType.DMA
    return pl.pallas_call(
        exchange_kernel,
        in_specs=[vmem] * 5 + [hbm] * 6,
        out_specs=[hbm] * 6 + [vmem] * 5,
        out_shape=[jax.ShapeDtypeStruct((experts, ff, rows), BF16)] * 3 + [jax.ShapeDtypeStruct((2, 4, n, d), BF16), jax.ShapeDtypeStruct((4, experts * SLOTS, n), BF16), jax.ShapeDtypeStruct((4, experts * SLOTS, 1), F32)] + [jax.ShapeDtypeStruct((ff, n), BF16)] * 3 + [jax.ShapeDtypeStruct((d, n), F32)] * 2,
        scratch_shapes=[
            pltpu.VMEM((3, n, d), BF16), pltpu.VMEM((3, n, d), BF16), pltpu.VMEM((3,) + ids.shape, jnp.int32), pltpu.VMEM((3,) + ids.shape, jnp.int32), pltpu.VMEM((3,) + ids.shape, F32),
            pltpu.VMEM((RING, 2, COLS, ff), BF16), pltpu.VMEM((RING2, ff, COLS), BF16),
            pltpu.VMEM((d, ff), BF16), pltpu.VMEM((d, ff), BF16), pltpu.VMEM((ff, d), BF16),
            pltpu.VMEM((2, experts, rows, ff), F32), pltpu.VMEM((experts, ff, rows), F32), pltpu.VMEM((3, experts, ff, rows), BF16),
            pltpu.VMEM((experts, rows, COLS), BF16), pltpu.VMEM((4, experts * SLOTS, n), BF16), pltpu.VMEM((4, experts * SLOTS, 1), F32),
            pltpu.VMEM((2, COLS, experts * 2 * SLOTS), BF16), pltpu.VMEM((2, experts * 2 * SLOTS, 2 * n), BF16),
            pltpu.VMEM((chunks, COLS, 2 * n), F32), pltpu.VMEM((chunks, COLS, 2 * n), F32),
            dma((2,)), dma((2,)), dma((2, chunks)), dma((2, chunks)), dma((2, chunks)), dma((2, chunks)), dma((3, 3)), dma((3, 3)), dma((chunks,)), dma((chunks,)),
            dma((RING, 2)), dma((RING2,)), dma((3,)), dma((9,)),
        ],
        compiler_params=pltpu.CompilerParams(collective_id=0, has_side_effects=True, vmem_limit_bytes=67043328),
        cost_estimate=pl.CostEstimate(flops=12 * experts * rows * d * ff, bytes_accessed=96 * 2**20, transcendentals=0),
        name='exchange',
    )(x, dy, ids, slots, gates, w1, w3, w2, s1, s3, s2)


def weight_kernel(sdat, sdbt, sht, tok_h, pick_h, gate_h, dat_h, dbt_h, ht_h, dw1, dw3, dw2, ds1, ds3, ds2, tok, pick, gate, act, rows, obuf, tsem, asem, osem):
    experts, d, _ = dw1.shape
    chunks = d // COLS
    slots = obuf.shape[0]

    def each(start, stop, body):
        def step(i, carry):
            body(i)
            return carry

        lax.fori_loop(start, stop, step, 0)

    def tok_copy(c):
        return pltpu.make_async_copy(tok_h.at[:, :, :, span(c, COLS)], tok.at[:, :, :, span(c, COLS)], tsem.at[c])

    def act_copy(k, i):
        return pltpu.make_async_copy((dat_h, dbt_h, ht_h)[k].at[i], act.at[k, i], asem.at[k, i])

    def out_copy(refs, k, i, c, slot):
        dst = refs[k].at[i, :, span(c, COLS)] if k == 2 else refs[k].at[i, span(c, COLS), :]
        return pltpu.make_async_copy(obuf.at[slot, k], dst, osem.at[slot, k])

    pick_copy = pltpu.make_async_copy(pick_h, pick, tsem.at[chunks])
    gate_copy = pltpu.make_async_copy(gate_h, gate, tsem.at[chunks + 1])
    tok_copy(0).start()
    pick_copy.start()
    gate_copy.start()
    each(1, chunks, lambda c: tok_copy(c).start())

    def start_act(i):
        for k in range(3):
            act_copy(k, i).start()

    each(0, experts, start_act)

    routed, shared = (dw1, dw3, dw2), (ds1, ds3, ds2)

    def claim(t):
        @pl.when(t >= slots)
        def _():
            for k in range(3):
                out_copy(routed, k, 0, 0, t % slots).wait()

    def shared_item(c):
        t = c * (experts + 1)
        claim(t)
        slot = t % slots
        xt = tok[0, 0, :, span(c, COLS)].T
        obuf[slot, 0] = dot_nt(xt, sdat[...])
        obuf[slot, 1] = dot_nt(xt, sdbt[...])
        obuf[slot, 2] = dot(sht[...], tok[1, 0, :, span(c, COLS)])
        for k in range(3):
            out_copy(shared, k, 0, c, slot).start()

    tok_copy(0).wait()
    shared_item(0)
    pick_copy.wait()
    gate_copy.wait()
    for q in range(4):
        put_rows(dot(pick[q], tok[0, q, :, :COLS]).astype(BF16), q, rows.at[0, 0])
        put_rows((dot(pick[q], tok[1, q, :, :COLS]) * gate[q]).astype(BF16), q, rows.at[0, 1])

    def chunk(c):
        now, later, follow = c % 2, (c + 1) % 2, (c + 1) % chunks

        @pl.when(c > 0)
        def _():
            shared_item(c)

        @pl.when(c + 1 < chunks)
        def _():
            tok_copy(c + 1).wait()

        def expert(e):
            t = c * (experts + 1) + 1 + e
            claim(t)

            @pl.when(c == 0)
            def _():
                for k in range(3):
                    act_copy(k, e).wait()

            slot = t % slots
            a, q = e % 2, e // 2
            got = dot(pick[q], tok[a, q, :, span(follow, COLS)]) * jnp.where(a == 1, gate[q], 1.0)
            xt = rows[now, 0, e].T
            obuf[slot, 0] = dot_nt(xt, act[0, e])
            obuf[slot, 1] = dot_nt(xt, act[1, e])
            obuf[slot, 2] = dot(act[2, e], rows[now, 1, e])
            put_rows(got.astype(BF16), q, rows.at[later, a])
            for k in range(3):
                out_copy(routed, k, e, c, slot).start()

        each(0, experts, expert)

    each(0, chunks, chunk)
    for slot in range(slots):
        for k in range(3):
            out_copy(routed, k, 0, 0, slot).wait()


def weight_call(tok, pick, gate, dat, dbt, ht, sdat, sdbt, sht):
    experts, ff, rows = dat.shape
    _, d = tok.shape[2:]
    chunks = d // COLS
    vmem, hbm = pl.BlockSpec(memory_space=pltpu.VMEM), pl.BlockSpec(memory_space=pl.ANY)
    dma = pltpu.SemaphoreType.DMA
    return pl.pallas_call(
        weight_kernel,
        in_specs=[vmem] * 3 + [hbm] * 6,
        out_specs=[hbm] * 6,
        out_shape=[jax.ShapeDtypeStruct((experts, d, ff), F32)] * 2 + [jax.ShapeDtypeStruct((experts, ff, d), F32)] + [jax.ShapeDtypeStruct((1, d, ff), F32)] * 2 + [jax.ShapeDtypeStruct((1, ff, d), F32)],
        scratch_shapes=[
            pltpu.VMEM(tok.shape, BF16), pltpu.VMEM(pick.shape, BF16), pltpu.VMEM(gate.shape, F32), pltpu.VMEM((3, experts, ff, rows), BF16),
            pltpu.VMEM((2, 2, experts, rows, COLS), BF16), pltpu.VMEM((OUTS, 3, COLS, ff), F32),
            dma((chunks + 2,)), dma((3, experts)), dma((OUTS, 3)),
        ],
        compiler_params=pltpu.CompilerParams(vmem_limit_bytes=60 * 2**20),
        cost_estimate=pl.CostEstimate(flops=6 * experts * rows * d * ff, bytes_accessed=124 * 2**20, transcendentals=0),
        name='weights',
    )(sdat, sdbt, sht, tok, pick, gate, dat, dbt, ht)


def final_kernel(own_h, back_h, out_h, own, back, out, isem, osem):
    parts = own.shape[0] // COLS
    loads = [[pltpu.make_async_copy(src.at[pl.ds(p * COLS, COLS), :], dst.at[pl.ds(p * COLS, COLS), :], isem.at[k, p]) for k, (src, dst) in enumerate(((own_h, own), (back_h, back)))] for p in range(parts)]
    for pair in loads:
        for copy in pair:
            copy.start()
    stores = []
    for p in range(parts):
        for copy in loads[p]:
            copy.wait()
        at = pl.ds(p * COLS, COLS)
        out[:, at] = (own[at, :] + back[at, :]).T.astype(BF16)
        stores.append(pltpu.make_async_copy(out.at[:, at], out_h.at[:, at], osem.at[p]))
        stores[-1].start()
    for copy in stores:
        copy.wait()


def final_call(own, back):
    d, n = own.shape
    hbm = pl.BlockSpec(memory_space=pl.ANY)
    return pl.pallas_call(
        final_kernel,
        in_specs=[hbm, hbm],
        out_specs=hbm,
        out_shape=jax.ShapeDtypeStruct((n, d), BF16),
        scratch_shapes=[pltpu.VMEM((d, n), F32), pltpu.VMEM((d, n), F32), pltpu.VMEM((n, d), BF16), pltpu.SemaphoreType.DMA((2, d // COLS)), pltpu.SemaphoreType.DMA((d // COLS,))],
        compiler_params=pltpu.CompilerParams(vmem_limit_bytes=67043328),
        name='final',
    )(own, back)


def solution(mesh):
    token_spec = P(('dp', 'ep'), None)
    expert_spec = P('ep', None, None)
    whole_spec = P(None, None)
    grad_spec = P(('dp', 'ep'), None, None)
    group = mesh.shape['ep']

    def local_backward(x, dy, expert_ids, gate_vals, slot_pos, w1, w3, w2, s1, s3, s2):
        dat, dbt, ht, tok, pick, gate, sdat, sdbt, sht, own, far = exchange_call(x, dy, expert_ids.T, slot_pos.T, gate_vals.T, w1, w3, w2, s1, s3, s2)
        back = lax.ppermute(far, 'ep', [(i, i ^ 2) for i in range(group)])
        dw1, dw3, dw2, ds1, ds3, ds2 = weight_call(tok, pick, gate, dat, dbt, ht, sdat, sdbt, sht)
        grad_x = final_call(own, back)
        return grad_x, dw1, dw3, dw2, ds1, ds3, ds2

    return jax.shard_map(local_backward, mesh=mesh, in_specs=(token_spec, token_spec, token_spec, token_spec, token_spec, expert_spec, expert_spec, expert_spec, whole_spec, whole_spec, whole_spec), out_specs=(token_spec, grad_spec, grad_spec, grad_spec, grad_spec, grad_spec, grad_spec), check_vma=False)
```

```python
import jax
import jax.numpy as jnp
from jax import lax
from jax.experimental import pallas as pl
from jax.experimental.pallas import tpu as pltpu
from jax.sharding import PartitionSpec as P


F32, BF16 = jnp.float32, jnp.bfloat16
MESH = pl.DeviceIdType.MESH
SLOTS = 64
COLS = 512
RING, RING2 = 16, 8
OUTS = 5
UP, DOWN, BACK = 4, 4, 8


def dot(a, b):
    return jnp.dot(a, b, preferred_element_type=F32)


def dot_nt(a, b):
    return lax.dot_general(a, b, (((1,), (1,)), ((), ())), preferred_element_type=F32)


def span(index, size):
    return pl.ds(pl.multiple_of(index * size, size), size)


def swiglu_factors(a, b):
    a, b = a.astype(F32), b.astype(F32)
    sigma = 0.5 * jnp.tanh(0.5 * a) + 0.5
    silu = a * sigma
    return (silu * b).astype(BF16), b * (sigma + silu * (1.0 - sigma)), silu


def put_rows(got, q, rows):
    for e in range(rows.shape[0]):
        rows[e, span(q, SLOTS), :] = got[e * SLOTS:(e + 1) * SLOTS]


def exchange_kernel(x, dy, ids, slots, gates, w1, w3, w2, s1, s3, s2, dat_o, dbt_o, ht_o, tok_o, pick_o, gate_o, sdat_o, sdbt_o, sht_o, own, far,
                    xg, yg, idg, slotg, gateg, wring, w2ring, s1v, s3v, s2v, acc, gacc, act, rows, pick, gate, ret, spread, sbuf, rbuf,
                    near_s, near_r, far_s, far_r, hop_s, hop_r, tab_s, tab_r, sum_s, sum_r, wsem, w2sem, ssem, osem):
    me = lax.axis_index('ep')
    core = me % 2
    mate = me + 1 - 2 * core
    other = (me + 2) % 4
    diag = (mate + 2) % 4
    experts, d, ff = w1.shape
    n = x.shape[0]
    chunks = d // COLS
    pieces = chunks * experts

    barrier = pltpu.get_barrier_semaphore()
    for peer in (mate, other, diag):
        pl.semaphore_signal(barrier, inc=1, device_id={'ep': peer}, device_id_type=MESH)

    def w_copy(i, k):
        src = (w1, w3)[k].at[i % experts, span((i // experts) % chunks, COLS), :]
        return pltpu.make_async_copy(src, wring.at[i % RING, k], wsem.at[i % RING, k])

    def w2_copy(j):
        return pltpu.make_async_copy(w2.at[j % experts, :, span(j // experts, COLS)], w2ring.at[j % RING2], w2sem.at[j % RING2])

    def s_copy(k):
        return pltpu.make_async_copy((s1, s3, s2)[k], (s1v, s3v, s2v)[k], ssem.at[k])

    def each(count, body):
        def step(i, carry):
            body(i)
            return carry

        lax.fori_loop(0, count, step, 0)

    def start_w(i):
        w_copy(i, 0).start()
        w_copy(i, 1).start()

    def wait_w(i):
        w_copy(i, 0).wait()
        w_copy(i, 1).wait()

    for k in range(3):
        s_copy(k).start()
    each(RING, start_w)
    each(RING2, lambda j: w2_copy(j).start())

    def remote(src, dst, send, recv, peer):
        return pltpu.make_async_remote_copy(src_ref=src, dst_ref=dst, send_sem=send, recv_sem=recv, device_id={'ep': peer}, device_id_type=MESH)

    own_of, got_of = (x, dy), (xg, yg)

    def far_copy(a, c):
        return remote(own_of[a].at[:, span(c, COLS)], got_of[a].at[0, :, span(c, COLS)], far_s.at[a, c], far_r.at[a, c], other)

    def near_copy(a):
        return remote(own_of[a], got_of[a].at[1], near_s.at[a], near_r.at[a], mate)

    def hop_copy(a, c):
        return remote(got_of[a].at[0, :, span(c, COLS)], got_of[a].at[2, :, span(c, COLS)], hop_s.at[a, c], hop_r.at[a, c], mate)

    def tab_copy(t, k):
        return remote((ids, slots, gates)[t], (idg, slotg, gateg)[t].at[k], tab_s.at[t, k], tab_r.at[t, k], (other, mate, diag)[k])

    def sum_copy(m):
        return remote(sbuf.at[m], rbuf.at[m], sum_s.at[m], sum_r.at[m], mate)

    pl.semaphore_wait(barrier, 3)
    for t in range(3):
        for k in range(3):
            tab_copy(t, k).start()
    each(chunks, lambda c: far_copy(0, c).start())
    near_copy(0).start()
    near_copy(1).start()

    def clear(e):
        acc[0, e] = jnp.zeros_like(acc[0, e])
        acc[1, e] = jnp.zeros_like(acc[1, e])
        gacc[e] = jnp.zeros_like(gacc[e])

    each(experts, clear)
    for k in range(3):
        s_copy(k).wait()
    at = dot(x[...], s1v[...]).astype(BF16).astype(F32).T
    bt = dot(x[...], s3v[...]).astype(BF16).astype(F32).T
    grad = dot_nt(s2v[...], dy[...])
    sht_o[...], by_a, by_b = swiglu_factors(at, bt)
    sdat_o[...], sdbt_o[...] = (grad * by_a).astype(BF16), (grad * by_b).astype(BF16)

    def shared_back(m):
        own[span(m, COLS), :] = dot(s1v[span(m, COLS), :], sdat_o[...]) + dot(s3v[span(m, COLS), :], sdbt_o[...])

    each(chunks, shared_back)

    for t in range(3):
        for k in range(3):
            tab_copy(t, k).wait()
    mine = me * experts + lax.broadcasted_iota(jnp.int32, (experts, n), 0)
    rank = lax.broadcasted_iota(jnp.int32, (SLOTS, n), 0)
    for q in range(4):
        idq, slotq, gateq = (ids, slots, gates) if q == 0 else (idg.at[q - 1], slotg.at[q - 1], gateg.at[q - 1])
        slot = jnp.full((experts, n), -1, jnp.int32)
        weight = jnp.zeros((experts, n), F32)
        for j in range(ids.shape[0]):
            hit = mine == idq[j:j + 1, :]
            slot = jnp.where(hit, slotq[j:j + 1, :], slot)
            weight = jnp.where(hit, gateq[j:j + 1, :], weight)
        for e in range(experts):
            hit = rank == slot[e:e + 1, :]
            pick[q, e * SLOTS:(e + 1) * SLOTS, :] = jnp.where(hit, 1.0, 0.0).astype(BF16)
            gate[q, e * SLOTS:(e + 1) * SLOTS, :] = jnp.sum(jnp.where(hit, weight[e:e + 1, :], 0.0), axis=1, keepdims=True)
    for h in range(2):
        spread[h] = jnp.zeros_like(spread[h])
        for e in range(experts):
            for j in range(2):
                spread[h, e * 2 * SLOTS + j * SLOTS:e * 2 * SLOTS + (j + 1) * SLOTS, j * n:(j + 1) * n] = pick[2 * h + j, e * SLOTS:(e + 1) * SLOTS, :]

    def expect(a, c):
        far_copy(a, c).wait()
        hop_copy(a, c).start()

    def gather_chunk(a, c):
        hop_copy(a, c).wait()
        for q in range(4):
            src = own_of[a] if q == 0 else got_of[a].at[q - 1]
            got = dot(pick[q], src[:, span(c, COLS)])
            if a == 1:
                got = got * gate[q]
            put_rows(got.astype(BF16), q, rows)

    expect(0, 0)
    near_copy(0).wait()

    def up_chunk(c):
        far_copy(1, c).start()
        gather_chunk(0, c)

        def up(p):
            base = c * experts + UP * p
            for k in range(UP):
                wait_w(base + k)
            for k in range(UP):
                e, i = UP * p + k, base + k
                acc[0, e] += dot(rows[e], wring[i % RING, 0])
                acc[1, e] += dot(rows[e], wring[i % RING, 1])
            for k in range(UP):
                start_w(base + k + RING)

        each(experts // UP // 2, up)

        @pl.when(c + 1 < chunks)
        def _():
            expect(0, c + 1)

        @pl.when(c + 1 == chunks)
        def _():
            expect(1, 0)

        each(experts // UP // 2, lambda p: up(p + experts // UP // 2))

    each(chunks, up_chunk)
    near_copy(1).wait()

    half = ff // 2

    def prepare(e):
        for h in range(2):
            part = slice(h * half, (h + 1) * half)
            a, b = acc[0, e, :, part].T.astype(BF16), acc[1, e, :, part].T.astype(BF16)
            act[2, e, part, :], acc[0, e, :, part], acc[1, e, :, part] = swiglu_factors(a, b)

    def down_chunk(c):
        gather_chunk(1, c)

        def down(p):
            base = c * experts + DOWN * p
            for k in range(DOWN):
                w2_copy(base + k).wait()
            parts = [dot_nt(w2ring[(base + k) % RING2], rows[DOWN * p + k]) for k in range(DOWN)]
            for k in range(DOWN):
                gacc[DOWN * p + k] += parts[k]
            prepare(c * (experts // DOWN) + p)

            @pl.when(base + RING2 < pieces)
            def _():
                for k in range(DOWN):
                    w2_copy(base + k + RING2).start()

        down(0)

        @pl.when(c + 1 < chunks)
        def _():
            expect(1, c + 1)

        each(experts // DOWN - 1, lambda p: down(p + 1))

    each(chunks, down_chunk)
    outs = [pltpu.make_async_copy(x, tok_o.at[0, 0], osem.at[0]), pltpu.make_async_copy(xg, tok_o.at[0, 1:4], osem.at[1]),
            pltpu.make_async_copy(dy, tok_o.at[1, 0], osem.at[2]), pltpu.make_async_copy(yg, tok_o.at[1, 1:4], osem.at[3]),
            pltpu.make_async_copy(pick, pick_o, osem.at[4]), pltpu.make_async_copy(gate, gate_o, osem.at[5])]
    for copy in outs:
        copy.start()

    def middle(e):
        for h in range(2):
            part = slice(h * half, (h + 1) * half)
            for k in range(2):
                act[k, e, part, :] = (gacc[e, part, :] * acc[k, e, :, part]).astype(BF16)

    each(experts, middle)
    outs += [pltpu.make_async_copy(act.at[k], (dat_o, dbt_o, ht_o)[k], osem.at[6 + k]) for k in range(3)]
    for copy in outs[6:]:
        copy.start()

    def back_chunk(m):
        def back(p):
            base = pieces + m * experts + BACK * p
            for k in range(BACK):
                wait_w(base + k)
            for k in range(BACK):
                e, i = BACK * p + k, base + k
                part = (dot(wring[i % RING, 0], act[0, e]) + dot(wring[i % RING, 1], act[1, e])).astype(BF16)
                for h in range(2):
                    ret[h, :, span(e, 2 * SLOTS)] = part[:, h * 2 * SLOTS:(h + 1) * 2 * SLOTS]

            @pl.when(base + RING < 2 * pieces)
            def _():
                for k in range(BACK):
                    start_w(base + k + RING)

        each(experts // BACK, back)
        give = dot(ret[1], spread[1])
        keep = dot(ret[0], spread[0])
        sbuf[m] = give
        own[span(m, COLS), :] += keep[:, :n]
        far[span(m, COLS), :] = keep[:, n:]
        sum_copy(m).start()

    each(chunks, back_chunk)

    def add_mate(m):
        sum_copy(m).wait()
        own[span(m, COLS), :] += rbuf[m, :, :n]
        far[span(m, COLS), :] += rbuf[m, :, n:]

    each(chunks, add_mate)
    for copy in outs:
        copy.wait()


def exchange_call(x, dy, ids, slots, gates, w1, w3, w2, s1, s3, s2):
    experts, d, ff = w1.shape
    n = x.shape[0]
    chunks, rows = d // COLS, 4 * SLOTS
    vmem, hbm = pl.BlockSpec(memory_space=pltpu.VMEM), pl.BlockSpec(memory_space=pl.ANY)
    dma = pltpu.SemaphoreType.DMA
    return pl.pallas_call(
        exchange_kernel,
        in_specs=[vmem] * 5 + [hbm] * 6,
        out_specs=[hbm] * 6 + [vmem] * 5,
        out_shape=[jax.ShapeDtypeStruct((experts, ff, rows), BF16)] * 3 + [jax.ShapeDtypeStruct((2, 4, n, d), BF16), jax.ShapeDtypeStruct((4, experts * SLOTS, n), BF16), jax.ShapeDtypeStruct((4, experts * SLOTS, 1), F32)] + [jax.ShapeDtypeStruct((ff, n), BF16)] * 3 + [jax.ShapeDtypeStruct((d, n), F32)] * 2,
        scratch_shapes=[
            pltpu.VMEM((3, n, d), BF16), pltpu.VMEM((3, n, d), BF16), pltpu.VMEM((3,) + ids.shape, jnp.int32), pltpu.VMEM((3,) + ids.shape, jnp.int32), pltpu.VMEM((3,) + ids.shape, F32),
            pltpu.VMEM((RING, 2, COLS, ff), BF16), pltpu.VMEM((RING2, ff, COLS), BF16),
            pltpu.VMEM((d, ff), BF16), pltpu.VMEM((d, ff), BF16), pltpu.VMEM((ff, d), BF16),
            pltpu.VMEM((2, experts, rows, ff), F32), pltpu.VMEM((experts, ff, rows), F32), pltpu.VMEM((3, experts, ff, rows), BF16),
            pltpu.VMEM((experts, rows, COLS), BF16), pltpu.VMEM((4, experts * SLOTS, n), BF16), pltpu.VMEM((4, experts * SLOTS, 1), F32),
            pltpu.VMEM((2, COLS, experts * 2 * SLOTS), BF16), pltpu.VMEM((2, experts * 2 * SLOTS, 2 * n), BF16),
            pltpu.VMEM((chunks, COLS, 2 * n), F32), pltpu.VMEM((chunks, COLS, 2 * n), F32),
            dma((2,)), dma((2,)), dma((2, chunks)), dma((2, chunks)), dma((2, chunks)), dma((2, chunks)), dma((3, 3)), dma((3, 3)), dma((chunks,)), dma((chunks,)),
            dma((RING, 2)), dma((RING2,)), dma((3,)), dma((9,)),
        ],
        compiler_params=pltpu.CompilerParams(collective_id=0, has_side_effects=True, vmem_limit_bytes=67043328),
        cost_estimate=pl.CostEstimate(flops=12 * experts * rows * d * ff, bytes_accessed=96 * 2**20, transcendentals=0),
        name='exchange',
    )(x, dy, ids, slots, gates, w1, w3, w2, s1, s3, s2)


def weight_kernel(sdat, sdbt, sht, tok_h, pick_h, gate_h, dat_h, dbt_h, ht_h, dw1, dw3, dw2, ds1, ds3, ds2, tok, pick, gate, act, rows, obuf, tsem, asem, osem):
    experts, d, _ = dw1.shape
    chunks = d // COLS
    slots = obuf.shape[0]

    def each(start, stop, body):
        def step(i, carry):
            body(i)
            return carry

        lax.fori_loop(start, stop, step, 0)

    def tok_copy(c):
        return pltpu.make_async_copy(tok_h.at[:, :, :, span(c, COLS)], tok.at[:, :, :, span(c, COLS)], tsem.at[c])

    def act_copy(k, i):
        return pltpu.make_async_copy((dat_h, dbt_h, ht_h)[k].at[i], act.at[k, i], asem.at[k, i])

    def out_copy(refs, k, i, c, slot):
        dst = refs[k].at[i, :, span(c, COLS)] if k == 2 else refs[k].at[i, span(c, COLS), :]
        return pltpu.make_async_copy(obuf.at[slot, k], dst, osem.at[slot, k])

    pick_copy = pltpu.make_async_copy(pick_h, pick, tsem.at[chunks])
    gate_copy = pltpu.make_async_copy(gate_h, gate, tsem.at[chunks + 1])
    tok_copy(0).start()
    pick_copy.start()
    gate_copy.start()
    each(1, chunks, lambda c: tok_copy(c).start())

    def start_act(i):
        for k in range(3):
            act_copy(k, i).start()

    each(0, experts, start_act)

    routed, shared = (dw1, dw3, dw2), (ds1, ds3, ds2)

    def claim(t):
        @pl.when(t >= slots)
        def _():
            for k in range(3):
                out_copy(routed, k, 0, 0, t % slots).wait()

    def shared_item(c):
        t = c * (experts + 1)
        claim(t)
        slot = t % slots
        xt = tok[0, 0, :, span(c, COLS)].T
        obuf[slot, 0] = dot_nt(xt, sdat[...])
        obuf[slot, 1] = dot_nt(xt, sdbt[...])
        obuf[slot, 2] = dot(sht[...], tok[1, 0, :, span(c, COLS)])
        for k in range(3):
            out_copy(shared, k, 0, c, slot).start()

    tok_copy(0).wait()
    shared_item(0)
    pick_copy.wait()
    gate_copy.wait()
    for q in range(4):
        put_rows(dot(pick[q], tok[0, q, :, :COLS]).astype(BF16), q, rows.at[0, 0])
        put_rows((dot(pick[q], tok[1, q, :, :COLS]) * gate[q]).astype(BF16), q, rows.at[0, 1])

    def chunk(c):
        now, later, follow = c % 2, (c + 1) % 2, (c + 1) % chunks

        @pl.when(c > 0)
        def _():
            shared_item(c)

        @pl.when(c + 1 < chunks)
        def _():
            tok_copy(c + 1).wait()

        def expert(e):
            t = c * (experts + 1) + 1 + e
            claim(t)

            @pl.when(c == 0)
            def _():
                for k in range(3):
                    act_copy(k, e).wait()

            slot = t % slots
            a, q = e % 2, e // 2
            got = dot(pick[q], tok[a, q, :, span(follow, COLS)]) * jnp.where(a == 1, gate[q], 1.0)
            xt = rows[now, 0, e].T
            obuf[slot, 0] = dot_nt(xt, act[0, e])
            obuf[slot, 1] = dot_nt(xt, act[1, e])
            obuf[slot, 2] = dot(act[2, e], rows[now, 1, e])
            put_rows(got.astype(BF16), q, rows.at[later, a])
            for k in range(3):
                out_copy(routed, k, e, c, slot).start()

        each(0, experts, expert)

    each(0, chunks, chunk)
    for slot in range(slots):
        for k in range(3):
            out_copy(routed, k, 0, 0, slot).wait()


def weight_call(tok, pick, gate, dat, dbt, ht, sdat, sdbt, sht):
    experts, ff, rows = dat.shape
    _, d = tok.shape[2:]
    chunks = d // COLS
    vmem, hbm = pl.BlockSpec(memory_space=pltpu.VMEM), pl.BlockSpec(memory_space=pl.ANY)
    dma = pltpu.SemaphoreType.DMA
    return pl.pallas_call(
        weight_kernel,
        in_specs=[vmem] * 3 + [hbm] * 6,
        out_specs=[hbm] * 6,
        out_shape=[jax.ShapeDtypeStruct((experts, d, ff), F32)] * 2 + [jax.ShapeDtypeStruct((experts, ff, d), F32)] + [jax.ShapeDtypeStruct((1, d, ff), F32)] * 2 + [jax.ShapeDtypeStruct((1, ff, d), F32)],
        scratch_shapes=[
            pltpu.VMEM(tok.shape, BF16), pltpu.VMEM(pick.shape, BF16), pltpu.VMEM(gate.shape, F32), pltpu.VMEM((3, experts, ff, rows), BF16),
            pltpu.VMEM((2, 2, experts, rows, COLS), BF16), pltpu.VMEM((OUTS, 3, COLS, ff), F32),
            dma((chunks + 2,)), dma((3, experts)), dma((OUTS, 3)),
        ],
        compiler_params=pltpu.CompilerParams(vmem_limit_bytes=60 * 2**20),
        cost_estimate=pl.CostEstimate(flops=6 * experts * rows * d * ff, bytes_accessed=124 * 2**20, transcendentals=0),
        name='weights',
    )(sdat, sdbt, sht, tok, pick, gate, dat, dbt, ht)


def final_kernel(own_h, back_h, out_h, own, back, out, isem, osem):
    parts = own.shape[0] // COLS
    loads = [[pltpu.make_async_copy(src.at[pl.ds(p * COLS, COLS), :], dst.at[pl.ds(p * COLS, COLS), :], isem.at[k, p]) for k, (src, dst) in enumerate(((own_h, own), (back_h, back)))] for p in range(parts)]
    for pair in loads:
        for copy in pair:
            copy.start()
    stores = []
    for p in range(parts):
        for copy in loads[p]:
            copy.wait()
        at = pl.ds(p * COLS, COLS)
        out[:, at] = (own[at, :] + back[at, :]).T.astype(BF16)
        stores.append(pltpu.make_async_copy(out.at[:, at], out_h.at[:, at], osem.at[p]))
        stores[-1].start()
    for copy in stores:
        copy.wait()


def final_call(own, back):
    d, n = own.shape
    hbm = pl.BlockSpec(memory_space=pl.ANY)
    return pl.pallas_call(
        final_kernel,
        in_specs=[hbm, hbm],
        out_specs=hbm,
        out_shape=jax.ShapeDtypeStruct((n, d), BF16),
        scratch_shapes=[pltpu.VMEM((d, n), F32), pltpu.VMEM((d, n), F32), pltpu.VMEM((n, d), BF16), pltpu.SemaphoreType.DMA((2, d // COLS)), pltpu.SemaphoreType.DMA((d // COLS,))],
        compiler_params=pltpu.CompilerParams(vmem_limit_bytes=67043328),
        name='final',
    )(own, back)


def solution(mesh):
    token_spec = P(('dp', 'ep'), None)
    expert_spec = P('ep', None, None)
    whole_spec = P(None, None)
    grad_spec = P(('dp', 'ep'), None, None)
    group = mesh.shape['ep']

    def local_backward(x, dy, expert_ids, gate_vals, slot_pos, w1, w3, w2, s1, s3, s2):
        dat, dbt, ht, tok, pick, gate, sdat, sdbt, sht, own, far = exchange_call(x, dy, expert_ids.T, slot_pos.T, gate_vals.T, w1, w3, w2, s1, s3, s2)
        back = lax.ppermute(far, 'ep', [(i, i ^ 2) for i in range(group)])
        dw1, dw3, dw2, ds1, ds3, ds2 = weight_call(tok, pick, gate, dat, dbt, ht, sdat, sdbt, sht)
        grad_x = final_call(own, back)
        return grad_x, dw1, dw3, dw2, ds1, ds3, ds2

    return jax.shard_map(local_backward, mesh=mesh, in_specs=(token_spec, token_spec, token_spec, token_spec, token_spec, expert_spec, expert_spec, expert_spec, whole_spec, whole_spec, whole_spec), out_specs=(token_spec, grad_spec, grad_spec, grad_spec, grad_spec, grad_spec, grad_spec), check_vma=False)
```

```python
import jax
import jax.numpy as jnp
from jax import lax
from jax.experimental import pallas as pl
from jax.experimental.pallas import tpu as pltpu
from jax.sharding import PartitionSpec as P


F32, BF16 = jnp.float32, jnp.bfloat16
MESH = pl.DeviceIdType.MESH
SLOTS = 64
COLS = 512
RING, RING2 = 16, 8
OUTS = 5
UP, DOWN, BACK = 4, 4, 8


def dot(a, b):
    return jnp.dot(a, b, preferred_element_type=F32)


def dot_nt(a, b):
    return lax.dot_general(a, b, (((1,), (1,)), ((), ())), preferred_element_type=F32)


def span(index, size):
    return pl.ds(pl.multiple_of(index * size, size), size)


def swiglu_factors(a, b):
    a, b = a.astype(F32), b.astype(F32)
    sigma = 0.5 * jnp.tanh(0.5 * a) + 0.5
    silu = a * sigma
    return (silu * b).astype(BF16), b * (sigma + silu * (1.0 - sigma)), silu


def put_rows(got, q, rows):
    for e in range(rows.shape[0]):
        rows[e, span(q, SLOTS), :] = got[e * SLOTS:(e + 1) * SLOTS]


def exchange_kernel(x, dy, ids, slots, gates, w1, w3, w2, s1, s3, s2, dat_o, dbt_o, ht_o, tok_o, pick_o, gate_o, own_o, far_o, sdat_o, sdbt_o, sht_o,
                    xg, yg, idg, slotg, gateg, wring, w2ring, s1v, s3v, s2v, acc, gacc, act, rows, pick, gate, ret, spread, sbuf, rbuf, own, far,
                    near_s, near_r, far_s, far_r, hop_s, hop_r, tab_s, tab_r, sum_s, sum_r, wsem, w2sem, ssem, osem, esem):
    me = lax.axis_index('ep')
    core = me % 2
    mate = me + 1 - 2 * core
    other = (me + 2) % 4
    diag = (mate + 2) % 4
    experts, d, ff = w1.shape
    n = x.shape[0]
    chunks = d // COLS
    pieces = chunks * experts

    barrier = pltpu.get_barrier_semaphore()
    for peer in (mate, other, diag):
        pl.semaphore_signal(barrier, inc=1, device_id={'ep': peer}, device_id_type=MESH)

    def w_copy(i, k):
        src = (w1, w3)[k].at[i % experts, span((i // experts) % chunks, COLS), :]
        return pltpu.make_async_copy(src, wring.at[i % RING, k], wsem.at[i % RING, k])

    def w2_copy(j):
        return pltpu.make_async_copy(w2.at[j % experts, :, span(j // experts, COLS)], w2ring.at[j % RING2], w2sem.at[j % RING2])

    def s_copy(k):
        return pltpu.make_async_copy((s1, s3, s2)[k], (s1v, s3v, s2v)[k], ssem.at[k])

    def each(count, body):
        def step(i, carry):
            body(i)
            return carry

        lax.fori_loop(0, count, step, 0)

    def start_w(i):
        w_copy(i, 0).start()
        w_copy(i, 1).start()

    def wait_w(i):
        w_copy(i, 0).wait()
        w_copy(i, 1).wait()

    for k in range(3):
        s_copy(k).start()

    def clear(e):
        acc[0, e] = jnp.zeros_like(acc[0, e])
        acc[1, e] = jnp.zeros_like(acc[1, e])
        gacc[e] = jnp.zeros_like(gacc[e])

    each(experts, clear)

    def remote(src, dst, send, recv, peer):
        return pltpu.make_async_remote_copy(src_ref=src, dst_ref=dst, send_sem=send, recv_sem=recv, device_id={'ep': peer}, device_id_type=MESH)

    own_of, got_of = (x, dy), (xg, yg)

    def far_copy(a, c):
        return remote(own_of[a].at[:, span(c, COLS)], got_of[a].at[0, :, span(c, COLS)], far_s.at[a, c], far_r.at[a, c], other)

    def near_copy(a):
        return remote(own_of[a], got_of[a].at[1], near_s.at[a], near_r.at[a], mate)

    def hop_copy(a, c):
        return remote(got_of[a].at[0, :, span(c, COLS)], got_of[a].at[2, :, span(c, COLS)], hop_s.at[a, c], hop_r.at[a, c], mate)

    def tab_copy(t, k):
        return remote((ids, slots, gates)[t], (idg, slotg, gateg)[t].at[k], tab_s.at[t, k], tab_r.at[t, k], (other, mate, diag)[k])

    def sum_copy(m):
        return remote(sbuf.at[m], rbuf.at[m], sum_s.at[m], sum_r.at[m], mate)

    pl.semaphore_wait(barrier, 3)
    for t in range(3):
        for k in range(3):
            tab_copy(t, k).start()
    each(chunks, lambda c: far_copy(0, c).start())
    near_copy(0).start()
    near_copy(1).start()

    for k in range(3):
        s_copy(k).wait()
    each(RING // 2, start_w)
    at = dot(x[...], s1v[...]).astype(BF16).astype(F32).T
    bt = dot(x[...], s3v[...]).astype(BF16).astype(F32).T
    grad = dot_nt(s2v[...], dy[...])
    sht_o[...], by_a, by_b = swiglu_factors(at, bt)
    sdat_o[...], sdbt_o[...] = (grad * by_a).astype(BF16), (grad * by_b).astype(BF16)

    def shared_back(m):
        own[span(m, COLS), :] = dot(s1v[span(m, COLS), :], sdat_o[...]) + dot(s3v[span(m, COLS), :], sdbt_o[...])

    each(RING // 2, lambda i: start_w(i + RING // 2))
    each(RING2, lambda j: w2_copy(j).start())
    each(chunks, shared_back)

    for t in range(3):
        for k in range(3):
            tab_copy(t, k).wait()
    mine = me * experts + lax.broadcasted_iota(jnp.int32, (experts, n), 0)
    rank = lax.broadcasted_iota(jnp.int32, (SLOTS, n), 0)
    for q in range(4):
        idq, slotq, gateq = (ids, slots, gates) if q == 0 else (idg.at[q - 1], slotg.at[q - 1], gateg.at[q - 1])
        slot = jnp.full((experts, n), -1, jnp.int32)
        weight = jnp.zeros((experts, n), F32)
        for j in range(ids.shape[0]):
            hit = mine == idq[j:j + 1, :]
            slot = jnp.where(hit, slotq[j:j + 1, :], slot)
            weight = jnp.where(hit, gateq[j:j + 1, :], weight)
        for e in range(experts):
            hit = rank == slot[e:e + 1, :]
            pick[q, e * SLOTS:(e + 1) * SLOTS, :] = jnp.where(hit, 1.0, 0.0).astype(BF16)
            gate[q, e * SLOTS:(e + 1) * SLOTS, :] = jnp.sum(jnp.where(hit, weight[e:e + 1, :], 0.0), axis=1, keepdims=True)
    for h in range(2):
        spread[h] = jnp.zeros_like(spread[h])
        for e in range(experts):
            for j in range(2):
                spread[h, e * 2 * SLOTS + j * SLOTS:e * 2 * SLOTS + (j + 1) * SLOTS, j * n:(j + 1) * n] = pick[2 * h + j, e * SLOTS:(e + 1) * SLOTS, :]

    def expect(a, c):
        far_copy(a, c).wait()
        hop_copy(a, c).start()

    def gather_chunk(a, c):
        hop_copy(a, c).wait()
        for q in range(4):
            src = own_of[a] if q == 0 else got_of[a].at[q - 1]
            got = dot(pick[q], src[:, span(c, COLS)])
            if a == 1:
                got = got * gate[q]
            put_rows(got.astype(BF16), q, rows)

    expect(0, 0)
    near_copy(0).wait()

    def up_chunk(c):
        far_copy(1, c).start()
        gather_chunk(0, c)

        def up(p):
            base = c * experts + UP * p
            for k in range(UP):
                wait_w(base + k)
            for k in range(UP):
                e, i = UP * p + k, base + k
                acc[0, e] += dot(rows[e], wring[i % RING, 0])
                acc[1, e] += dot(rows[e], wring[i % RING, 1])
            for k in range(UP):
                start_w(base + k + RING)

        each(experts // UP // 2, up)

        @pl.when(c + 1 < chunks)
        def _():
            expect(0, c + 1)

        @pl.when(c + 1 == chunks)
        def _():
            expect(1, 0)

        each(experts // UP // 2, lambda p: up(p + experts // UP // 2))

    each(chunks, up_chunk)
    near_copy(1).wait()

    half = ff // 2

    def prepare(e):
        for h in range(2):
            part = slice(h * half, (h + 1) * half)
            a, b = acc[0, e, :, part].T.astype(BF16), acc[1, e, :, part].T.astype(BF16)
            act[2, e, part, :], acc[0, e, :, part], acc[1, e, :, part] = swiglu_factors(a, b)

    def down_chunk(c):
        gather_chunk(1, c)

        def down(p):
            base = c * experts + DOWN * p
            for k in range(DOWN):
                w2_copy(base + k).wait()
            parts = [dot_nt(w2ring[(base + k) % RING2], rows[DOWN * p + k]) for k in range(DOWN)]
            for k in range(DOWN):
                gacc[DOWN * p + k] += parts[k]
            prepare(c * (experts // DOWN) + p)

            @pl.when(base + RING2 < pieces)
            def _():
                for k in range(DOWN):
                    w2_copy(base + k + RING2).start()

        down(0)

        @pl.when(c + 1 < chunks)
        def _():
            expect(1, c + 1)

        each(experts // DOWN - 1, lambda p: down(p + 1))

    each(chunks, down_chunk)
    outs = [pltpu.make_async_copy(x, tok_o.at[0, 0], osem.at[0]), pltpu.make_async_copy(xg, tok_o.at[0, 1:4], osem.at[1]),
            pltpu.make_async_copy(dy, tok_o.at[1, 0], osem.at[2]), pltpu.make_async_copy(yg, tok_o.at[1, 1:4], osem.at[3]),
            pltpu.make_async_copy(pick, pick_o, osem.at[4]), pltpu.make_async_copy(gate, gate_o, osem.at[5])]
    for copy in outs:
        copy.start()

    def middle(e):
        for h in range(2):
            part = slice(h * half, (h + 1) * half)
            for k in range(2):
                act[k, e, part, :] = (gacc[e, part, :] * acc[k, e, :, part]).astype(BF16)

    each(experts, middle)
    outs += [pltpu.make_async_copy(act.at[k], (dat_o, dbt_o, ht_o)[k], osem.at[6 + k]) for k in range(3)]
    for copy in outs[6:]:
        copy.start()

    def back_chunk(m):
        def back(p):
            base = pieces + m * experts + BACK * p
            for k in range(BACK):
                wait_w(base + k)
            for k in range(BACK):
                e, i = BACK * p + k, base + k
                part = (dot(wring[i % RING, 0], act[0, e]) + dot(wring[i % RING, 1], act[1, e])).astype(BF16)
                for h in range(2):
                    ret[h, :, span(e, 2 * SLOTS)] = part[:, h * 2 * SLOTS:(h + 1) * 2 * SLOTS]

            @pl.when(base + RING < 2 * pieces)
            def _():
                for k in range(BACK):
                    start_w(base + k + RING)

        each(experts // BACK, back)
        give = dot(ret[1], spread[1])
        keep = dot(ret[0], spread[0])
        sbuf[m] = give
        own[span(m, COLS), :] += keep[:, :n]
        far[span(m, COLS), :] = keep[:, n:]
        sum_copy(m).start()

        @pl.when(m > 0)
        def _():
            add_mate(m - 1)

    def out_copies(m):
        at = span(m, COLS)
        return pltpu.make_async_copy(own.at[at, :], own_o.at[at, :], esem.at[0, m]), pltpu.make_async_copy(far.at[at, :], far_o.at[at, :], esem.at[1, m])

    def add_mate(m):
        sum_copy(m).wait()
        own[span(m, COLS), :] += rbuf[m, :, :n]
        far[span(m, COLS), :] += rbuf[m, :, n:]
        for copy in out_copies(m):
            copy.start()

    each(chunks, back_chunk)
    add_mate(chunks - 1)
    for m in range(chunks):
        for copy in out_copies(m):
            copy.wait()
    for copy in outs:
        copy.wait()


def exchange_call(x, dy, ids, slots, gates, w1, w3, w2, s1, s3, s2):
    experts, d, ff = w1.shape
    n = x.shape[0]
    chunks, rows = d // COLS, 4 * SLOTS
    vmem, hbm = pl.BlockSpec(memory_space=pltpu.VMEM), pl.BlockSpec(memory_space=pl.ANY)
    dma = pltpu.SemaphoreType.DMA
    return pl.pallas_call(
        exchange_kernel,
        in_specs=[vmem] * 5 + [hbm] * 6,
        out_specs=[hbm] * 8 + [vmem] * 3,
        out_shape=[jax.ShapeDtypeStruct((experts, ff, rows), BF16)] * 3 + [jax.ShapeDtypeStruct((2, 4, n, d), BF16), jax.ShapeDtypeStruct((4, experts * SLOTS, n), BF16), jax.ShapeDtypeStruct((4, experts * SLOTS, 1), F32)] + [jax.ShapeDtypeStruct((d, n), F32)] * 2 + [jax.ShapeDtypeStruct((ff, n), BF16)] * 3,
        scratch_shapes=[
            pltpu.VMEM((3, n, d), BF16), pltpu.VMEM((3, n, d), BF16), pltpu.VMEM((3,) + ids.shape, jnp.int32), pltpu.VMEM((3,) + ids.shape, jnp.int32), pltpu.VMEM((3,) + ids.shape, F32),
            pltpu.VMEM((RING, 2, COLS, ff), BF16), pltpu.VMEM((RING2, ff, COLS), BF16),
            pltpu.VMEM((d, ff), BF16), pltpu.VMEM((d, ff), BF16), pltpu.VMEM((ff, d), BF16),
            pltpu.VMEM((2, experts, rows, ff), F32), pltpu.VMEM((experts, ff, rows), F32), pltpu.VMEM((3, experts, ff, rows), BF16),
            pltpu.VMEM((experts, rows, COLS), BF16), pltpu.VMEM((4, experts * SLOTS, n), BF16), pltpu.VMEM((4, experts * SLOTS, 1), F32),
            pltpu.VMEM((2, COLS, experts * 2 * SLOTS), BF16), pltpu.VMEM((2, experts * 2 * SLOTS, 2 * n), BF16),
            pltpu.VMEM((chunks, COLS, 2 * n), F32), pltpu.VMEM((chunks, COLS, 2 * n), F32), pltpu.VMEM((d, n), F32), pltpu.VMEM((d, n), F32),
            dma((2,)), dma((2,)), dma((2, chunks)), dma((2, chunks)), dma((2, chunks)), dma((2, chunks)), dma((3, 3)), dma((3, 3)), dma((chunks,)), dma((chunks,)),
            dma((RING, 2)), dma((RING2,)), dma((3,)), dma((9,)), dma((2, chunks)),
        ],
        compiler_params=pltpu.CompilerParams(collective_id=0, has_side_effects=True, vmem_limit_bytes=67043328),
        cost_estimate=pl.CostEstimate(flops=12 * experts * rows * d * ff, bytes_accessed=96 * 2**20, transcendentals=0),
        name='exchange',
    )(x, dy, ids, slots, gates, w1, w3, w2, s1, s3, s2)


def weight_kernel(sdat, sdbt, sht, tok_h, pick_h, gate_h, dat_h, dbt_h, ht_h, dw1, dw3, dw2, ds1, ds3, ds2, tok, pick, gate, act, rows, obuf, tsem, asem, osem):
    experts, d, _ = dw1.shape
    chunks = d // COLS
    slots = obuf.shape[0]

    def each(start, stop, body):
        def step(i, carry):
            body(i)
            return carry

        lax.fori_loop(start, stop, step, 0)

    def tok_copy(c):
        return pltpu.make_async_copy(tok_h.at[:, :, :, span(c, COLS)], tok.at[:, :, :, span(c, COLS)], tsem.at[c])

    def act_copy(k, i):
        return pltpu.make_async_copy((dat_h, dbt_h, ht_h)[k].at[i], act.at[k, i], asem.at[k, i])

    def out_copy(refs, k, i, c, slot):
        dst = refs[k].at[i, :, span(c, COLS)] if k == 2 else refs[k].at[i, span(c, COLS), :]
        return pltpu.make_async_copy(obuf.at[slot, k], dst, osem.at[slot, k])

    pick_copy = pltpu.make_async_copy(pick_h, pick, tsem.at[chunks])
    gate_copy = pltpu.make_async_copy(gate_h, gate, tsem.at[chunks + 1])
    tok_copy(0).start()
    pick_copy.start()
    gate_copy.start()
    each(1, chunks, lambda c: tok_copy(c).start())

    def start_act(i):
        for k in range(3):
            act_copy(k, i).start()

    each(0, experts, start_act)

    routed, shared = (dw1, dw3, dw2), (ds1, ds3, ds2)

    def claim(t):
        @pl.when(t >= slots)
        def _():
            for k in range(3):
                out_copy(routed, k, 0, 0, t % slots).wait()

    def shared_item(c):
        t = c * (experts + 1)
        claim(t)
        slot = t % slots
        xt = tok[0, 0, :, span(c, COLS)].T
        obuf[slot, 0] = dot_nt(xt, sdat[...])
        obuf[slot, 1] = dot_nt(xt, sdbt[...])
        obuf[slot, 2] = dot(sht[...], tok[1, 0, :, span(c, COLS)])
        for k in range(3):
            out_copy(shared, k, 0, c, slot).start()

    tok_copy(0).wait()
    shared_item(0)
    pick_copy.wait()
    gate_copy.wait()
    for q in range(4):
        put_rows(dot(pick[q], tok[0, q, :, :COLS]).astype(BF16), q, rows.at[0, 0])
        put_rows((dot(pick[q], tok[1, q, :, :COLS]) * gate[q]).astype(BF16), q, rows.at[0, 1])

    def chunk(c):
        now, later, follow = c % 2, (c + 1) % 2, (c + 1) % chunks

        @pl.when(c > 0)
        def _():
            shared_item(c)

        @pl.when(c + 1 < chunks)
        def _():
            tok_copy(c + 1).wait()

        def expert(e):
            t = c * (experts + 1) + 1 + e
            claim(t)

            @pl.when(c == 0)
            def _():
                for k in range(3):
                    act_copy(k, e).wait()

            slot = t % slots
            a, q = e % 2, e // 2
            got = dot(pick[q], tok[a, q, :, span(follow, COLS)]) * jnp.where(a == 1, gate[q], 1.0)
            xt = rows[now, 0, e].T
            obuf[slot, 0] = dot_nt(xt, act[0, e])
            obuf[slot, 1] = dot_nt(xt, act[1, e])
            obuf[slot, 2] = dot(act[2, e], rows[now, 1, e])
            put_rows(got.astype(BF16), q, rows.at[later, a])
            for k in range(3):
                out_copy(routed, k, e, c, slot).start()

        each(0, experts, expert)

    each(0, chunks, chunk)
    for slot in range(slots):
        for k in range(3):
            out_copy(routed, k, 0, 0, slot).wait()


def weight_call(tok, pick, gate, dat, dbt, ht, sdat, sdbt, sht):
    experts, ff, rows = dat.shape
    _, d = tok.shape[2:]
    chunks = d // COLS
    vmem, hbm = pl.BlockSpec(memory_space=pltpu.VMEM), pl.BlockSpec(memory_space=pl.ANY)
    dma = pltpu.SemaphoreType.DMA
    return pl.pallas_call(
        weight_kernel,
        in_specs=[vmem] * 3 + [hbm] * 6,
        out_specs=[hbm] * 6,
        out_shape=[jax.ShapeDtypeStruct((experts, d, ff), F32)] * 2 + [jax.ShapeDtypeStruct((experts, ff, d), F32)] + [jax.ShapeDtypeStruct((1, d, ff), F32)] * 2 + [jax.ShapeDtypeStruct((1, ff, d), F32)],
        scratch_shapes=[
            pltpu.VMEM(tok.shape, BF16), pltpu.VMEM(pick.shape, BF16), pltpu.VMEM(gate.shape, F32), pltpu.VMEM((3, experts, ff, rows), BF16),
            pltpu.VMEM((2, 2, experts, rows, COLS), BF16), pltpu.VMEM((OUTS, 3, COLS, ff), F32),
            dma((chunks + 2,)), dma((3, experts)), dma((OUTS, 3)),
        ],
        compiler_params=pltpu.CompilerParams(vmem_limit_bytes=60 * 2**20),
        cost_estimate=pl.CostEstimate(flops=6 * experts * rows * d * ff, bytes_accessed=124 * 2**20, transcendentals=0),
        name='weights',
    )(sdat, sdbt, sht, tok, pick, gate, dat, dbt, ht)


def final_kernel(own_h, back_h, out_h, own, back, out, isem, osem):
    parts = own.shape[0] // COLS
    loads = [[pltpu.make_async_copy(src.at[pl.ds(p * COLS, COLS), :], dst.at[pl.ds(p * COLS, COLS), :], isem.at[k, p]) for k, (src, dst) in enumerate(((own_h, own), (back_h, back)))] for p in range(parts)]
    for pair in loads:
        for copy in pair:
            copy.start()
    stores = []
    for p in range(parts):
        for copy in loads[p]:
            copy.wait()
        at = pl.ds(p * COLS, COLS)
        out[:, at] = (own[at, :] + back[at, :]).T.astype(BF16)
        stores.append(pltpu.make_async_copy(out.at[:, at], out_h.at[:, at], osem.at[p]))
        stores[-1].start()
    for copy in stores:
        copy.wait()


def final_call(own, back):
    d, n = own.shape
    hbm = pl.BlockSpec(memory_space=pl.ANY)
    return pl.pallas_call(
        final_kernel,
        in_specs=[hbm, hbm],
        out_specs=hbm,
        out_shape=jax.ShapeDtypeStruct((n, d), BF16),
        scratch_shapes=[pltpu.VMEM((d, n), F32), pltpu.VMEM((d, n), F32), pltpu.VMEM((n, d), BF16), pltpu.SemaphoreType.DMA((2, d // COLS)), pltpu.SemaphoreType.DMA((d // COLS,))],
        compiler_params=pltpu.CompilerParams(vmem_limit_bytes=67043328),
        name='final',
    )(own, back)


def solution(mesh):
    token_spec = P(('dp', 'ep'), None)
    expert_spec = P('ep', None, None)
    whole_spec = P(None, None)
    grad_spec = P(('dp', 'ep'), None, None)
    group = mesh.shape['ep']

    def local_backward(x, dy, expert_ids, gate_vals, slot_pos, w1, w3, w2, s1, s3, s2):
        dat, dbt, ht, tok, pick, gate, own, far, sdat, sdbt, sht = exchange_call(x, dy, expert_ids.T, slot_pos.T, gate_vals.T, w1, w3, w2, s1, s3, s2)
        back = lax.ppermute(far, 'ep', [(i, i ^ 2) for i in range(group)])
        dw1, dw3, dw2, ds1, ds3, ds2 = weight_call(tok, pick, gate, dat, dbt, ht, sdat, sdbt, sht)
        grad_x = final_call(own, back)
        return grad_x, dw1, dw3, dw2, ds1, ds3, ds2

    return jax.shard_map(local_backward, mesh=mesh, in_specs=(token_spec, token_spec, token_spec, token_spec, token_spec, expert_spec, expert_spec, expert_spec, whole_spec, whole_spec, whole_spec), out_specs=(token_spec, grad_spec, grad_spec, grad_spec, grad_spec, grad_spec, grad_spec), check_vma=False)
```

```python
import jax
import jax.numpy as jnp
from jax import lax
from jax.experimental import pallas as pl
from jax.experimental.pallas import tpu as pltpu
from jax.sharding import PartitionSpec as P


F32, BF16 = jnp.float32, jnp.bfloat16
MESH = pl.DeviceIdType.MESH
SLOTS = 64
COLS = 512
RING, RING2 = 20, 12
OUTS = 5
UP, DOWN, BACK = 4, 4, 8


def dot(a, b):
    return jnp.dot(a, b, preferred_element_type=F32)


def dot_nt(a, b):
    return lax.dot_general(a, b, (((1,), (1,)), ((), ())), preferred_element_type=F32)


def span(index, size):
    return pl.ds(pl.multiple_of(index * size, size), size)


def swiglu_factors(a, b):
    a, b = a.astype(F32), b.astype(F32)
    sigma = 0.5 * jnp.tanh(0.5 * a) + 0.5
    silu = a * sigma
    return (silu * b).astype(BF16), b * (sigma + silu * (1.0 - sigma)), silu


def put_rows(got, q, rows):
    for e in range(rows.shape[0]):
        rows[e, span(q, SLOTS), :] = got[e * SLOTS:(e + 1) * SLOTS]


def exchange_kernel(x, dy, ids, slots, gates, w1, w3, w2, s1, s3, s2, dat_o, dbt_o, ht_o, tok_o, pick_o, gate_o, own_o, far_o, sdat_o, sdbt_o, sht_o,
                    xg, yg, idg, slotg, gateg, wring, w2ring, acc, gacc, act, rows, pick, gate, ret, spread, sbuf, rbuf, own, far,
                    near_s, near_r, far_s, far_r, hop_s, hop_r, tab_s, tab_r, sum_s, sum_r, wsem, w2sem, osem, esem):
    me = lax.axis_index('ep')
    core = me % 2
    mate = me + 1 - 2 * core
    other = (me + 2) % 4
    diag = (mate + 2) % 4
    experts, d, ff = w1.shape
    n = x.shape[0]
    chunks = d // COLS
    pieces = chunks * experts

    barrier = pltpu.get_barrier_semaphore()
    for peer in (mate, other, diag):
        pl.semaphore_signal(barrier, inc=1, device_id={'ep': peer}, device_id_type=MESH)

    def w_copy(i, k):
        src = (w1, w3)[k].at[i % experts, span((i // experts) % chunks, COLS), :]
        return pltpu.make_async_copy(src, wring.at[i % RING, k], wsem.at[i % RING, k])

    def w2_copy(j):
        return pltpu.make_async_copy(w2.at[j % experts, :, span(j // experts, COLS)], w2ring.at[j % RING2], w2sem.at[j % RING2])

    def s_copy(k, c):
        src = s2.at[:, span(c, COLS)] if k == 2 else (s1, s3)[k].at[span(c, COLS), :]
        return pltpu.make_async_copy(src, w2ring.at[k * chunks + c], w2sem.at[k * chunks + c])

    def each(count, body):
        def step(i, carry):
            body(i)
            return carry

        lax.fori_loop(0, count, step, 0)

    def start_w(i):
        w_copy(i, 0).start()
        w_copy(i, 1).start()

    def wait_w(i):
        w_copy(i, 0).wait()
        w_copy(i, 1).wait()

    for k in range(3):
        each(chunks, lambda c: s_copy(k, c).start())

    def clear(e):
        acc[0, e] = jnp.zeros_like(acc[0, e])
        acc[1, e] = jnp.zeros_like(acc[1, e])
        gacc[e] = jnp.zeros_like(gacc[e])

    each(experts, clear)

    def remote(src, dst, send, recv, peer):
        return pltpu.make_async_remote_copy(src_ref=src, dst_ref=dst, send_sem=send, recv_sem=recv, device_id={'ep': peer}, device_id_type=MESH)

    own_of, got_of = (x, dy), (xg, yg)

    def far_copy(a, c):
        return remote(own_of[a].at[:, span(c, COLS)], got_of[a].at[0, :, span(c, COLS)], far_s.at[a, c], far_r.at[a, c], other)

    def near_copy(a):
        return remote(own_of[a], got_of[a].at[1], near_s.at[a], near_r.at[a], mate)

    def hop_copy(a, c):
        return remote(got_of[a].at[0, :, span(c, COLS)], got_of[a].at[2, :, span(c, COLS)], hop_s.at[a, c], hop_r.at[a, c], mate)

    def tab_copy(t, k):
        return remote((ids, slots, gates)[t], (idg, slotg, gateg)[t].at[k], tab_s.at[t, k], tab_r.at[t, k], (other, mate, diag)[k])

    def sum_copy(m):
        return remote(sbuf.at[m], rbuf.at[m], sum_s.at[m], sum_r.at[m], mate)

    pl.semaphore_wait(barrier, 3)
    for t in range(3):
        for k in range(3):
            tab_copy(t, k).start()
    far_copy(0, 0).start()
    near_copy(0).start()
    near_copy(1).start()

    for k in range(3):
        each(chunks, lambda c: s_copy(k, c).wait())
    far_copy(0, 1).start()
    each(RING // 2, start_w)

    def over_chunks(one):
        total = one(0)
        for c in range(1, chunks):
            total += one(c)
        return total

    def cols(c):
        return slice(c * COLS, (c + 1) * COLS)

    at = over_chunks(lambda c: dot(x[:, cols(c)], w2ring[c])).astype(BF16).astype(F32).T
    bt = over_chunks(lambda c: dot(x[:, cols(c)], w2ring[chunks + c])).astype(BF16).astype(F32).T
    grad = over_chunks(lambda c: dot_nt(w2ring[2 * chunks + c], dy[:, cols(c)]))
    sht_o[...], by_a, by_b = swiglu_factors(at, bt)
    sdat_o[...], sdbt_o[...] = (grad * by_a).astype(BF16), (grad * by_b).astype(BF16)
    far_copy(0, 2).start()
    each(RING // 2, lambda i: start_w(i + RING // 2))

    def shared_back(m):
        own[span(m, COLS), :] = dot(w2ring[m], sdat_o[...]) + dot(w2ring[chunks + m], sdbt_o[...])

    each(chunks, shared_back)
    far_copy(0, 3).start()
    each(RING2, lambda j: w2_copy(j).start())

    for t in range(3):
        for k in range(3):
            tab_copy(t, k).wait()
    mine = me * experts + lax.broadcasted_iota(jnp.int32, (experts, n), 0)
    rank = lax.broadcasted_iota(jnp.int32, (SLOTS, n), 0)
    for q in range(4):
        idq, slotq, gateq = (ids, slots, gates) if q == 0 else (idg.at[q - 1], slotg.at[q - 1], gateg.at[q - 1])
        slot = jnp.full((experts, n), -1, jnp.int32)
        weight = jnp.zeros((experts, n), F32)
        for j in range(ids.shape[0]):
            hit = mine == idq[j:j + 1, :]
            slot = jnp.where(hit, slotq[j:j + 1, :], slot)
            weight = jnp.where(hit, gateq[j:j + 1, :], weight)
        for e in range(experts):
            hit = rank == slot[e:e + 1, :]
            pick[q, e * SLOTS:(e + 1) * SLOTS, :] = jnp.where(hit, 1.0, 0.0).astype(BF16)
            gate[q, e * SLOTS:(e + 1) * SLOTS, :] = jnp.sum(jnp.where(hit, weight[e:e + 1, :], 0.0), axis=1, keepdims=True)
    for h in range(2):
        spread[h] = jnp.zeros_like(spread[h])
        for e in range(experts):
            for j in range(2):
                spread[h, e * 2 * SLOTS + j * SLOTS:e * 2 * SLOTS + (j + 1) * SLOTS, j * n:(j + 1) * n] = pick[2 * h + j, e * SLOTS:(e + 1) * SLOTS, :]

    def expect(a, c):
        far_copy(a, c).wait()
        hop_copy(a, c).start()

    def gather_chunk(a, c):
        hop_copy(a, c).wait()
        for q in range(4):
            src = own_of[a] if q == 0 else got_of[a].at[q - 1]
            got = dot(pick[q], src[:, span(c, COLS)])
            if a == 1:
                got = got * gate[q]
            put_rows(got.astype(BF16), q, rows)

    expect(0, 0)
    near_copy(0).wait()

    def up_chunk(c):
        far_copy(1, c).start()
        gather_chunk(0, c)

        def up(p):
            base = c * experts + UP * p
            for k in range(UP):
                wait_w(base + k)
            for k in range(UP):
                e, i = UP * p + k, base + k
                acc[0, e] += dot(rows[e], wring[i % RING, 0])
                acc[1, e] += dot(rows[e], wring[i % RING, 1])
            for k in range(UP):
                start_w(base + k + RING)

        each(experts // UP // 2, up)

        @pl.when(c + 1 < chunks)
        def _():
            expect(0, c + 1)

        @pl.when(c + 1 == chunks)
        def _():
            expect(1, 0)

        each(experts // UP // 2, lambda p: up(p + experts // UP // 2))

    each(chunks, up_chunk)
    near_copy(1).wait()

    half = ff // 2

    def prepare(e):
        for h in range(2):
            part = slice(h * half, (h + 1) * half)
            a, b = acc[0, e, :, part].T.astype(BF16), acc[1, e, :, part].T.astype(BF16)
            act[2, e, part, :], acc[0, e, :, part], acc[1, e, :, part] = swiglu_factors(a, b)

    def down_chunk(c):
        gather_chunk(1, c)

        def down(p):
            base = c * experts + DOWN * p
            for k in range(DOWN):
                w2_copy(base + k).wait()
            parts = [dot_nt(w2ring[(base + k) % RING2], rows[DOWN * p + k]) for k in range(DOWN)]
            for k in range(DOWN):
                gacc[DOWN * p + k] += parts[k]
            prepare(c * (experts // DOWN) + p)

            @pl.when(base + RING2 < pieces)
            def _():
                for k in range(DOWN):
                    w2_copy(base + k + RING2).start()

        down(0)

        @pl.when(c + 1 < chunks)
        def _():
            expect(1, c + 1)

        each(experts // DOWN - 1, lambda p: down(p + 1))

    each(chunks, down_chunk)
    outs = [pltpu.make_async_copy(x, tok_o.at[0, 0], osem.at[0]), pltpu.make_async_copy(xg, tok_o.at[0, 1:4], osem.at[1]),
            pltpu.make_async_copy(dy, tok_o.at[1, 0], osem.at[2]), pltpu.make_async_copy(yg, tok_o.at[1, 1:4], osem.at[3]),
            pltpu.make_async_copy(pick, pick_o, osem.at[4]), pltpu.make_async_copy(gate, gate_o, osem.at[5])]
    for copy in outs:
        copy.start()

    def middle(e):
        for h in range(2):
            part = slice(h * half, (h + 1) * half)
            for k in range(2):
                act[k, e, part, :] = (gacc[e, part, :] * acc[k, e, :, part]).astype(BF16)

    each(experts, middle)
    outs += [pltpu.make_async_copy(act.at[k], (dat_o, dbt_o, ht_o)[k], osem.at[6 + k]) for k in range(3)]
    for copy in outs[6:]:
        copy.start()

    def back_chunk(m):
        def back(p):
            base = pieces + m * experts + BACK * p
            for k in range(BACK):
                wait_w(base + k)
            for k in range(BACK):
                e, i = BACK * p + k, base + k
                part = (dot(wring[i % RING, 0], act[0, e]) + dot(wring[i % RING, 1], act[1, e])).astype(BF16)
                for h in range(2):
                    ret[h, :, span(e, 2 * SLOTS)] = part[:, h * 2 * SLOTS:(h + 1) * 2 * SLOTS]

            for half in (0, BACK // 2):
                @pl.when(base + half + RING < 2 * pieces)
                def _():
                    for k in range(half, half + BACK // 2):
                        start_w(base + k + RING)

        each(experts // BACK, back)
        give = dot(ret[1], spread[1])
        keep = dot(ret[0], spread[0])
        sbuf[m] = give
        own[span(m, COLS), :] += keep[:, :n]
        far[span(m, COLS), :] = keep[:, n:]
        sum_copy(m).start()

        @pl.when(m > 0)
        def _():
            add_mate(m - 1)

    def out_copies(m):
        at = span(m, COLS)
        return pltpu.make_async_copy(own.at[at, :], own_o.at[at, :], esem.at[0, m]), pltpu.make_async_copy(far.at[at, :], far_o.at[at, :], esem.at[1, m])

    def add_mate(m):
        sum_copy(m).wait()
        own[span(m, COLS), :] += rbuf[m, :, :n]
        far[span(m, COLS), :] += rbuf[m, :, n:]
        for copy in out_copies(m):
            copy.start()

    each(chunks, back_chunk)
    add_mate(chunks - 1)
    for m in range(chunks):
        for copy in out_copies(m):
            copy.wait()
    for copy in outs:
        copy.wait()


def exchange_call(x, dy, ids, slots, gates, w1, w3, w2, s1, s3, s2):
    experts, d, ff = w1.shape
    n = x.shape[0]
    chunks, rows = d // COLS, 4 * SLOTS
    vmem, hbm = pl.BlockSpec(memory_space=pltpu.VMEM), pl.BlockSpec(memory_space=pl.ANY)
    dma = pltpu.SemaphoreType.DMA
    return pl.pallas_call(
        exchange_kernel,
        in_specs=[vmem] * 5 + [hbm] * 6,
        out_specs=[hbm] * 8 + [vmem] * 3,
        out_shape=[jax.ShapeDtypeStruct((experts, ff, rows), BF16)] * 3 + [jax.ShapeDtypeStruct((2, 4, n, d), BF16), jax.ShapeDtypeStruct((4, experts * SLOTS, n), BF16), jax.ShapeDtypeStruct((4, experts * SLOTS, 1), F32)] + [jax.ShapeDtypeStruct((d, n), F32)] * 2 + [jax.ShapeDtypeStruct((ff, n), BF16)] * 3,
        scratch_shapes=[
            pltpu.VMEM((3, n, d), BF16), pltpu.VMEM((3, n, d), BF16), pltpu.VMEM((3,) + ids.shape, jnp.int32), pltpu.VMEM((3,) + ids.shape, jnp.int32), pltpu.VMEM((3,) + ids.shape, F32),
            pltpu.VMEM((RING, 2, COLS, ff), BF16), pltpu.VMEM((RING2, ff, COLS), BF16),
            pltpu.VMEM((2, experts, rows, ff), F32), pltpu.VMEM((experts, ff, rows), F32), pltpu.VMEM((3, experts, ff, rows), BF16),
            pltpu.VMEM((experts, rows, COLS), BF16), pltpu.VMEM((4, experts * SLOTS, n), BF16), pltpu.VMEM((4, experts * SLOTS, 1), F32),
            pltpu.VMEM((2, COLS, experts * 2 * SLOTS), BF16), pltpu.VMEM((2, experts * 2 * SLOTS, 2 * n), BF16),
            pltpu.VMEM((chunks, COLS, 2 * n), F32), pltpu.VMEM((chunks, COLS, 2 * n), F32), pltpu.VMEM((d, n), F32), pltpu.VMEM((d, n), F32),
            dma((2,)), dma((2,)), dma((2, chunks)), dma((2, chunks)), dma((2, chunks)), dma((2, chunks)), dma((3, 3)), dma((3, 3)), dma((chunks,)), dma((chunks,)),
            dma((RING, 2)), dma((RING2,)), dma((9,)), dma((2, chunks)),
        ],
        compiler_params=pltpu.CompilerParams(collective_id=0, has_side_effects=True, vmem_limit_bytes=67043328),
        cost_estimate=pl.CostEstimate(flops=12 * experts * rows * d * ff, bytes_accessed=96 * 2**20, transcendentals=0),
        name='exchange',
    )(x, dy, ids, slots, gates, w1, w3, w2, s1, s3, s2)


def weight_kernel(sdat, sdbt, sht, tok_h, pick_h, gate_h, dat_h, dbt_h, ht_h, dw1, dw3, dw2, ds1, ds3, ds2, tok, pick, gate, act, rows, obuf, tsem, asem, osem):
    experts, d, _ = dw1.shape
    chunks = d // COLS
    slots = obuf.shape[0]

    def each(start, stop, body):
        def step(i, carry):
            body(i)
            return carry

        lax.fori_loop(start, stop, step, 0)

    def tok_copy(c):
        return pltpu.make_async_copy(tok_h.at[:, :, :, span(c, COLS)], tok.at[:, :, :, span(c, COLS)], tsem.at[c])

    def act_copy(k, i):
        return pltpu.make_async_copy((dat_h, dbt_h, ht_h)[k].at[i], act.at[k, i], asem.at[k, i])

    def out_copy(refs, k, i, c, slot):
        dst = refs[k].at[i, :, span(c, COLS)] if k == 2 else refs[k].at[i, span(c, COLS), :]
        return pltpu.make_async_copy(obuf.at[slot, k], dst, osem.at[slot, k])

    pick_copy = pltpu.make_async_copy(pick_h, pick, tsem.at[chunks])
    gate_copy = pltpu.make_async_copy(gate_h, gate, tsem.at[chunks + 1])
    tok_copy(0).start()
    pick_copy.start()
    gate_copy.start()
    each(1, chunks, lambda c: tok_copy(c).start())

    def start_act(i):
        for k in range(3):
            act_copy(k, i).start()

    each(0, experts, start_act)

    routed, shared = (dw1, dw3, dw2), (ds1, ds3, ds2)

    def claim(t):
        @pl.when(t >= slots)
        def _():
            for k in range(3):
                out_copy(routed, k, 0, 0, t % slots).wait()

    def shared_item(c):
        t = c * (experts + 1)
        claim(t)
        slot = t % slots
        xt = tok[0, 0, :, span(c, COLS)].T
        obuf[slot, 0] = dot_nt(xt, sdat[...])
        obuf[slot, 1] = dot_nt(xt, sdbt[...])
        obuf[slot, 2] = dot(sht[...], tok[1, 0, :, span(c, COLS)])
        for k in range(3):
            out_copy(shared, k, 0, c, slot).start()

    tok_copy(0).wait()
    shared_item(0)
    pick_copy.wait()
    gate_copy.wait()
    for q in range(4):
        put_rows(dot(pick[q], tok[0, q, :, :COLS]).astype(BF16), q, rows.at[0, 0])
        put_rows((dot(pick[q], tok[1, q, :, :COLS]) * gate[q]).astype(BF16), q, rows.at[0, 1])

    def chunk(c):
        now, later, follow = c % 2, (c + 1) % 2, (c + 1) % chunks

        @pl.when(c > 0)
        def _():
            shared_item(c)

        @pl.when(c + 1 < chunks)
        def _():
            tok_copy(c + 1).wait()

        def expert(e):
            t = c * (experts + 1) + 1 + e
            claim(t)

            @pl.when(c == 0)
            def _():
                for k in range(3):
                    act_copy(k, e).wait()

            slot = t % slots
            a, q = e % 2, e // 2
            got = dot(pick[q], tok[a, q, :, span(follow, COLS)]) * jnp.where(a == 1, gate[q], 1.0)
            xt = rows[now, 0, e].T
            obuf[slot, 0] = dot_nt(xt, act[0, e])
            obuf[slot, 1] = dot_nt(xt, act[1, e])
            obuf[slot, 2] = dot(act[2, e], rows[now, 1, e])
            put_rows(got.astype(BF16), q, rows.at[later, a])
            for k in range(3):
                out_copy(routed, k, e, c, slot).start()

        each(0, experts, expert)

    each(0, chunks, chunk)
    for slot in range(slots):
        for k in range(3):
            out_copy(routed, k, 0, 0, slot).wait()


def weight_call(tok, pick, gate, dat, dbt, ht, sdat, sdbt, sht):
    experts, ff, rows = dat.shape
    _, d = tok.shape[2:]
    chunks = d // COLS
    vmem, hbm = pl.BlockSpec(memory_space=pltpu.VMEM), pl.BlockSpec(memory_space=pl.ANY)
    dma = pltpu.SemaphoreType.DMA
    return pl.pallas_call(
        weight_kernel,
        in_specs=[vmem] * 3 + [hbm] * 6,
        out_specs=[hbm] * 6,
        out_shape=[jax.ShapeDtypeStruct((experts, d, ff), F32)] * 2 + [jax.ShapeDtypeStruct((experts, ff, d), F32)] + [jax.ShapeDtypeStruct((1, d, ff), F32)] * 2 + [jax.ShapeDtypeStruct((1, ff, d), F32)],
        scratch_shapes=[
            pltpu.VMEM(tok.shape, BF16), pltpu.VMEM(pick.shape, BF16), pltpu.VMEM(gate.shape, F32), pltpu.VMEM((3, experts, ff, rows), BF16),
            pltpu.VMEM((2, 2, experts, rows, COLS), BF16), pltpu.VMEM((OUTS, 3, COLS, ff), F32),
            dma((chunks + 2,)), dma((3, experts)), dma((OUTS, 3)),
        ],
        compiler_params=pltpu.CompilerParams(vmem_limit_bytes=60 * 2**20),
        cost_estimate=pl.CostEstimate(flops=6 * experts * rows * d * ff, bytes_accessed=124 * 2**20, transcendentals=0),
        name='weights',
    )(sdat, sdbt, sht, tok, pick, gate, dat, dbt, ht)


def final_kernel(own_h, back_h, out_h, own, back, out, isem, osem):
    parts = own.shape[0] // COLS
    loads = [[pltpu.make_async_copy(src.at[pl.ds(p * COLS, COLS), :], dst.at[pl.ds(p * COLS, COLS), :], isem.at[k, p]) for k, (src, dst) in enumerate(((own_h, own), (back_h, back)))] for p in range(parts)]
    for pair in loads:
        for copy in pair:
            copy.start()
    stores = []
    for p in range(parts):
        for copy in loads[p]:
            copy.wait()
        at = pl.ds(p * COLS, COLS)
        out[:, at] = (own[at, :] + back[at, :]).T.astype(BF16)
        stores.append(pltpu.make_async_copy(out.at[:, at], out_h.at[:, at], osem.at[p]))
        stores[-1].start()
    for copy in stores:
        copy.wait()


def final_call(own, back):
    d, n = own.shape
    hbm = pl.BlockSpec(memory_space=pl.ANY)
    return pl.pallas_call(
        final_kernel,
        in_specs=[hbm, hbm],
        out_specs=hbm,
        out_shape=jax.ShapeDtypeStruct((n, d), BF16),
        scratch_shapes=[pltpu.VMEM((d, n), F32), pltpu.VMEM((d, n), F32), pltpu.VMEM((n, d), BF16), pltpu.SemaphoreType.DMA((2, d // COLS)), pltpu.SemaphoreType.DMA((d // COLS,))],
        compiler_params=pltpu.CompilerParams(vmem_limit_bytes=67043328),
        name='final',
    )(own, back)


def solution(mesh):
    token_spec = P(('dp', 'ep'), None)
    expert_spec = P('ep', None, None)
    whole_spec = P(None, None)
    grad_spec = P(('dp', 'ep'), None, None)
    group = mesh.shape['ep']

    def local_backward(x, dy, expert_ids, gate_vals, slot_pos, w1, w3, w2, s1, s3, s2):
        dat, dbt, ht, tok, pick, gate, own, far, sdat, sdbt, sht = exchange_call(x, dy, expert_ids.T, slot_pos.T, gate_vals.T, w1, w3, w2, s1, s3, s2)
        back = lax.ppermute(far, 'ep', [(i, i ^ 2) for i in range(group)])
        dw1, dw3, dw2, ds1, ds3, ds2 = weight_call(tok, pick, gate, dat, dbt, ht, sdat, sdbt, sht)
        grad_x = final_call(own, back)
        return grad_x, dw1, dw3, dw2, ds1, ds3, ds2

    return jax.shard_map(local_backward, mesh=mesh, in_specs=(token_spec, token_spec, token_spec, token_spec, token_spec, expert_spec, expert_spec, expert_spec, whole_spec, whole_spec, whole_spec), out_specs=(token_spec, grad_spec, grad_spec, grad_spec, grad_spec, grad_spec, grad_spec), check_vma=False)
```

```python
import jax
import jax.numpy as jnp
from jax import lax
from jax.experimental import pallas as pl
from jax.experimental.pallas import tpu as pltpu
from jax.sharding import PartitionSpec as P


F32, BF16 = jnp.float32, jnp.bfloat16
MESH = pl.DeviceIdType.MESH
SLOTS = 64
COLS = 512
RING, RING2 = 20, 12
OUTS = 5
UP, DOWN, BACK = 4, 4, 8


def dot(a, b):
    return jnp.dot(a, b, preferred_element_type=F32)


def dot_nt(a, b):
    return lax.dot_general(a, b, (((1,), (1,)), ((), ())), preferred_element_type=F32)


def span(index, size):
    return pl.ds(pl.multiple_of(index * size, size), size)


def swiglu_factors(a, b):
    a, b = a.astype(F32), b.astype(F32)
    sigma = 0.5 * jnp.tanh(0.5 * a) + 0.5
    silu = a * sigma
    return (silu * b).astype(BF16), b * (sigma + silu * (1.0 - sigma)), silu


def put_rows(got, q, rows):
    for e in range(rows.shape[0]):
        rows[e, span(q, SLOTS), :] = got[e * SLOTS:(e + 1) * SLOTS]


def exchange_kernel(x, dy, ids, slots, gates, w1, w3, w2, s1, s3, s2, dat_o, dbt_o, ht_o, tok_o, pick_o, gate_o, own_o, far_o, sdat_o, sdbt_o, sht_o,
                    xg, yg, idg, slotg, gateg, wring, w2ring, acc, gacc, act, rows, pick, gate, ret, spread, sbuf, rbuf, own, far,
                    near_s, near_r, far_s, far_r, hop_s, hop_r, tab_s, tab_r, sum_s, sum_r, wsem, w2sem, osem, esem):
    me = lax.axis_index('ep')
    core = me % 2
    mate = me + 1 - 2 * core
    other = (me + 2) % 4
    diag = (mate + 2) % 4
    experts, d, ff = w1.shape
    n = x.shape[0]
    chunks = d // COLS
    pieces = chunks * experts

    barrier = pltpu.get_barrier_semaphore()
    for peer in (mate, other, diag):
        pl.semaphore_signal(barrier, inc=1, device_id={'ep': peer}, device_id_type=MESH)

    def w_copy(i, k):
        src = (w1, w3)[k].at[i % experts, span((i // experts) % chunks, COLS), :]
        return pltpu.make_async_copy(src, wring.at[i % RING, k], wsem.at[i % RING, k])

    def w2_copy(j):
        return pltpu.make_async_copy(w2.at[j % experts, :, span(j // experts, COLS)], w2ring.at[j % RING2], w2sem.at[j % RING2])

    def s_copy(k, c):
        src = s2.at[:, span(c, COLS)] if k == 2 else (s1, s3)[k].at[span(c, COLS), :]
        return pltpu.make_async_copy(src, w2ring.at[k * chunks + c], w2sem.at[k * chunks + c])

    def each(count, body):
        def step(i, carry):
            body(i)
            return carry

        lax.fori_loop(0, count, step, 0)

    def start_w(i):
        w_copy(i, 0).start()
        w_copy(i, 1).start()

    def wait_w(i):
        w_copy(i, 0).wait()
        w_copy(i, 1).wait()

    for k in range(3):
        each(chunks, lambda c: s_copy(k, c).start())

    def clear(e):
        acc[0, e] = jnp.zeros_like(acc[0, e])
        acc[1, e] = jnp.zeros_like(acc[1, e])
        gacc[e] = jnp.zeros_like(gacc[e])

    each(experts, clear)

    def remote(src, dst, send, recv, peer):
        return pltpu.make_async_remote_copy(src_ref=src, dst_ref=dst, send_sem=send, recv_sem=recv, device_id={'ep': peer}, device_id_type=MESH)

    own_of, got_of = (x, dy), (xg, yg)

    def far_copy(a, c):
        return remote(own_of[a].at[:, span(c, COLS)], got_of[a].at[0, :, span(c, COLS)], far_s.at[a, c], far_r.at[a, c], other)

    def near_copy(a):
        return remote(own_of[a], got_of[a].at[1], near_s.at[a], near_r.at[a], mate)

    def hop_copy(a, c):
        return remote(got_of[a].at[0, :, span(c, COLS)], got_of[a].at[2, :, span(c, COLS)], hop_s.at[a, c], hop_r.at[a, c], mate)

    def tab_copy(t, k):
        return remote((ids, slots, gates)[t], (idg, slotg, gateg)[t].at[k], tab_s.at[t, k], tab_r.at[t, k], (other, mate, diag)[k])

    def sum_copy(m):
        return remote(sbuf.at[m], rbuf.at[m], sum_s.at[m], sum_r.at[m], mate)

    pl.semaphore_wait(barrier, 3)
    for t in range(3):
        for k in range(3):
            tab_copy(t, k).start()
    each(chunks, lambda c: far_copy(0, c).start())
    near_copy(0).start()
    near_copy(1).start()

    for k in range(3):
        each(chunks, lambda c: s_copy(k, c).wait())
    each(RING // 2, start_w)

    def over_chunks(one):
        total = one(0)
        for c in range(1, chunks):
            total += one(c)
        return total

    def cols(c):
        return slice(c * COLS, (c + 1) * COLS)

    at = over_chunks(lambda c: dot(x[:, cols(c)], w2ring[c])).astype(BF16).astype(F32).T
    bt = over_chunks(lambda c: dot(x[:, cols(c)], w2ring[chunks + c])).astype(BF16).astype(F32).T
    grad = over_chunks(lambda c: dot_nt(w2ring[2 * chunks + c], dy[:, cols(c)]))
    sht_o[...], by_a, by_b = swiglu_factors(at, bt)
    sdat_o[...], sdbt_o[...] = (grad * by_a).astype(BF16), (grad * by_b).astype(BF16)
    each(RING // 2, lambda i: start_w(i + RING // 2))

    def shared_back(m):
        own[span(m, COLS), :] = dot(w2ring[m], sdat_o[...]) + dot(w2ring[chunks + m], sdbt_o[...])

    each(chunks, shared_back)
    each(RING2, lambda j: w2_copy(j).start())

    for t in range(3):
        for k in range(3):
            tab_copy(t, k).wait()
    mine = me * experts + lax.broadcasted_iota(jnp.int32, (experts, n), 0)
    rank = lax.broadcasted_iota(jnp.int32, (SLOTS, n), 0)
    for q in range(4):
        idq, slotq, gateq = (ids, slots, gates) if q == 0 else (idg.at[q - 1], slotg.at[q - 1], gateg.at[q - 1])
        slot = jnp.full((experts, n), -1, jnp.int32)
        weight = jnp.zeros((experts, n), F32)
        for j in range(ids.shape[0]):
            hit = mine == idq[j:j + 1, :]
            slot = jnp.where(hit, slotq[j:j + 1, :], slot)
            weight = jnp.where(hit, gateq[j:j + 1, :], weight)
        for e in range(experts):
            hit = rank == slot[e:e + 1, :]
            pick[q, e * SLOTS:(e + 1) * SLOTS, :] = jnp.where(hit, 1.0, 0.0).astype(BF16)
            gate[q, e * SLOTS:(e + 1) * SLOTS, :] = jnp.sum(jnp.where(hit, weight[e:e + 1, :], 0.0), axis=1, keepdims=True)
    for h in range(2):
        spread[h] = jnp.zeros_like(spread[h])
        for e in range(experts):
            for j in range(2):
                spread[h, e * 2 * SLOTS + j * SLOTS:e * 2 * SLOTS + (j + 1) * SLOTS, j * n:(j + 1) * n] = pick[2 * h + j, e * SLOTS:(e + 1) * SLOTS, :]

    def expect(a, c):
        far_copy(a, c).wait()
        hop_copy(a, c).start()

    def gather_chunk(a, c):
        hop_copy(a, c).wait()
        for q in range(4):
            src = own_of[a] if q == 0 else got_of[a].at[q - 1]
            got = dot(pick[q], src[:, span(c, COLS)])
            if a == 1:
                got = got * gate[q]
            put_rows(got.astype(BF16), q, rows)

    expect(0, 0)
    near_copy(0).wait()

    def up_chunk(c):
        far_copy(1, c).start()
        gather_chunk(0, c)

        def up(p):
            @pl.when((p == 1) & (c + 1 < chunks))
            def _():
                expect(0, c + 1)

            @pl.when((p == 1) & (c + 1 == chunks))
            def _():
                expect(1, 0)

            base = c * experts + UP * p
            for k in range(UP):
                wait_w(base + k)
            for k in range(UP):
                e, i = UP * p + k, base + k
                acc[0, e] += dot(rows[e], wring[i % RING, 0])
                acc[1, e] += dot(rows[e], wring[i % RING, 1])
            for k in range(UP):
                start_w(base + k + RING)

        each(experts // UP, up)

    each(chunks, up_chunk)
    near_copy(1).wait()

    half = ff // 2

    def prepare(e):
        for h in range(2):
            part = slice(h * half, (h + 1) * half)
            a, b = acc[0, e, :, part].T.astype(BF16), acc[1, e, :, part].T.astype(BF16)
            act[2, e, part, :], acc[0, e, :, part], acc[1, e, :, part] = swiglu_factors(a, b)

    def down_chunk(c):
        gather_chunk(1, c)

        def down(p):
            @pl.when((p == 1) & (c + 1 < chunks))
            def _():
                expect(1, c + 1)

            base = c * experts + DOWN * p
            for k in range(DOWN):
                w2_copy(base + k).wait()
            parts = [dot_nt(w2ring[(base + k) % RING2], rows[DOWN * p + k]) for k in range(DOWN)]
            for k in range(DOWN):
                gacc[DOWN * p + k] += parts[k]
            prepare(c * (experts // DOWN) + p)

            @pl.when(base + RING2 < pieces)
            def _():
                for k in range(DOWN):
                    w2_copy(base + k + RING2).start()

        each(experts // DOWN, down)

    each(chunks, down_chunk)
    outs = [pltpu.make_async_copy(x, tok_o.at[0, 0], osem.at[0]), pltpu.make_async_copy(xg, tok_o.at[0, 1:4], osem.at[1]),
            pltpu.make_async_copy(dy, tok_o.at[1, 0], osem.at[2]), pltpu.make_async_copy(yg, tok_o.at[1, 1:4], osem.at[3]),
            pltpu.make_async_copy(pick, pick_o, osem.at[4]), pltpu.make_async_copy(gate, gate_o, osem.at[5])]
    for copy in outs:
        copy.start()

    def middle(e):
        for h in range(2):
            part = slice(h * half, (h + 1) * half)
            for k in range(2):
                act[k, e, part, :] = (gacc[e, part, :] * acc[k, e, :, part]).astype(BF16)

    each(experts, middle)
    outs += [pltpu.make_async_copy(act.at[k], (dat_o, dbt_o, ht_o)[k], osem.at[6 + k]) for k in range(3)]
    for copy in outs[6:]:
        copy.start()

    def back_chunk(m):
        def back(p):
            base = pieces + m * experts + BACK * p
            for k in range(BACK):
                wait_w(base + k)
            for k in range(BACK):
                e, i = BACK * p + k, base + k
                part = (dot(wring[i % RING, 0], act[0, e]) + dot(wring[i % RING, 1], act[1, e])).astype(BF16)
                for h in range(2):
                    ret[h, :, span(e, 2 * SLOTS)] = part[:, h * 2 * SLOTS:(h + 1) * 2 * SLOTS]

            for half in (0, BACK // 2):
                @pl.when(base + half + RING < 2 * pieces)
                def _():
                    for k in range(half, half + BACK // 2):
                        start_w(base + k + RING)

        each(experts // BACK, back)
        give = dot(ret[1], spread[1])
        keep = dot(ret[0], spread[0])
        sbuf[m] = give
        own[span(m, COLS), :] += keep[:, :n]
        far[span(m, COLS), :] = keep[:, n:]
        sum_copy(m).start()

        @pl.when(m > 0)
        def _():
            add_mate(m - 1)

    def out_copies(m):
        at = span(m, COLS)
        return pltpu.make_async_copy(own.at[at, :], own_o.at[at, :], esem.at[0, m]), pltpu.make_async_copy(far.at[at, :], far_o.at[at, :], esem.at[1, m])

    def add_mate(m):
        sum_copy(m).wait()
        own[span(m, COLS), :] += rbuf[m, :, :n]
        far[span(m, COLS), :] += rbuf[m, :, n:]
        for copy in out_copies(m):
            copy.start()

    each(chunks, back_chunk)
    add_mate(chunks - 1)
    for m in range(chunks):
        for copy in out_copies(m):
            copy.wait()
    for copy in outs:
        copy.wait()


def exchange_call(x, dy, ids, slots, gates, w1, w3, w2, s1, s3, s2):
    experts, d, ff = w1.shape
    n = x.shape[0]
    chunks, rows = d // COLS, 4 * SLOTS
    vmem, hbm = pl.BlockSpec(memory_space=pltpu.VMEM), pl.BlockSpec(memory_space=pl.ANY)
    dma = pltpu.SemaphoreType.DMA
    return pl.pallas_call(
        exchange_kernel,
        in_specs=[vmem] * 5 + [hbm] * 6,
        out_specs=[hbm] * 8 + [vmem] * 3,
        out_shape=[jax.ShapeDtypeStruct((experts, ff, rows), BF16)] * 3 + [jax.ShapeDtypeStruct((2, 4, n, d), BF16), jax.ShapeDtypeStruct((4, experts * SLOTS, n), BF16), jax.ShapeDtypeStruct((4, experts * SLOTS, 1), F32)] + [jax.ShapeDtypeStruct((d, n), F32)] * 2 + [jax.ShapeDtypeStruct((ff, n), BF16)] * 3,
        scratch_shapes=[
            pltpu.VMEM((3, n, d), BF16), pltpu.VMEM((3, n, d), BF16), pltpu.VMEM((3,) + ids.shape, jnp.int32), pltpu.VMEM((3,) + ids.shape, jnp.int32), pltpu.VMEM((3,) + ids.shape, F32),
            pltpu.VMEM((RING, 2, COLS, ff), BF16), pltpu.VMEM((RING2, ff, COLS), BF16),
            pltpu.VMEM((2, experts, rows, ff), F32), pltpu.VMEM((experts, ff, rows), F32), pltpu.VMEM((3, experts, ff, rows), BF16),
            pltpu.VMEM((experts, rows, COLS), BF16), pltpu.VMEM((4, experts * SLOTS, n), BF16), pltpu.VMEM((4, experts * SLOTS, 1), F32),
            pltpu.VMEM((2, COLS, experts * 2 * SLOTS), BF16), pltpu.VMEM((2, experts * 2 * SLOTS, 2 * n), BF16),
            pltpu.VMEM((chunks, COLS, 2 * n), F32), pltpu.VMEM((chunks, COLS, 2 * n), F32), pltpu.VMEM((d, n), F32), pltpu.VMEM((d, n), F32),
            dma((2,)), dma((2,)), dma((2, chunks)), dma((2, chunks)), dma((2, chunks)), dma((2, chunks)), dma((3, 3)), dma((3, 3)), dma((chunks,)), dma((chunks,)),
            dma((RING, 2)), dma((RING2,)), dma((9,)), dma((2, chunks)),
        ],
        compiler_params=pltpu.CompilerParams(collective_id=0, has_side_effects=True, vmem_limit_bytes=67043328),
        cost_estimate=pl.CostEstimate(flops=12 * experts * rows * d * ff, bytes_accessed=96 * 2**20, transcendentals=0),
        name='exchange',
    )(x, dy, ids, slots, gates, w1, w3, w2, s1, s3, s2)


def weight_kernel(sdat, sdbt, sht, tok_h, pick_h, gate_h, dat_h, dbt_h, ht_h, dw1, dw3, dw2, ds1, ds3, ds2, tok, pick, gate, act, rows, obuf, tsem, asem, osem):
    experts, d, _ = dw1.shape
    chunks = d // COLS
    slots = obuf.shape[0]

    def each(start, stop, body):
        def step(i, carry):
            body(i)
            return carry

        lax.fori_loop(start, stop, step, 0)

    def tok_copy(c):
        return pltpu.make_async_copy(tok_h.at[:, :, :, span(c, COLS)], tok.at[:, :, :, span(c, COLS)], tsem.at[c])

    def act_copy(k, i):
        return pltpu.make_async_copy((dat_h, dbt_h, ht_h)[k].at[i], act.at[k, i], asem.at[k, i])

    def out_copy(refs, k, i, c, slot):
        dst = refs[k].at[i, :, span(c, COLS)] if k == 2 else refs[k].at[i, span(c, COLS), :]
        return pltpu.make_async_copy(obuf.at[slot, k], dst, osem.at[slot, k])

    pick_copy = pltpu.make_async_copy(pick_h, pick, tsem.at[chunks])
    gate_copy = pltpu.make_async_copy(gate_h, gate, tsem.at[chunks + 1])
    tok_copy(0).start()
    pick_copy.start()
    gate_copy.start()
    each(1, chunks, lambda c: tok_copy(c).start())

    def start_act(i):
        for k in range(3):
            act_copy(k, i).start()

    each(0, experts, start_act)

    routed, shared = (dw1, dw3, dw2), (ds1, ds3, ds2)

    def claim(t):
        @pl.when(t >= slots)
        def _():
            for k in range(3):
                out_copy(routed, k, 0, 0, t % slots).wait()

    def shared_item(c):
        t = c * (experts + 1)
        claim(t)
        slot = t % slots
        xt = tok[0, 0, :, span(c, COLS)].T
        obuf[slot, 0] = dot_nt(xt, sdat[...])
        obuf[slot, 1] = dot_nt(xt, sdbt[...])
        obuf[slot, 2] = dot(sht[...], tok[1, 0, :, span(c, COLS)])
        for k in range(3):
            out_copy(shared, k, 0, c, slot).start()

    tok_copy(0).wait()
    shared_item(0)
    pick_copy.wait()
    gate_copy.wait()
    for q in range(4):
        put_rows(dot(pick[q], tok[0, q, :, :COLS]).astype(BF16), q, rows.at[0, 0])
        put_rows((dot(pick[q], tok[1, q, :, :COLS]) * gate[q]).astype(BF16), q, rows.at[0, 1])

    def chunk(c):
        now, later, follow = c % 2, (c + 1) % 2, (c + 1) % chunks

        @pl.when(c > 0)
        def _():
            shared_item(c)

        @pl.when(c + 1 < chunks)
        def _():
            tok_copy(c + 1).wait()

        def expert(e):
            t = c * (experts + 1) + 1 + e
            claim(t)

            @pl.when(c == 0)
            def _():
                for k in range(3):
                    act_copy(k, e).wait()

            slot = t % slots
            a, q = e % 2, e // 2
            got = dot(pick[q], tok[a, q, :, span(follow, COLS)]) * jnp.where(a == 1, gate[q], 1.0)
            xt = rows[now, 0, e].T
            obuf[slot, 0] = dot_nt(xt, act[0, e])
            obuf[slot, 1] = dot_nt(xt, act[1, e])
            obuf[slot, 2] = dot(act[2, e], rows[now, 1, e])
            put_rows(got.astype(BF16), q, rows.at[later, a])
            for k in range(3):
                out_copy(routed, k, e, c, slot).start()

        each(0, experts, expert)

    each(0, chunks, chunk)
    for slot in range(slots):
        for k in range(3):
            out_copy(routed, k, 0, 0, slot).wait()


def weight_call(tok, pick, gate, dat, dbt, ht, sdat, sdbt, sht):
    experts, ff, rows = dat.shape
    _, d = tok.shape[2:]
    chunks = d // COLS
    vmem, hbm = pl.BlockSpec(memory_space=pltpu.VMEM), pl.BlockSpec(memory_space=pl.ANY)
    dma = pltpu.SemaphoreType.DMA
    return pl.pallas_call(
        weight_kernel,
        in_specs=[vmem] * 3 + [hbm] * 6,
        out_specs=[hbm] * 6,
        out_shape=[jax.ShapeDtypeStruct((experts, d, ff), F32)] * 2 + [jax.ShapeDtypeStruct((experts, ff, d), F32)] + [jax.ShapeDtypeStruct((1, d, ff), F32)] * 2 + [jax.ShapeDtypeStruct((1, ff, d), F32)],
        scratch_shapes=[
            pltpu.VMEM(tok.shape, BF16), pltpu.VMEM(pick.shape, BF16), pltpu.VMEM(gate.shape, F32), pltpu.VMEM((3, experts, ff, rows), BF16),
            pltpu.VMEM((2, 2, experts, rows, COLS), BF16), pltpu.VMEM((OUTS, 3, COLS, ff), F32),
            dma((chunks + 2,)), dma((3, experts)), dma((OUTS, 3)),
        ],
        compiler_params=pltpu.CompilerParams(vmem_limit_bytes=60 * 2**20),
        cost_estimate=pl.CostEstimate(flops=6 * experts * rows * d * ff, bytes_accessed=124 * 2**20, transcendentals=0),
        name='weights',
    )(sdat, sdbt, sht, tok, pick, gate, dat, dbt, ht)


def final_kernel(own_h, back_h, out_h, own, back, out, isem, osem):
    parts = own.shape[0] // COLS
    loads = [[pltpu.make_async_copy(src.at[pl.ds(p * COLS, COLS), :], dst.at[pl.ds(p * COLS, COLS), :], isem.at[k, p]) for k, (src, dst) in enumerate(((own_h, own), (back_h, back)))] for p in range(parts)]
    for pair in loads:
        for copy in pair:
            copy.start()
    stores = []
    for p in range(parts):
        for copy in loads[p]:
            copy.wait()
        at = pl.ds(p * COLS, COLS)
        out[:, at] = (own[at, :] + back[at, :]).T.astype(BF16)
        stores.append(pltpu.make_async_copy(out.at[:, at], out_h.at[:, at], osem.at[p]))
        stores[-1].start()
    for copy in stores:
        copy.wait()


def final_call(own, back):
    d, n = own.shape
    hbm = pl.BlockSpec(memory_space=pl.ANY)
    return pl.pallas_call(
        final_kernel,
        in_specs=[hbm, hbm],
        out_specs=hbm,
        out_shape=jax.ShapeDtypeStruct((n, d), BF16),
        scratch_shapes=[pltpu.VMEM((d, n), F32), pltpu.VMEM((d, n), F32), pltpu.VMEM((n, d), BF16), pltpu.SemaphoreType.DMA((2, d // COLS)), pltpu.SemaphoreType.DMA((d // COLS,))],
        compiler_params=pltpu.CompilerParams(vmem_limit_bytes=67043328),
        name='final',
    )(own, back)


def solution(mesh):
    token_spec = P(('dp', 'ep'), None)
    expert_spec = P('ep', None, None)
    whole_spec = P(None, None)
    grad_spec = P(('dp', 'ep'), None, None)
    group = mesh.shape['ep']

    def local_backward(x, dy, expert_ids, gate_vals, slot_pos, w1, w3, w2, s1, s3, s2):
        dat, dbt, ht, tok, pick, gate, own, far, sdat, sdbt, sht = exchange_call(x, dy, expert_ids.T, slot_pos.T, gate_vals.T, w1, w3, w2, s1, s3, s2)
        back = lax.ppermute(far, 'ep', [(i, i ^ 2) for i in range(group)])
        dw1, dw3, dw2, ds1, ds3, ds2 = weight_call(tok, pick, gate, dat, dbt, ht, sdat, sdbt, sht)
        grad_x = final_call(own, back)
        return grad_x, dw1, dw3, dw2, ds1, ds3, ds2

    return jax.shard_map(local_backward, mesh=mesh, in_specs=(token_spec, token_spec, token_spec, token_spec, token_spec, expert_spec, expert_spec, expert_spec, whole_spec, whole_spec, whole_spec), out_specs=(token_spec, grad_spec, grad_spec, grad_spec, grad_spec, grad_spec, grad_spec), check_vma=False)
```

```python
import jax
import jax.numpy as jnp
from jax import lax
from jax.experimental import pallas as pl
from jax.experimental.pallas import tpu as pltpu
from jax.sharding import PartitionSpec as P


F32, BF16 = jnp.float32, jnp.bfloat16
MESH = pl.DeviceIdType.MESH
SLOTS = 64
COLS = 512
RING, RING2 = 16, 16
OUTS = 5
BACK = 8


def dot(a, b):
    return jnp.dot(a, b, preferred_element_type=F32)


def dot_nt(a, b):
    return lax.dot_general(a, b, (((1,), (1,)), ((), ())), preferred_element_type=F32)


def span(index, size):
    return pl.ds(pl.multiple_of(index * size, size), size)


def swiglu_factors(a, b):
    a, b = a.astype(F32), b.astype(F32)
    sigma = 0.5 * jnp.tanh(0.5 * a) + 0.5
    silu = a * sigma
    return (silu * b).astype(BF16), b * (sigma + silu * (1.0 - sigma)), silu


def put_rows(got, q, rows):
    for e in range(rows.shape[0]):
        rows[e, span(q, SLOTS), :] = got[e * SLOTS:(e + 1) * SLOTS]


def exchange_kernel(x, dy, ids, slots, gates, w1, w3, w2, s1, s3, s2, dat_o, dbt_o, ht_o, tok_o, pick_o, gate_o, own_o, far_o, sdat_o, sdbt_o, sht_o,
                    xg, yg, idg, slotg, gateg, wring, w2ring, acc, gacc, act, rows, pick, gate, ret, spread, sbuf, rbuf, own, far,
                    near_s, near_r, far_s, far_r, hop_s, hop_r, tab_s, tab_r, sum_s, sum_r, wsem, w2sem, osem, esem):
    me = lax.axis_index('ep')
    core = me % 2
    mate = me + 1 - 2 * core
    other = (me + 2) % 4
    diag = (mate + 2) % 4
    experts, d, ff = w1.shape
    n = x.shape[0]
    chunks = d // COLS
    pieces = chunks * experts

    barrier = pltpu.get_barrier_semaphore()
    for peer in (mate, other, diag):
        pl.semaphore_signal(barrier, inc=1, device_id={'ep': peer}, device_id_type=MESH)

    def w_copy(i, k):
        src = (w1, w3)[k].at[i % experts, span((i // experts) % chunks, COLS), :]
        return pltpu.make_async_copy(src, wring.at[i % RING, k], wsem.at[i % RING, k])

    def w2_copy(j):
        return pltpu.make_async_copy(w2.at[j % experts, :, span(j // experts, COLS)], w2ring.at[j % RING2], w2sem.at[j % RING2])

    def s_copy(k, c):
        src = s2.at[:, span(c, COLS)] if k == 2 else (s1, s3)[k].at[span(c, COLS), :]
        return pltpu.make_async_copy(src, w2ring.at[k * chunks + c], w2sem.at[k * chunks + c])

    def each(count, body):
        def step(i, carry):
            body(i)
            return carry

        lax.fori_loop(0, count, step, 0)

    def start_w(i):
        w_copy(i, 0).start()
        w_copy(i, 1).start()

    def wait_w(i):
        w_copy(i, 0).wait()
        w_copy(i, 1).wait()

    for k in range(3):
        each(chunks, lambda c: s_copy(k, c).start())

    def clear(e):
        acc[0, e] = jnp.zeros_like(acc[0, e])
        acc[1, e] = jnp.zeros_like(acc[1, e])
        gacc[e] = jnp.zeros_like(gacc[e])

    each(experts, clear)

    def remote(src, dst, send, recv, peer):
        return pltpu.make_async_remote_copy(src_ref=src, dst_ref=dst, send_sem=send, recv_sem=recv, device_id={'ep': peer}, device_id_type=MESH)

    own_of, got_of = (x, dy), (xg, yg)

    def far_copy(a, c):
        return remote(own_of[a].at[:, span(c, COLS)], got_of[a].at[0, :, span(c, COLS)], far_s.at[a, c], far_r.at[a, c], other)

    def near_copy(a):
        return remote(own_of[a], got_of[a].at[1], near_s.at[a], near_r.at[a], mate)

    def hop_copy(a, c):
        return remote(got_of[a].at[0, :, span(c, COLS)], got_of[a].at[2, :, span(c, COLS)], hop_s.at[a, c], hop_r.at[a, c], mate)

    def tab_copy(t, k):
        return remote((ids, slots, gates)[t], (idg, slotg, gateg)[t].at[k], tab_s.at[t, k], tab_r.at[t, k], (other, mate, diag)[k])

    def sum_copy(m):
        return remote(sbuf.at[m], rbuf.at[m], sum_s.at[m], sum_r.at[m], mate)

    pl.semaphore_wait(barrier, 3)
    for t in range(3):
        for k in range(3):
            tab_copy(t, k).start()
    each(chunks, lambda c: far_copy(0, c).start())
    near_copy(0).start()
    near_copy(1).start()

    for k in range(3):
        each(chunks, lambda c: s_copy(k, c).wait())
    each(RING // 2, start_w)

    def over_chunks(one):
        total = one(0)
        for c in range(1, chunks):
            total += one(c)
        return total

    def cols(c):
        return slice(c * COLS, (c + 1) * COLS)

    at = over_chunks(lambda c: dot(x[:, cols(c)], w2ring[c])).astype(BF16).astype(F32).T
    bt = over_chunks(lambda c: dot(x[:, cols(c)], w2ring[chunks + c])).astype(BF16).astype(F32).T
    grad = over_chunks(lambda c: dot_nt(w2ring[2 * chunks + c], dy[:, cols(c)]))
    sht_o[...], by_a, by_b = swiglu_factors(at, bt)
    sdat_o[...], sdbt_o[...] = (grad * by_a).astype(BF16), (grad * by_b).astype(BF16)
    each(RING // 2, lambda i: start_w(i + RING // 2))

    def shared_back(m):
        own[span(m, COLS), :] = dot(w2ring[m], sdat_o[...]) + dot(w2ring[chunks + m], sdbt_o[...])

    each(chunks, shared_back)
    each(RING2, lambda j: w2_copy(j).start())

    for t in range(3):
        for k in range(3):
            tab_copy(t, k).wait()
    mine = me * experts + lax.broadcasted_iota(jnp.int32, (experts, n), 0)
    rank = lax.broadcasted_iota(jnp.int32, (SLOTS, n), 0)
    for q in range(4):
        idq, slotq, gateq = (ids, slots, gates) if q == 0 else (idg.at[q - 1], slotg.at[q - 1], gateg.at[q - 1])
        slot = jnp.full((experts, n), -1, jnp.int32)
        weight = jnp.zeros((experts, n), F32)
        for j in range(ids.shape[0]):
            hit = mine == idq[j:j + 1, :]
            slot = jnp.where(hit, slotq[j:j + 1, :], slot)
            weight = jnp.where(hit, gateq[j:j + 1, :], weight)
        for e in range(experts):
            hit = rank == slot[e:e + 1, :]
            pick[q, e * SLOTS:(e + 1) * SLOTS, :] = jnp.where(hit, 1.0, 0.0).astype(BF16)
            gate[q, e * SLOTS:(e + 1) * SLOTS, :] = jnp.sum(jnp.where(hit, weight[e:e + 1, :], 0.0), axis=1, keepdims=True)
    for h in range(2):
        spread[h] = jnp.zeros_like(spread[h])
        for e in range(experts):
            for j in range(2):
                spread[h, e * 2 * SLOTS + j * SLOTS:e * 2 * SLOTS + (j + 1) * SLOTS, j * n:(j + 1) * n] = pick[2 * h + j, e * SLOTS:(e + 1) * SLOTS, :]

    def expect(a, c):
        far_copy(a, c).wait()
        hop_copy(a, c).start()

    def gather_chunk(a, c):
        for q in range(4):
            src = own_of[a] if q == 0 else got_of[a].at[q - 1]
            got = dot(pick[q], src[:, span(c, COLS)])
            if a == 1:
                got = got * gate[q]
            put_rows(got.astype(BF16), q, rows)

    expect(0, 0)
    near_copy(0).wait()

    def up_chunk(c):
        far_copy(1, c).start()
        hop_copy(0, c).wait()

        @pl.when(c + 1 < chunks)
        def _():
            expect(0, c + 1)

        @pl.when(c + 1 == chunks)
        def _():
            expect(1, 0)

        base = c * experts
        for e in range(experts):
            wait_w(base + e)
        gather_chunk(0, c)
        for e in range(experts):
            slot = (base + e) % RING
            acc[0, e] += dot(rows[e], wring[slot, 0])
            acc[1, e] += dot(rows[e], wring[slot, 1])
        for e in range(experts):
            start_w(base + e + RING)

    each(chunks, up_chunk)
    near_copy(1).wait()

    half = ff // 2

    def prepare(e):
        for h in range(2):
            part = slice(h * half, (h + 1) * half)
            a, b = acc[0, e, :, part].T.astype(BF16), acc[1, e, :, part].T.astype(BF16)
            act[2, e, part, :], acc[0, e, :, part], acc[1, e, :, part] = swiglu_factors(a, b)

    def down_chunk(c):
        hop_copy(1, c).wait()

        @pl.when(c + 1 < chunks)
        def _():
            expect(1, c + 1)

        base = c * experts
        for e in range(experts):
            w2_copy(base + e).wait()
        gather_chunk(1, c)
        for k in range(2):
            prepare(2 * c + k)
        for e in range(experts):
            gacc[e] += dot_nt(w2ring[(base + e) % RING2], rows[e])

        @pl.when(base + RING2 < pieces)
        def _():
            for e in range(experts):
                w2_copy(base + e + RING2).start()

    each(chunks, down_chunk)
    outs = [pltpu.make_async_copy(x, tok_o.at[0, 0], osem.at[0]), pltpu.make_async_copy(xg, tok_o.at[0, 1:4], osem.at[1]),
            pltpu.make_async_copy(dy, tok_o.at[1, 0], osem.at[2]), pltpu.make_async_copy(yg, tok_o.at[1, 1:4], osem.at[3]),
            pltpu.make_async_copy(pick, pick_o, osem.at[4]), pltpu.make_async_copy(gate, gate_o, osem.at[5])]
    for copy in outs:
        copy.start()

    def middle(e):
        for h in range(2):
            part = slice(h * half, (h + 1) * half)
            for k in range(2):
                act[k, e, part, :] = (gacc[e, part, :] * acc[k, e, :, part]).astype(BF16)

    each(experts, middle)
    outs += [pltpu.make_async_copy(act.at[k], (dat_o, dbt_o, ht_o)[k], osem.at[6 + k]) for k in range(3)]
    for copy in outs[6:]:
        copy.start()

    def back_chunk(m):
        def back(p):
            base = pieces + m * experts + BACK * p
            for k in range(BACK):
                wait_w(base + k)
            for k in range(BACK):
                e, i = BACK * p + k, base + k
                part = (dot(wring[i % RING, 0], act[0, e]) + dot(wring[i % RING, 1], act[1, e])).astype(BF16)
                for h in range(2):
                    ret[h, :, span(e, 2 * SLOTS)] = part[:, h * 2 * SLOTS:(h + 1) * 2 * SLOTS]

            for half in (0, BACK // 2):
                @pl.when(base + half + RING < 2 * pieces)
                def _():
                    for k in range(half, half + BACK // 2):
                        start_w(base + k + RING)

        each(experts // BACK, back)
        give = dot(ret[1], spread[1])
        keep = dot(ret[0], spread[0])
        sbuf[m] = give
        own[span(m, COLS), :] += keep[:, :n]
        far[span(m, COLS), :] = keep[:, n:]
        sum_copy(m).start()

        @pl.when(m > 0)
        def _():
            add_mate(m - 1)

    def out_copies(m):
        at = span(m, COLS)
        return pltpu.make_async_copy(own.at[at, :], own_o.at[at, :], esem.at[0, m]), pltpu.make_async_copy(far.at[at, :], far_o.at[at, :], esem.at[1, m])

    def add_mate(m):
        sum_copy(m).wait()
        own[span(m, COLS), :] += rbuf[m, :, :n]
        far[span(m, COLS), :] += rbuf[m, :, n:]
        for copy in out_copies(m):
            copy.start()

    each(chunks, back_chunk)
    add_mate(chunks - 1)
    for m in range(chunks):
        for copy in out_copies(m):
            copy.wait()
    for copy in outs:
        copy.wait()


def exchange_call(x, dy, ids, slots, gates, w1, w3, w2, s1, s3, s2):
    experts, d, ff = w1.shape
    n = x.shape[0]
    chunks, rows = d // COLS, 4 * SLOTS
    vmem, hbm = pl.BlockSpec(memory_space=pltpu.VMEM), pl.BlockSpec(memory_space=pl.ANY)
    dma = pltpu.SemaphoreType.DMA
    return pl.pallas_call(
        exchange_kernel,
        in_specs=[vmem] * 5 + [hbm] * 6,
        out_specs=[hbm] * 8 + [vmem] * 3,
        out_shape=[jax.ShapeDtypeStruct((experts, ff, rows), BF16)] * 3 + [jax.ShapeDtypeStruct((2, 4, n, d), BF16), jax.ShapeDtypeStruct((4, experts * SLOTS, n), BF16), jax.ShapeDtypeStruct((4, experts * SLOTS, 1), F32)] + [jax.ShapeDtypeStruct((d, n), F32)] * 2 + [jax.ShapeDtypeStruct((ff, n), BF16)] * 3,
        scratch_shapes=[
            pltpu.VMEM((3, n, d), BF16), pltpu.VMEM((3, n, d), BF16), pltpu.VMEM((3,) + ids.shape, jnp.int32), pltpu.VMEM((3,) + ids.shape, jnp.int32), pltpu.VMEM((3,) + ids.shape, F32),
            pltpu.VMEM((RING, 2, COLS, ff), BF16), pltpu.VMEM((RING2, ff, COLS), BF16),
            pltpu.VMEM((2, experts, rows, ff), F32), pltpu.VMEM((experts, ff, rows), F32), pltpu.VMEM((3, experts, ff, rows), BF16),
            pltpu.VMEM((experts, rows, COLS), BF16), pltpu.VMEM((4, experts * SLOTS, n), BF16), pltpu.VMEM((4, experts * SLOTS, 1), F32),
            pltpu.VMEM((2, COLS, experts * 2 * SLOTS), BF16), pltpu.VMEM((2, experts * 2 * SLOTS, 2 * n), BF16),
            pltpu.VMEM((chunks, COLS, 2 * n), F32), pltpu.VMEM((chunks, COLS, 2 * n), F32), pltpu.VMEM((d, n), F32), pltpu.VMEM((d, n), F32),
            dma((2,)), dma((2,)), dma((2, chunks)), dma((2, chunks)), dma((2, chunks)), dma((2, chunks)), dma((3, 3)), dma((3, 3)), dma((chunks,)), dma((chunks,)),
            dma((RING, 2)), dma((RING2,)), dma((9,)), dma((2, chunks)),
        ],
        compiler_params=pltpu.CompilerParams(collective_id=0, has_side_effects=True, vmem_limit_bytes=67043328),
        cost_estimate=pl.CostEstimate(flops=12 * experts * rows * d * ff, bytes_accessed=96 * 2**20, transcendentals=0),
        name='exchange',
    )(x, dy, ids, slots, gates, w1, w3, w2, s1, s3, s2)


def weight_kernel(sdat, sdbt, sht, tok_h, pick_h, gate_h, dat_h, dbt_h, ht_h, dw1, dw3, dw2, ds1, ds3, ds2, tok, pick, gate, act, rows, obuf, tsem, asem, osem):
    experts, d, _ = dw1.shape
    chunks = d // COLS
    slots = obuf.shape[0]

    def each(start, stop, body):
        def step(i, carry):
            body(i)
            return carry

        lax.fori_loop(start, stop, step, 0)

    def tok_copy(c):
        return pltpu.make_async_copy(tok_h.at[:, :, :, span(c, COLS)], tok.at[:, :, :, span(c, COLS)], tsem.at[c])

    def act_copy(k, i):
        return pltpu.make_async_copy((dat_h, dbt_h, ht_h)[k].at[i], act.at[k, i], asem.at[k, i])

    def out_copy(refs, k, i, c, slot):
        dst = refs[k].at[i, :, span(c, COLS)] if k == 2 else refs[k].at[i, span(c, COLS), :]
        return pltpu.make_async_copy(obuf.at[slot, k], dst, osem.at[slot, k])

    pick_copy = pltpu.make_async_copy(pick_h, pick, tsem.at[chunks])
    gate_copy = pltpu.make_async_copy(gate_h, gate, tsem.at[chunks + 1])
    tok_copy(0).start()
    pick_copy.start()
    gate_copy.start()
    each(1, chunks, lambda c: tok_copy(c).start())

    def start_act(i):
        for k in range(3):
            act_copy(k, i).start()

    each(0, experts, start_act)

    routed, shared = (dw1, dw3, dw2), (ds1, ds3, ds2)

    def claim(t):
        @pl.when(t >= slots)
        def _():
            for k in range(3):
                out_copy(routed, k, 0, 0, t % slots).wait()

    def shared_item(c):
        t = c * (experts + 1)
        claim(t)
        slot = t % slots
        xt = tok[0, 0, :, span(c, COLS)].T
        obuf[slot, 0] = dot_nt(xt, sdat[...])
        obuf[slot, 1] = dot_nt(xt, sdbt[...])
        obuf[slot, 2] = dot(sht[...], tok[1, 0, :, span(c, COLS)])
        for k in range(3):
            out_copy(shared, k, 0, c, slot).start()

    tok_copy(0).wait()
    shared_item(0)
    pick_copy.wait()
    gate_copy.wait()
    for q in range(4):
        put_rows(dot(pick[q], tok[0, q, :, :COLS]).astype(BF16), q, rows.at[0, 0])
        put_rows((dot(pick[q], tok[1, q, :, :COLS]) * gate[q]).astype(BF16), q, rows.at[0, 1])

    def chunk(c):
        now, later, follow = c % 2, (c + 1) % 2, (c + 1) % chunks

        @pl.when(c > 0)
        def _():
            shared_item(c)

        @pl.when(c + 1 < chunks)
        def _():
            tok_copy(c + 1).wait()

        def expert(e):
            t = c * (experts + 1) + 1 + e
            claim(t)

            @pl.when(c == 0)
            def _():
                for k in range(3):
                    act_copy(k, e).wait()

            slot = t % slots
            a, q = e % 2, e // 2
            got = dot(pick[q], tok[a, q, :, span(follow, COLS)]) * jnp.where(a == 1, gate[q], 1.0)
            xt = rows[now, 0, e].T
            obuf[slot, 0] = dot_nt(xt, act[0, e])
            obuf[slot, 1] = dot_nt(xt, act[1, e])
            obuf[slot, 2] = dot(act[2, e], rows[now, 1, e])
            put_rows(got.astype(BF16), q, rows.at[later, a])
            for k in range(3):
                out_copy(routed, k, e, c, slot).start()

        each(0, experts, expert)

    each(0, chunks, chunk)
    for slot in range(slots):
        for k in range(3):
            out_copy(routed, k, 0, 0, slot).wait()


def weight_call(tok, pick, gate, dat, dbt, ht, sdat, sdbt, sht):
    experts, ff, rows = dat.shape
    _, d = tok.shape[2:]
    chunks = d // COLS
    vmem, hbm = pl.BlockSpec(memory_space=pltpu.VMEM), pl.BlockSpec(memory_space=pl.ANY)
    dma = pltpu.SemaphoreType.DMA
    return pl.pallas_call(
        weight_kernel,
        in_specs=[vmem] * 3 + [hbm] * 6,
        out_specs=[hbm] * 6,
        out_shape=[jax.ShapeDtypeStruct((experts, d, ff), F32)] * 2 + [jax.ShapeDtypeStruct((experts, ff, d), F32)] + [jax.ShapeDtypeStruct((1, d, ff), F32)] * 2 + [jax.ShapeDtypeStruct((1, ff, d), F32)],
        scratch_shapes=[
            pltpu.VMEM(tok.shape, BF16), pltpu.VMEM(pick.shape, BF16), pltpu.VMEM(gate.shape, F32), pltpu.VMEM((3, experts, ff, rows), BF16),
            pltpu.VMEM((2, 2, experts, rows, COLS), BF16), pltpu.VMEM((OUTS, 3, COLS, ff), F32),
            dma((chunks + 2,)), dma((3, experts)), dma((OUTS, 3)),
        ],
        compiler_params=pltpu.CompilerParams(vmem_limit_bytes=60 * 2**20),
        cost_estimate=pl.CostEstimate(flops=6 * experts * rows * d * ff, bytes_accessed=124 * 2**20, transcendentals=0),
        name='weights',
    )(sdat, sdbt, sht, tok, pick, gate, dat, dbt, ht)


def final_kernel(own_h, back_h, out_h, own, back, out, isem, osem):
    parts = own.shape[0] // COLS
    loads = [[pltpu.make_async_copy(src.at[pl.ds(p * COLS, COLS), :], dst.at[pl.ds(p * COLS, COLS), :], isem.at[k, p]) for k, (src, dst) in enumerate(((own_h, own), (back_h, back)))] for p in range(parts)]
    for pair in loads:
        for copy in pair:
            copy.start()
    stores = []
    for p in range(parts):
        for copy in loads[p]:
            copy.wait()
        at = pl.ds(p * COLS, COLS)
        out[:, at] = (own[at, :] + back[at, :]).T.astype(BF16)
        stores.append(pltpu.make_async_copy(out.at[:, at], out_h.at[:, at], osem.at[p]))
        stores[-1].start()
    for copy in stores:
        copy.wait()


def final_call(own, back):
    d, n = own.shape
    hbm = pl.BlockSpec(memory_space=pl.ANY)
    return pl.pallas_call(
        final_kernel,
        in_specs=[hbm, hbm],
        out_specs=hbm,
        out_shape=jax.ShapeDtypeStruct((n, d), BF16),
        scratch_shapes=[pltpu.VMEM((d, n), F32), pltpu.VMEM((d, n), F32), pltpu.VMEM((n, d), BF16), pltpu.SemaphoreType.DMA((2, d // COLS)), pltpu.SemaphoreType.DMA((d // COLS,))],
        compiler_params=pltpu.CompilerParams(vmem_limit_bytes=67043328),
        name='final',
    )(own, back)


def solution(mesh):
    token_spec = P(('dp', 'ep'), None)
    expert_spec = P('ep', None, None)
    whole_spec = P(None, None)
    grad_spec = P(('dp', 'ep'), None, None)
    group = mesh.shape['ep']

    def local_backward(x, dy, expert_ids, gate_vals, slot_pos, w1, w3, w2, s1, s3, s2):
        dat, dbt, ht, tok, pick, gate, own, far, sdat, sdbt, sht = exchange_call(x, dy, expert_ids.T, slot_pos.T, gate_vals.T, w1, w3, w2, s1, s3, s2)
        back = lax.ppermute(far, 'ep', [(i, i ^ 2) for i in range(group)])
        dw1, dw3, dw2, ds1, ds3, ds2 = weight_call(tok, pick, gate, dat, dbt, ht, sdat, sdbt, sht)
        grad_x = final_call(own, back)
        return grad_x, dw1, dw3, dw2, ds1, ds3, ds2

    return jax.shard_map(local_backward, mesh=mesh, in_specs=(token_spec, token_spec, token_spec, token_spec, token_spec, expert_spec, expert_spec, expert_spec, whole_spec, whole_spec, whole_spec), out_specs=(token_spec, grad_spec, grad_spec, grad_spec, grad_spec, grad_spec, grad_spec), check_vma=False)
```

```python
import jax
import jax.numpy as jnp
from jax import lax
from jax.experimental import pallas as pl
from jax.experimental.pallas import tpu as pltpu
from jax.sharding import PartitionSpec as P


F32, BF16 = jnp.float32, jnp.bfloat16
MESH = pl.DeviceIdType.MESH
SLOTS = 64
COLS = 512
RING, RING2 = 16, 16
OUTS = 5


def dot(a, b):
    return jnp.dot(a, b, preferred_element_type=F32)


def dot_nt(a, b):
    return lax.dot_general(a, b, (((1,), (1,)), ((), ())), preferred_element_type=F32)


def span(index, size):
    return pl.ds(pl.multiple_of(index * size, size), size)


def swiglu_factors(a, b):
    a, b = a.astype(F32), b.astype(F32)
    sigma = 0.5 * jnp.tanh(0.5 * a) + 0.5
    silu = a * sigma
    return (silu * b).astype(BF16), b * (sigma + silu * (1.0 - sigma)), silu


def put_rows(got, q, rows):
    for e in range(rows.shape[0]):
        rows[e, span(q, SLOTS), :] = got[e * SLOTS:(e + 1) * SLOTS]


def exchange_kernel(x, dy, ids, slots, gates, w1, w3, w2, s1, s3, s2, dat_o, dbt_o, ht_o, tok_o, pick_o, gate_o, own_o, far_o, sdat_o, sdbt_o, sht_o,
                    xg, yg, tabv, tabg, wring, w2ring, acc, gacc, act, rows, pick, gate, ret, spread, sbuf, rbuf, own, far,
                    near_s, near_r, far_s, far_r, hop_s, hop_r, tab_s, tab_r, sum_s, sum_r, wsem, w2sem, osem, esem):
    me = lax.axis_index('ep')
    core = me % 2
    mate = me + 1 - 2 * core
    other = (me + 2) % 4
    diag = (mate + 2) % 4
    experts, d, ff = w1.shape
    n = x.shape[0]
    chunks = d // COLS
    pieces = chunks * experts

    barrier = pltpu.get_barrier_semaphore()
    for peer in (mate, other, diag):
        pl.semaphore_signal(barrier, inc=1, device_id={'ep': peer}, device_id_type=MESH)

    tabv[...] = jnp.zeros_like(tabv)
    top_k = ids.shape[0]
    tabv[0, :top_k, :] = ids[...].astype(F32)
    tabv[1, :top_k, :] = slots[...].astype(F32)
    tabv[2, :top_k, :] = gates[...]

    def w_copy(i, k):
        src = (w1, w3)[k].at[i % experts, span((i // experts) % chunks, COLS), :]
        return pltpu.make_async_copy(src, wring.at[i % RING, k], wsem.at[i % RING, k])

    def w2_copy(j):
        return pltpu.make_async_copy(w2.at[j % experts, :, span(j // experts, COLS)], w2ring.at[j % RING2], w2sem.at[j % RING2])

    def s_copy(k, c):
        src = s2.at[:, span(c, COLS)] if k == 2 else (s1, s3)[k].at[span(c, COLS), :]
        return pltpu.make_async_copy(src, w2ring.at[k * chunks + c], w2sem.at[k * chunks + c])

    def each(count, body):
        def step(i, carry):
            body(i)
            return carry

        lax.fori_loop(0, count, step, 0)

    def start_w(i):
        w_copy(i, 0).start()
        w_copy(i, 1).start()

    def wait_w(i):
        w_copy(i, 0).wait()
        w_copy(i, 1).wait()

    for k in range(3):
        each(chunks, lambda c: s_copy(k, c).start())

    def clear(e):
        acc[0, e] = jnp.zeros_like(acc[0, e])
        acc[1, e] = jnp.zeros_like(acc[1, e])
        gacc[e] = jnp.zeros_like(gacc[e])

    each(experts, clear)

    def remote(src, dst, send, recv, peer):
        return pltpu.make_async_remote_copy(src_ref=src, dst_ref=dst, send_sem=send, recv_sem=recv, device_id={'ep': peer}, device_id_type=MESH)

    own_of, got_of = (x, dy), (xg, yg)

    def far_copy(a, c):
        return remote(own_of[a].at[:, span(c, COLS)], got_of[a].at[0, :, span(c, COLS)], far_s.at[a, c], far_r.at[a, c], other)

    def near_copy(a):
        return remote(own_of[a], got_of[a].at[1], near_s.at[a], near_r.at[a], mate)

    def hop_copy(a, c):
        return remote(got_of[a].at[0, :, span(c, COLS)], got_of[a].at[2, :, span(c, COLS)], hop_s.at[a, c], hop_r.at[a, c], mate)

    def tab_copy(k):
        return remote(tabv, tabg.at[k], tab_s.at[k], tab_r.at[k], (other, mate, diag)[k])

    def sum_copy(m):
        return remote(sbuf.at[m], rbuf.at[m], sum_s.at[m], sum_r.at[m], mate)

    pl.semaphore_wait(barrier, 3)
    for k in range(3):
        tab_copy(k).start()
    each(chunks, lambda c: far_copy(0, c).start())
    near_copy(0).start()
    near_copy(1).start()

    for k in range(3):
        each(chunks, lambda c: s_copy(k, c).wait())
    each(RING // 2, start_w)

    def over_chunks(one):
        total = one(0)
        for c in range(1, chunks):
            total += one(c)
        return total

    def cols(c):
        return slice(c * COLS, (c + 1) * COLS)

    at = over_chunks(lambda c: dot(x[:, cols(c)], w2ring[c])).astype(BF16).astype(F32).T
    bt = over_chunks(lambda c: dot(x[:, cols(c)], w2ring[chunks + c])).astype(BF16).astype(F32).T
    grad = over_chunks(lambda c: dot_nt(w2ring[2 * chunks + c], dy[:, cols(c)]))
    sht_o[...], by_a, by_b = swiglu_factors(at, bt)
    sdat_o[...], sdbt_o[...] = (grad * by_a).astype(BF16), (grad * by_b).astype(BF16)
    each(RING // 2, lambda i: start_w(i + RING // 2))

    def shared_back(m):
        own[span(m, COLS), :] = dot(w2ring[m], sdat_o[...]) + dot(w2ring[chunks + m], sdbt_o[...])

    each(chunks, shared_back)
    each(RING2, lambda j: w2_copy(j).start())

    for k in range(3):
        tab_copy(k).wait()
    mine = (me * experts + lax.broadcasted_iota(jnp.int32, (experts, n), 0)).astype(F32)
    rank = lax.broadcasted_iota(jnp.int32, (SLOTS, n), 0).astype(F32)
    for q in range(4):
        tabq = tabv if q == 0 else tabg.at[q - 1]
        slot = jnp.full((experts, n), -1.0, F32)
        weight = jnp.zeros((experts, n), F32)
        for j in range(ids.shape[0]):
            hit = mine == tabq[0, j:j + 1, :]
            slot = jnp.where(hit, tabq[1, j:j + 1, :], slot)
            weight = jnp.where(hit, tabq[2, j:j + 1, :], weight)
        for e in range(experts):
            hit = rank == slot[e:e + 1, :]
            pick[q, e * SLOTS:(e + 1) * SLOTS, :] = jnp.where(hit, 1.0, 0.0).astype(BF16)
            gate[q, e * SLOTS:(e + 1) * SLOTS, :] = jnp.sum(jnp.where(hit, weight[e:e + 1, :], 0.0), axis=1, keepdims=True)
    for h in range(2):
        spread[h] = jnp.zeros_like(spread[h])
        for e in range(experts):
            for j in range(2):
                spread[h, e * 2 * SLOTS + j * SLOTS:e * 2 * SLOTS + (j + 1) * SLOTS, j * n:(j + 1) * n] = pick[2 * h + j, e * SLOTS:(e + 1) * SLOTS, :]

    def expect(a, c):
        far_copy(a, c).wait()
        hop_copy(a, c).start()

    def gather_chunk(a, c):
        for q in range(4):
            src = own_of[a] if q == 0 else got_of[a].at[q - 1]
            got = dot(pick[q], src[:, span(c, COLS)])
            if a == 1:
                got = got * gate[q]
            put_rows(got.astype(BF16), q, rows)

    expect(0, 0)
    near_copy(0).wait()

    def up_chunk(c):
        far_copy(1, c).start()
        hop_copy(0, c).wait()

        @pl.when(c + 1 < chunks)
        def _():
            expect(0, c + 1)

        @pl.when(c + 1 == chunks)
        def _():
            expect(1, 0)

        base = c * experts
        for e in range(experts):
            wait_w(base + e)
        gather_chunk(0, c)
        for e in range(experts):
            slot = (base + e) % RING
            acc[0, e] += dot(rows[e], wring[slot, 0])
            acc[1, e] += dot(rows[e], wring[slot, 1])
        for e in range(experts):
            start_w(base + e + RING)

    each(chunks, up_chunk)
    near_copy(1).wait()

    half = ff // 2

    def prepare(e):
        for h in range(2):
            part = slice(h * half, (h + 1) * half)
            a, b = acc[0, e, :, part].T.astype(BF16), acc[1, e, :, part].T.astype(BF16)
            act[2, e, part, :], acc[0, e, :, part], acc[1, e, :, part] = swiglu_factors(a, b)

    def down_chunk(c):
        hop_copy(1, c).wait()

        @pl.when(c + 1 < chunks)
        def _():
            expect(1, c + 1)

        base = c * experts
        for e in range(experts):
            w2_copy(base + e).wait()
        gather_chunk(1, c)
        for k in range(2):
            prepare(2 * c + k)
        for e in range(experts):
            gacc[e] += dot_nt(w2ring[(base + e) % RING2], rows[e])

        @pl.when(base + RING2 < pieces)
        def _():
            for e in range(experts):
                w2_copy(base + e + RING2).start()

    each(chunks, down_chunk)
    outs = [pltpu.make_async_copy(x, tok_o.at[0, 0], osem.at[0]), pltpu.make_async_copy(xg, tok_o.at[0, 1:4], osem.at[1]),
            pltpu.make_async_copy(dy, tok_o.at[1, 0], osem.at[2]), pltpu.make_async_copy(yg, tok_o.at[1, 1:4], osem.at[3]),
            pltpu.make_async_copy(pick, pick_o, osem.at[4]), pltpu.make_async_copy(gate, gate_o, osem.at[5])]
    for copy in outs:
        copy.start()

    def middle(e):
        for h in range(2):
            part = slice(h * half, (h + 1) * half)
            for k in range(2):
                act[k, e, part, :] = (gacc[e, part, :] * acc[k, e, :, part]).astype(BF16)

    each(experts, middle)
    outs += [pltpu.make_async_copy(act.at[k], (dat_o, dbt_o, ht_o)[k], osem.at[6 + k]) for k in range(3)]
    for copy in outs[6:]:
        copy.start()

    def back_chunk(m):
        base = pieces + m * experts
        for e in range(experts):
            wait_w(base + e)
        for e in range(experts):
            slot = (base + e) % RING
            part = (dot(wring[slot, 0], act[0, e]) + dot(wring[slot, 1], act[1, e])).astype(BF16)
            for h in range(2):
                ret[h, :, e * 2 * SLOTS:(e + 1) * 2 * SLOTS] = part[:, h * 2 * SLOTS:(h + 1) * 2 * SLOTS]
        give = dot(ret[1], spread[1])
        keep = dot(ret[0], spread[0])
        sbuf[m] = give
        own[span(m, COLS), :] += keep[:, :n]
        far[span(m, COLS), :] = keep[:, n:]
        sum_copy(m).start()

        for half in (0, experts // 2):
            @pl.when(base + half + RING < 2 * pieces)
            def _():
                for k in range(half, half + experts // 2):
                    start_w(base + k + RING)

        @pl.when(m > 0)
        def _():
            add_mate(m - 1)

    def out_copies(m):
        at = span(m, COLS)
        return pltpu.make_async_copy(own.at[at, :], own_o.at[at, :], esem.at[0, m]), pltpu.make_async_copy(far.at[at, :], far_o.at[at, :], esem.at[1, m])

    def add_mate(m):
        sum_copy(m).wait()
        own[span(m, COLS), :] += rbuf[m, :, :n]
        far[span(m, COLS), :] += rbuf[m, :, n:]
        for copy in out_copies(m):
            copy.start()

    each(chunks, back_chunk)
    add_mate(chunks - 1)
    for m in range(chunks):
        for copy in out_copies(m):
            copy.wait()
    for copy in outs:
        copy.wait()


def exchange_call(x, dy, ids, slots, gates, w1, w3, w2, s1, s3, s2):
    experts, d, ff = w1.shape
    n = x.shape[0]
    chunks, rows = d // COLS, 4 * SLOTS
    vmem, hbm = pl.BlockSpec(memory_space=pltpu.VMEM), pl.BlockSpec(memory_space=pl.ANY)
    dma = pltpu.SemaphoreType.DMA
    return pl.pallas_call(
        exchange_kernel,
        in_specs=[vmem] * 5 + [hbm] * 6,
        out_specs=[hbm] * 8 + [vmem] * 3,
        out_shape=[jax.ShapeDtypeStruct((experts, ff, rows), BF16)] * 3 + [jax.ShapeDtypeStruct((2, 4, n, d), BF16), jax.ShapeDtypeStruct((4, experts * SLOTS, n), BF16), jax.ShapeDtypeStruct((4, experts * SLOTS, 1), F32)] + [jax.ShapeDtypeStruct((d, n), F32)] * 2 + [jax.ShapeDtypeStruct((ff, n), BF16)] * 3,
        scratch_shapes=[
            pltpu.VMEM((3, n, d), BF16), pltpu.VMEM((3, n, d), BF16), pltpu.VMEM((3, 16, n), F32), pltpu.VMEM((3, 3, 16, n), F32),
            pltpu.VMEM((RING, 2, COLS, ff), BF16), pltpu.VMEM((RING2, ff, COLS), BF16),
            pltpu.VMEM((2, experts, rows, ff), F32), pltpu.VMEM((experts, ff, rows), F32), pltpu.VMEM((3, experts, ff, rows), BF16),
            pltpu.VMEM((experts, rows, COLS), BF16), pltpu.VMEM((4, experts * SLOTS, n), BF16), pltpu.VMEM((4, experts * SLOTS, 1), F32),
            pltpu.VMEM((2, COLS, experts * 2 * SLOTS), BF16), pltpu.VMEM((2, experts * 2 * SLOTS, 2 * n), BF16),
            pltpu.VMEM((chunks, COLS, 2 * n), F32), pltpu.VMEM((chunks, COLS, 2 * n), F32), pltpu.VMEM((d, n), F32), pltpu.VMEM((d, n), F32),
            dma((2,)), dma((2,)), dma((2, chunks)), dma((2, chunks)), dma((2, chunks)), dma((2, chunks)), dma((3,)), dma((3,)), dma((chunks,)), dma((chunks,)),
            dma((RING, 2)), dma((RING2,)), dma((9,)), dma((2, chunks)),
        ],
        compiler_params=pltpu.CompilerParams(collective_id=0, has_side_effects=True, vmem_limit_bytes=67043328),
        cost_estimate=pl.CostEstimate(flops=12 * experts * rows * d * ff, bytes_accessed=96 * 2**20, transcendentals=0),
        name='exchange',
    )(x, dy, ids, slots, gates, w1, w3, w2, s1, s3, s2)


def weight_kernel(sdat, sdbt, sht, tok_h, pick_h, gate_h, dat_h, dbt_h, ht_h, dw1, dw3, dw2, ds1, ds3, ds2, tok, pick, gate, act, rows, obuf, tsem, asem, osem):
    experts, d, _ = dw1.shape
    chunks = d // COLS
    slots = obuf.shape[0]

    def each(start, stop, body):
        def step(i, carry):
            body(i)
            return carry

        lax.fori_loop(start, stop, step, 0)

    def tok_copy(c):
        return pltpu.make_async_copy(tok_h.at[:, :, :, span(c, COLS)], tok.at[:, :, :, span(c, COLS)], tsem.at[c])

    def act_copy(k, i):
        return pltpu.make_async_copy((dat_h, dbt_h, ht_h)[k].at[i], act.at[k, i], asem.at[k, i])

    def out_copy(refs, k, i, c, slot):
        dst = refs[k].at[i, :, span(c, COLS)] if k == 2 else refs[k].at[i, span(c, COLS), :]
        return pltpu.make_async_copy(obuf.at[slot, k], dst, osem.at[slot, k])

    pick_copy = pltpu.make_async_copy(pick_h, pick, tsem.at[chunks])
    gate_copy = pltpu.make_async_copy(gate_h, gate, tsem.at[chunks + 1])
    tok_copy(0).start()
    pick_copy.start()
    gate_copy.start()
    each(1, chunks, lambda c: tok_copy(c).start())

    def start_act(i):
        for k in range(3):
            act_copy(k, i).start()

    each(0, experts, start_act)

    routed, shared = (dw1, dw3, dw2), (ds1, ds3, ds2)

    def claim(t):
        @pl.when(t >= slots)
        def _():
            for k in range(3):
                out_copy(routed, k, 0, 0, t % slots).wait()

    def shared_item(c):
        t = c * (experts + 1)
        claim(t)
        slot = t % slots
        xt = tok[0, 0, :, span(c, COLS)].T
        obuf[slot, 0] = dot_nt(xt, sdat[...])
        obuf[slot, 1] = dot_nt(xt, sdbt[...])
        obuf[slot, 2] = dot(sht[...], tok[1, 0, :, span(c, COLS)])
        for k in range(3):
            out_copy(shared, k, 0, c, slot).start()

    tok_copy(0).wait()
    shared_item(0)
    pick_copy.wait()
    gate_copy.wait()
    for q in range(4):
        put_rows(dot(pick[q], tok[0, q, :, :COLS]).astype(BF16), q, rows.at[0, 0])
        put_rows((dot(pick[q], tok[1, q, :, :COLS]) * gate[q]).astype(BF16), q, rows.at[0, 1])

    def chunk(c):
        now, later, follow = c % 2, (c + 1) % 2, (c + 1) % chunks

        @pl.when(c > 0)
        def _():
            shared_item(c)

        @pl.when(c + 1 < chunks)
        def _():
            tok_copy(c + 1).wait()

        def expert(e):
            t = c * (experts + 1) + 1 + e
            claim(t)

            @pl.when(c == 0)
            def _():
                for k in range(3):
                    act_copy(k, e).wait()

            slot = t % slots
            a, q = e % 2, e // 2
            got = dot(pick[q], tok[a, q, :, span(follow, COLS)]) * jnp.where(a == 1, gate[q], 1.0)
            xt = rows[now, 0, e].T
            obuf[slot, 0] = dot_nt(xt, act[0, e])
            obuf[slot, 1] = dot_nt(xt, act[1, e])
            obuf[slot, 2] = dot(act[2, e], rows[now, 1, e])
            put_rows(got.astype(BF16), q, rows.at[later, a])
            for k in range(3):
                out_copy(routed, k, e, c, slot).start()

        each(0, experts, expert)

    each(0, chunks, chunk)
    for slot in range(slots):
        for k in range(3):
            out_copy(routed, k, 0, 0, slot).wait()


def weight_call(tok, pick, gate, dat, dbt, ht, sdat, sdbt, sht):
    experts, ff, rows = dat.shape
    _, d = tok.shape[2:]
    chunks = d // COLS
    vmem, hbm = pl.BlockSpec(memory_space=pltpu.VMEM), pl.BlockSpec(memory_space=pl.ANY)
    dma = pltpu.SemaphoreType.DMA
    return pl.pallas_call(
        weight_kernel,
        in_specs=[vmem] * 3 + [hbm] * 6,
        out_specs=[hbm] * 6,
        out_shape=[jax.ShapeDtypeStruct((experts, d, ff), F32)] * 2 + [jax.ShapeDtypeStruct((experts, ff, d), F32)] + [jax.ShapeDtypeStruct((1, d, ff), F32)] * 2 + [jax.ShapeDtypeStruct((1, ff, d), F32)],
        scratch_shapes=[
            pltpu.VMEM(tok.shape, BF16), pltpu.VMEM(pick.shape, BF16), pltpu.VMEM(gate.shape, F32), pltpu.VMEM((3, experts, ff, rows), BF16),
            pltpu.VMEM((2, 2, experts, rows, COLS), BF16), pltpu.VMEM((OUTS, 3, COLS, ff), F32),
            dma((chunks + 2,)), dma((3, experts)), dma((OUTS, 3)),
        ],
        compiler_params=pltpu.CompilerParams(vmem_limit_bytes=60 * 2**20),
        cost_estimate=pl.CostEstimate(flops=6 * experts * rows * d * ff, bytes_accessed=124 * 2**20, transcendentals=0),
        name='weights',
    )(sdat, sdbt, sht, tok, pick, gate, dat, dbt, ht)


def final_kernel(own_h, back_h, out_h, own, back, out, isem, osem):
    parts = own.shape[0] // COLS
    loads = [[pltpu.make_async_copy(src.at[pl.ds(p * COLS, COLS), :], dst.at[pl.ds(p * COLS, COLS), :], isem.at[k, p]) for k, (src, dst) in enumerate(((own_h, own), (back_h, back)))] for p in range(parts)]
    for pair in loads:
        for copy in pair:
            copy.start()
    stores = []
    for p in range(parts):
        for copy in loads[p]:
            copy.wait()
        at = pl.ds(p * COLS, COLS)
        out[:, at] = (own[at, :] + back[at, :]).T.astype(BF16)
        stores.append(pltpu.make_async_copy(out.at[:, at], out_h.at[:, at], osem.at[p]))
        stores[-1].start()
    for copy in stores:
        copy.wait()


def final_call(own, back):
    d, n = own.shape
    hbm = pl.BlockSpec(memory_space=pl.ANY)
    return pl.pallas_call(
        final_kernel,
        in_specs=[hbm, hbm],
        out_specs=hbm,
        out_shape=jax.ShapeDtypeStruct((n, d), BF16),
        scratch_shapes=[pltpu.VMEM((d, n), F32), pltpu.VMEM((d, n), F32), pltpu.VMEM((n, d), BF16), pltpu.SemaphoreType.DMA((2, d // COLS)), pltpu.SemaphoreType.DMA((d // COLS,))],
        compiler_params=pltpu.CompilerParams(vmem_limit_bytes=67043328),
        name='final',
    )(own, back)


def solution(mesh):
    token_spec = P(('dp', 'ep'), None)
    expert_spec = P('ep', None, None)
    whole_spec = P(None, None)
    grad_spec = P(('dp', 'ep'), None, None)
    group = mesh.shape['ep']

    def local_backward(x, dy, expert_ids, gate_vals, slot_pos, w1, w3, w2, s1, s3, s2):
        dat, dbt, ht, tok, pick, gate, own, far, sdat, sdbt, sht = exchange_call(x, dy, expert_ids.T, slot_pos.T, gate_vals.T, w1, w3, w2, s1, s3, s2)
        back = lax.ppermute(far, 'ep', [(i, i ^ 2) for i in range(group)])
        dw1, dw3, dw2, ds1, ds3, ds2 = weight_call(tok, pick, gate, dat, dbt, ht, sdat, sdbt, sht)
        grad_x = final_call(own, back)
        return grad_x, dw1, dw3, dw2, ds1, ds3, ds2

    return jax.shard_map(local_backward, mesh=mesh, in_specs=(token_spec, token_spec, token_spec, token_spec, token_spec, expert_spec, expert_spec, expert_spec, whole_spec, whole_spec, whole_spec), out_specs=(token_spec, grad_spec, grad_spec, grad_spec, grad_spec, grad_spec, grad_spec), check_vma=False)
```

```python
import jax
import jax.numpy as jnp
from jax import lax
from jax.experimental import pallas as pl
from jax.experimental.pallas import tpu as pltpu
from jax.sharding import PartitionSpec as P


F32, BF16 = jnp.float32, jnp.bfloat16
MESH = pl.DeviceIdType.MESH
SLOTS = 64
COLS = 512
RING, RING2 = 16, 16
OUTS = 5


def dot(a, b):
    return jnp.dot(a, b, preferred_element_type=F32)


def dot_nt(a, b):
    return lax.dot_general(a, b, (((1,), (1,)), ((), ())), preferred_element_type=F32)


def span(index, size):
    return pl.ds(pl.multiple_of(index * size, size), size)


def swiglu_factors(a, b):
    a, b = a.astype(F32), b.astype(F32)
    sigma = 0.5 * jnp.tanh(0.5 * a) + 0.5
    silu = a * sigma
    return (silu * b).astype(BF16), b * (sigma + silu * (1.0 - sigma)), silu


def put_rows(got, q, rows):
    for e in range(rows.shape[0]):
        rows[e, span(q, SLOTS), :] = got[e * SLOTS:(e + 1) * SLOTS]


def exchange_kernel(x, dy, ids, slots, gates, w1, w3, w2, s1, s3, s2, dat_o, dbt_o, ht_o, tok_o, pick_o, gate_o, own_o, far_o, sdat_o, sdbt_o, sht_o,
                    xg, yg, tabv, tabg, wring, w2ring, acc, gacc, act, rows, pick, gate, ret, spread, sbuf, rbuf, own, far,
                    near_s, near_r, far_s, far_r, hop_s, hop_r, tab_s, tab_r, sum_s, sum_r, wsem, w2sem, osem, esem):
    me = lax.axis_index('ep')
    core = me % 2
    mate = me + 1 - 2 * core
    other = (me + 2) % 4
    diag = (mate + 2) % 4
    experts, d, ff = w1.shape
    n = x.shape[0]
    chunks = d // COLS
    pieces = chunks * experts

    barrier = pltpu.get_barrier_semaphore()
    for peer in (mate, other, diag):
        pl.semaphore_signal(barrier, inc=1, device_id={'ep': peer}, device_id_type=MESH)

    tabv[...] = jnp.zeros_like(tabv)
    top_k = ids.shape[0]
    tabv[0, :top_k, :] = ids[...].astype(F32)
    tabv[1, :top_k, :] = slots[...].astype(F32)
    tabv[2, :top_k, :] = gates[...]

    def w_copy(i, k):
        src = (w1, w3)[k].at[i % experts, span((i // experts) % chunks, COLS), :]
        return pltpu.make_async_copy(src, wring.at[i % RING, k], wsem.at[i % RING, k])

    def w2_copy(j):
        return pltpu.make_async_copy(w2.at[j % experts, :, span(j // experts, COLS)], w2ring.at[j % RING2], w2sem.at[j % RING2])

    def s_copy(k, c):
        src = s2.at[:, span(c, COLS)] if k == 2 else (s1, s3)[k].at[span(c, COLS), :]
        return pltpu.make_async_copy(src, w2ring.at[k * chunks + c], w2sem.at[k * chunks + c])

    def each(count, body):
        def step(i, carry):
            body(i)
            return carry

        lax.fori_loop(0, count, step, 0)

    def start_w(i):
        w_copy(i, 0).start()
        w_copy(i, 1).start()

    def wait_w(i):
        w_copy(i, 0).wait()
        w_copy(i, 1).wait()

    for k in range(3):
        each(chunks, lambda c: s_copy(k, c).start())

    def clear(e):
        acc[0, e] = jnp.zeros_like(acc[0, e])
        acc[1, e] = jnp.zeros_like(acc[1, e])
        gacc[e] = jnp.zeros_like(gacc[e])

    each(experts, clear)

    def remote(src, dst, send, recv, peer):
        return pltpu.make_async_remote_copy(src_ref=src, dst_ref=dst, send_sem=send, recv_sem=recv, device_id={'ep': peer}, device_id_type=MESH)

    own_of, got_of = (x, dy), (xg, yg)

    def far_copy(a, c):
        return remote(own_of[a].at[:, span(c, COLS)], got_of[a].at[0, :, span(c, COLS)], far_s.at[a, c], far_r.at[a, c], other)

    def near_copy(a):
        return remote(own_of[a], got_of[a].at[1], near_s.at[a], near_r.at[a], mate)

    def hop_copy(a, c):
        return remote(got_of[a].at[0, :, span(c, COLS)], got_of[a].at[2, :, span(c, COLS)], hop_s.at[a, c], hop_r.at[a, c], mate)

    def tab_copy(k):
        return remote(tabv, tabg.at[k], tab_s.at[k], tab_r.at[k], (other, mate, diag)[k])

    def sum_copy(m):
        return remote(sbuf.at[m], rbuf.at[m], sum_s.at[m], sum_r.at[m], mate)

    pl.semaphore_wait(barrier, 3)
    for k in range(3):
        tab_copy(k).start()
    each(chunks, lambda c: far_copy(0, c).start())
    near_copy(0).start()
    near_copy(1).start()

    for k in range(3):
        each(chunks, lambda c: s_copy(k, c).wait())
    each(RING // 2, start_w)

    def over_chunks(one):
        total = one(0)
        for c in range(1, chunks):
            total += one(c)
        return total

    def cols(c):
        return slice(c * COLS, (c + 1) * COLS)

    at = over_chunks(lambda c: dot(x[:, cols(c)], w2ring[c])).astype(BF16).astype(F32).T
    bt = over_chunks(lambda c: dot(x[:, cols(c)], w2ring[chunks + c])).astype(BF16).astype(F32).T
    grad = over_chunks(lambda c: dot_nt(w2ring[2 * chunks + c], dy[:, cols(c)]))
    sht_o[...], by_a, by_b = swiglu_factors(at, bt)
    sdat_o[...], sdbt_o[...] = (grad * by_a).astype(BF16), (grad * by_b).astype(BF16)
    each(RING // 2, lambda i: start_w(i + RING // 2))

    def shared_back(m):
        own[span(m, COLS), :] = dot(w2ring[m], sdat_o[...]) + dot(w2ring[chunks + m], sdbt_o[...])

    each(chunks, shared_back)
    each(RING2, lambda j: w2_copy(j).start())

    for k in range(3):
        tab_copy(k).wait()
    mine = (me * experts + lax.broadcasted_iota(jnp.int32, (experts, n), 0)).astype(F32)
    rank = lax.broadcasted_iota(jnp.int32, (SLOTS, n), 0).astype(F32)
    for q in range(4):
        tabq = tabv if q == 0 else tabg.at[q - 1]
        slot = jnp.full((experts, n), -1.0, F32)
        weight = jnp.zeros((experts, n), F32)
        for j in range(ids.shape[0]):
            hit = mine == tabq[0, j:j + 1, :]
            slot = jnp.where(hit, tabq[1, j:j + 1, :], slot)
            weight = jnp.where(hit, tabq[2, j:j + 1, :], weight)
        for e in range(experts):
            hit = rank == slot[e:e + 1, :]
            pick[q, e * SLOTS:(e + 1) * SLOTS, :] = jnp.where(hit, 1.0, 0.0).astype(BF16)
            gate[q, e * SLOTS:(e + 1) * SLOTS, :] = jnp.sum(jnp.where(hit, weight[e:e + 1, :], 0.0), axis=1, keepdims=True)
    for h in range(2):
        spread[h] = jnp.zeros_like(spread[h])
        for e in range(experts):
            for j in range(2):
                spread[h, e * 2 * SLOTS + j * SLOTS:e * 2 * SLOTS + (j + 1) * SLOTS, j * n:(j + 1) * n] = pick[2 * h + j, e * SLOTS:(e + 1) * SLOTS, :]

    def expect(a, c):
        far_copy(a, c).wait()
        hop_copy(a, c).start()

    def gather_chunk(a, c):
        for q in range(4):
            src = own_of[a] if q == 0 else got_of[a].at[q - 1]
            got = dot(pick[q], src[:, span(c, COLS)])
            if a == 1:
                got = got * gate[q]
            put_rows(got.astype(BF16), q, rows)

    expect(0, 0)
    near_copy(0).wait()

    def up_chunk(c):
        far_copy(1, c).start()
        hop_copy(0, c).wait()

        @pl.when((c > 0) & (c + 1 < chunks))
        def _():
            expect(0, c + 1)

        @pl.when(c + 1 == chunks)
        def _():
            expect(1, 0)

        base = c * experts
        for e in range(experts):
            wait_w(base + e)
        gather_chunk(0, c)
        for e in range(experts):
            slot = (base + e) % RING
            acc[0, e] += dot(rows[e], wring[slot, 0])
            acc[1, e] += dot(rows[e], wring[slot, 1])
        for e in range(experts):
            start_w(base + e + RING)

        @pl.when(c == 0)
        def _():
            expect(0, 1)

    each(chunks, up_chunk)
    near_copy(1).wait()

    half = ff // 2

    def prepare(e):
        for h in range(2):
            part = slice(h * half, (h + 1) * half)
            a, b = acc[0, e, :, part].T.astype(BF16), acc[1, e, :, part].T.astype(BF16)
            act[2, e, part, :], acc[0, e, :, part], acc[1, e, :, part] = swiglu_factors(a, b)

    def down_chunk(c):
        hop_copy(1, c).wait()

        @pl.when(c + 1 < chunks)
        def _():
            expect(1, c + 1)

        base = c * experts
        for e in range(experts):
            w2_copy(base + e).wait()
        gather_chunk(1, c)
        for k in range(2):
            prepare(2 * c + k)
        for e in range(experts):
            gacc[e] += dot_nt(w2ring[(base + e) % RING2], rows[e])

        @pl.when(base + RING2 < pieces)
        def _():
            for e in range(experts):
                w2_copy(base + e + RING2).start()

    each(chunks, down_chunk)
    outs = [pltpu.make_async_copy(x, tok_o.at[0, 0], osem.at[0]), pltpu.make_async_copy(xg, tok_o.at[0, 1:4], osem.at[1]),
            pltpu.make_async_copy(dy, tok_o.at[1, 0], osem.at[2]), pltpu.make_async_copy(yg, tok_o.at[1, 1:4], osem.at[3]),
            pltpu.make_async_copy(pick, pick_o, osem.at[4]), pltpu.make_async_copy(gate, gate_o, osem.at[5])]
    for copy in outs:
        copy.start()

    def middle(e):
        for h in range(2):
            part = slice(h * half, (h + 1) * half)
            for k in range(2):
                act[k, e, part, :] = (gacc[e, part, :] * acc[k, e, :, part]).astype(BF16)

    each(experts, middle)
    outs += [pltpu.make_async_copy(act.at[k], (dat_o, dbt_o, ht_o)[k], osem.at[6 + k]) for k in range(3)]
    for copy in outs[6:]:
        copy.start()

    def back_chunk(m):
        base = pieces + m * experts
        for e in range(experts):
            wait_w(base + e)
        for e in range(experts):
            slot = (base + e) % RING
            part = (dot(wring[slot, 0], act[0, e]) + dot(wring[slot, 1], act[1, e])).astype(BF16)
            for h in range(2):
                ret[h, :, e * 2 * SLOTS:(e + 1) * 2 * SLOTS] = part[:, h * 2 * SLOTS:(h + 1) * 2 * SLOTS]
        give = dot(ret[1], spread[1])
        keep = dot(ret[0], spread[0])
        sbuf[m] = give
        own[span(m, COLS), :] += keep[:, :n]
        far[span(m, COLS), :] = keep[:, n:]
        sum_copy(m).start()

        for half in (0, experts // 2):
            @pl.when(base + half + RING < 2 * pieces)
            def _():
                for k in range(half, half + experts // 2):
                    start_w(base + k + RING)

        @pl.when(m > 0)
        def _():
            add_mate(m - 1)

    def out_copies(m):
        at = span(m, COLS)
        return pltpu.make_async_copy(own.at[at, :], own_o.at[at, :], esem.at[0, m]), pltpu.make_async_copy(far.at[at, :], far_o.at[at, :], esem.at[1, m])

    def add_mate(m):
        sum_copy(m).wait()
        own[span(m, COLS), :] += rbuf[m, :, :n]
        far[span(m, COLS), :] += rbuf[m, :, n:]
        for copy in out_copies(m):
            copy.start()

    each(chunks, back_chunk)
    add_mate(chunks - 1)
    for m in range(chunks):
        for copy in out_copies(m):
            copy.wait()
    for copy in outs:
        copy.wait()


def exchange_call(x, dy, ids, slots, gates, w1, w3, w2, s1, s3, s2):
    experts, d, ff = w1.shape
    n = x.shape[0]
    chunks, rows = d // COLS, 4 * SLOTS
    vmem, hbm = pl.BlockSpec(memory_space=pltpu.VMEM), pl.BlockSpec(memory_space=pl.ANY)
    dma = pltpu.SemaphoreType.DMA
    return pl.pallas_call(
        exchange_kernel,
        in_specs=[vmem] * 5 + [hbm] * 6,
        out_specs=[hbm] * 8 + [vmem] * 3,
        out_shape=[jax.ShapeDtypeStruct((experts, ff, rows), BF16)] * 3 + [jax.ShapeDtypeStruct((2, 4, n, d), BF16), jax.ShapeDtypeStruct((4, experts * SLOTS, n), BF16), jax.ShapeDtypeStruct((4, experts * SLOTS, 1), F32)] + [jax.ShapeDtypeStruct((d, n), F32)] * 2 + [jax.ShapeDtypeStruct((ff, n), BF16)] * 3,
        scratch_shapes=[
            pltpu.VMEM((3, n, d), BF16), pltpu.VMEM((3, n, d), BF16), pltpu.VMEM((3, 16, n), F32), pltpu.VMEM((3, 3, 16, n), F32),
            pltpu.VMEM((RING, 2, COLS, ff), BF16), pltpu.VMEM((RING2, ff, COLS), BF16),
            pltpu.VMEM((2, experts, rows, ff), F32), pltpu.VMEM((experts, ff, rows), F32), pltpu.VMEM((3, experts, ff, rows), BF16),
            pltpu.VMEM((experts, rows, COLS), BF16), pltpu.VMEM((4, experts * SLOTS, n), BF16), pltpu.VMEM((4, experts * SLOTS, 1), F32),
            pltpu.VMEM((2, COLS, experts * 2 * SLOTS), BF16), pltpu.VMEM((2, experts * 2 * SLOTS, 2 * n), BF16),
            pltpu.VMEM((chunks, COLS, 2 * n), F32), pltpu.VMEM((chunks, COLS, 2 * n), F32), pltpu.VMEM((d, n), F32), pltpu.VMEM((d, n), F32),
            dma((2,)), dma((2,)), dma((2, chunks)), dma((2, chunks)), dma((2, chunks)), dma((2, chunks)), dma((3,)), dma((3,)), dma((chunks,)), dma((chunks,)),
            dma((RING, 2)), dma((RING2,)), dma((9,)), dma((2, chunks)),
        ],
        compiler_params=pltpu.CompilerParams(collective_id=0, has_side_effects=True, vmem_limit_bytes=67043328),
        cost_estimate=pl.CostEstimate(flops=12 * experts * rows * d * ff, bytes_accessed=96 * 2**20, transcendentals=0),
        name='exchange',
    )(x, dy, ids, slots, gates, w1, w3, w2, s1, s3, s2)


def weight_kernel(sdat, sdbt, sht, tok_h, pick_h, gate_h, dat_h, dbt_h, ht_h, dw1, dw3, dw2, ds1, ds3, ds2, tok, pick, gate, act, rows, obuf, tsem, asem, osem):
    experts, d, _ = dw1.shape
    chunks = d // COLS
    slots = obuf.shape[0]

    def each(start, stop, body):
        def step(i, carry):
            body(i)
            return carry

        lax.fori_loop(start, stop, step, 0)

    def tok_copy(c):
        return pltpu.make_async_copy(tok_h.at[:, :, :, span(c, COLS)], tok.at[:, :, :, span(c, COLS)], tsem.at[c])

    def act_copy(k, i):
        return pltpu.make_async_copy((dat_h, dbt_h, ht_h)[k].at[i], act.at[k, i], asem.at[k, i])

    def out_copy(refs, k, i, c, slot):
        dst = refs[k].at[i, :, span(c, COLS)] if k == 2 else refs[k].at[i, span(c, COLS), :]
        return pltpu.make_async_copy(obuf.at[slot, k], dst, osem.at[slot, k])

    pick_copy = pltpu.make_async_copy(pick_h, pick, tsem.at[chunks])
    gate_copy = pltpu.make_async_copy(gate_h, gate, tsem.at[chunks + 1])
    tok_copy(0).start()
    pick_copy.start()
    gate_copy.start()
    each(1, chunks, lambda c: tok_copy(c).start())

    def start_act(i):
        for k in range(3):
            act_copy(k, i).start()

    each(0, experts, start_act)

    routed, shared = (dw1, dw3, dw2), (ds1, ds3, ds2)

    def claim(t):
        @pl.when(t >= slots)
        def _():
            for k in range(3):
                out_copy(routed, k, 0, 0, t % slots).wait()

    def shared_item(c):
        t = c * (experts + 1)
        claim(t)
        slot = t % slots
        xt = tok[0, 0, :, span(c, COLS)].T
        obuf[slot, 0] = dot_nt(xt, sdat[...])
        obuf[slot, 1] = dot_nt(xt, sdbt[...])
        obuf[slot, 2] = dot(sht[...], tok[1, 0, :, span(c, COLS)])
        for k in range(3):
            out_copy(shared, k, 0, c, slot).start()

    tok_copy(0).wait()
    shared_item(0)
    pick_copy.wait()
    gate_copy.wait()
    for q in range(4):
        put_rows(dot(pick[q], tok[0, q, :, :COLS]).astype(BF16), q, rows.at[0, 0])
        put_rows((dot(pick[q], tok[1, q, :, :COLS]) * gate[q]).astype(BF16), q, rows.at[0, 1])

    def chunk(c):
        now, later, follow = c % 2, (c + 1) % 2, (c + 1) % chunks

        @pl.when(c > 0)
        def _():
            shared_item(c)

        @pl.when(c + 1 < chunks)
        def _():
            tok_copy(c + 1).wait()

        def expert(e):
            t = c * (experts + 1) + 1 + e
            claim(t)

            @pl.when(c == 0)
            def _():
                for k in range(3):
                    act_copy(k, e).wait()

            slot = t % slots
            a, q = e % 2, e // 2
            got = dot(pick[q], tok[a, q, :, span(follow, COLS)]) * jnp.where(a == 1, gate[q], 1.0)
            xt = rows[now, 0, e].T
            obuf[slot, 0] = dot_nt(xt, act[0, e])
            obuf[slot, 1] = dot_nt(xt, act[1, e])
            obuf[slot, 2] = dot(act[2, e], rows[now, 1, e])
            put_rows(got.astype(BF16), q, rows.at[later, a])
            for k in range(3):
                out_copy(routed, k, e, c, slot).start()

        each(0, experts, expert)

    each(0, chunks, chunk)
    for slot in range(slots):
        for k in range(3):
            out_copy(routed, k, 0, 0, slot).wait()


def weight_call(tok, pick, gate, dat, dbt, ht, sdat, sdbt, sht):
    experts, ff, rows = dat.shape
    _, d = tok.shape[2:]
    chunks = d // COLS
    vmem, hbm = pl.BlockSpec(memory_space=pltpu.VMEM), pl.BlockSpec(memory_space=pl.ANY)
    dma = pltpu.SemaphoreType.DMA
    return pl.pallas_call(
        weight_kernel,
        in_specs=[vmem] * 3 + [hbm] * 6,
        out_specs=[hbm] * 6,
        out_shape=[jax.ShapeDtypeStruct((experts, d, ff), F32)] * 2 + [jax.ShapeDtypeStruct((experts, ff, d), F32)] + [jax.ShapeDtypeStruct((1, d, ff), F32)] * 2 + [jax.ShapeDtypeStruct((1, ff, d), F32)],
        scratch_shapes=[
            pltpu.VMEM(tok.shape, BF16), pltpu.VMEM(pick.shape, BF16), pltpu.VMEM(gate.shape, F32), pltpu.VMEM((3, experts, ff, rows), BF16),
            pltpu.VMEM((2, 2, experts, rows, COLS), BF16), pltpu.VMEM((OUTS, 3, COLS, ff), F32),
            dma((chunks + 2,)), dma((3, experts)), dma((OUTS, 3)),
        ],
        compiler_params=pltpu.CompilerParams(vmem_limit_bytes=60 * 2**20),
        cost_estimate=pl.CostEstimate(flops=6 * experts * rows * d * ff, bytes_accessed=124 * 2**20, transcendentals=0),
        name='weights',
    )(sdat, sdbt, sht, tok, pick, gate, dat, dbt, ht)


def final_kernel(own_h, back_h, out_h, own, back, out, isem, osem):
    parts = own.shape[0] // COLS
    loads = [[pltpu.make_async_copy(src.at[pl.ds(p * COLS, COLS), :], dst.at[pl.ds(p * COLS, COLS), :], isem.at[k, p]) for k, (src, dst) in enumerate(((own_h, own), (back_h, back)))] for p in range(parts)]
    for pair in loads:
        for copy in pair:
            copy.start()
    stores = []
    for p in range(parts):
        for copy in loads[p]:
            copy.wait()
        at = pl.ds(p * COLS, COLS)
        out[:, at] = (own[at, :] + back[at, :]).T.astype(BF16)
        stores.append(pltpu.make_async_copy(out.at[:, at], out_h.at[:, at], osem.at[p]))
        stores[-1].start()
    for copy in stores:
        copy.wait()


def final_call(own, back):
    d, n = own.shape
    hbm = pl.BlockSpec(memory_space=pl.ANY)
    return pl.pallas_call(
        final_kernel,
        in_specs=[hbm, hbm],
        out_specs=hbm,
        out_shape=jax.ShapeDtypeStruct((n, d), BF16),
        scratch_shapes=[pltpu.VMEM((d, n), F32), pltpu.VMEM((d, n), F32), pltpu.VMEM((n, d), BF16), pltpu.SemaphoreType.DMA((2, d // COLS)), pltpu.SemaphoreType.DMA((d // COLS,))],
        compiler_params=pltpu.CompilerParams(vmem_limit_bytes=67043328),
        name='final',
    )(own, back)


def solution(mesh):
    token_spec = P(('dp', 'ep'), None)
    expert_spec = P('ep', None, None)
    whole_spec = P(None, None)
    grad_spec = P(('dp', 'ep'), None, None)
    group = mesh.shape['ep']

    def local_backward(x, dy, expert_ids, gate_vals, slot_pos, w1, w3, w2, s1, s3, s2):
        dat, dbt, ht, tok, pick, gate, own, far, sdat, sdbt, sht = exchange_call(x, dy, expert_ids.T, slot_pos.T, gate_vals.T, w1, w3, w2, s1, s3, s2)
        back = lax.ppermute(far, 'ep', [(i, i ^ 2) for i in range(group)])
        dw1, dw3, dw2, ds1, ds3, ds2 = weight_call(tok, pick, gate, dat, dbt, ht, sdat, sdbt, sht)
        grad_x = final_call(own, back)
        return grad_x, dw1, dw3, dw2, ds1, ds3, ds2

    return jax.shard_map(local_backward, mesh=mesh, in_specs=(token_spec, token_spec, token_spec, token_spec, token_spec, expert_spec, expert_spec, expert_spec, whole_spec, whole_spec, whole_spec), out_specs=(token_spec, grad_spec, grad_spec, grad_spec, grad_spec, grad_spec, grad_spec), check_vma=False)
```
